32 devices in a mesh: groups: 2 (over x), depth: 2 (over core), row: 8 (over z, y).
Axes of the slice: x: 2, y: 2, z: 4, core: 2. Of those that a mesh axis runs over, the one named last changes fastest.
Arguments:
- planes: float32 [4, 4, 512, 512], P('groups', None, 'row'), parts along dimension 0, may hold values from -6 to 6
- slowness: float32 [2, 512, 512], P('depth', 'row'), may hold values from 0.6 to 1.4
- ref_slowness: float32 [2], replicated, may hold values from 0.8 to 1.2
- freq_index: int32 [2], replicated, may hold values from 10 to 51
Outputs:
- image: float32 [4, 512, 512], P(('groups', 'depth'), 'row'), parts along dimension 0
- leaving: float32 [4, 4, 512, 512], P(('groups', 'depth'), None, 'row'), parts along dimension 0
The draws below stay inside these ranges and needn't reach their ends.
There are 2 independent parts, one for each index of `groups`. The reference program is written for one: setup_inputs(seed, part) draws one part's arguments, and reference() takes and returns one part's arrays. A program takes and returns all parts, laid end to end along the dimension named above; an argument that names none is the same for every part. Nothing has to cross between parts.
All inputs are finite; a program needn't handle non-finite values.
Results may differ from the reference program's by a relative error of at most 0.0003.
Values sent between devices are 32-bit elements; how exact they have to be, the bound alone decides.
No kernel may reach another device: no remote copies, remote signals or barrier semaphores. Data moves between devices by JAX's collectives and lax.ppermute only.
A program may use at most 64 MiB of HBM per device.

```python
import jax
import jax.numpy as jnp
from jax import lax

GRID = 512
FREQS = 2
NZ = 2


def steps_of(own_key, dims, cuts, smallest, largest):
    factor_of = 1.0
    for axis_at, shards_of in cuts:
        heights = jax.random.uniform(jax.random.fold_in(jax.random.fold_in(own_key, 6), axis_at), (shards_of,), jnp.float32, smallest / len(cuts), largest / len(cuts))
        factor_of = factor_of * jnp.repeat(jnp.exp(heights), dims[axis_at] // shards_of).reshape((-1,) + (1,) * (len(dims) - 1 - axis_at))
    return factor_of


def noise(rng, dims, width, most, cuts=(), kind=jnp.bfloat16):
    values = jax.random.normal(rng, dims, jnp.float32) * width
    if len(cuts) > 0:
        values = steps_of(rng, dims, cuts, -0.22, 0.18) * values
    return jnp.clip(values, min=-most, max=most).astype(kind)


def setup_inputs(seed: int = 0, part: int = 0) -> dict:
    key_list = jax.random.split(jax.random.key(seed), 5)
    part_keys = jax.random.split(jax.random.fold_in(key_list[4], part), 5)
    planes = noise(part_keys[0], (FREQS, 4, GRID, GRID), 1.0, 6.0, ((2, 8),), jnp.float32)
    slowness = jnp.clip(0.6 + 0.79999995 * jax.random.uniform(key_list[1], (NZ, GRID, GRID), jnp.float32) ** steps_of(key_list[1], (NZ, GRID, GRID), ((0, 2), (1, 8)), -0.2, 0.2), 0.6, 1.4)
    ref_slowness = jnp.clip(jax.random.uniform(key_list[2], (NZ,), jnp.float32, 0.8, 1.2), 0.8, 1.2)
    freq_index = jax.random.randint(key_list[3], (FREQS,), 10, 52).astype(jnp.int32)
    return {"planes": planes, "slowness": slowness, "ref_slowness": ref_slowness, "freq_index": freq_index}


omega_step = 0.05
depth_step = 1.0

def wavenumbers():
    positions = jnp.arange(GRID, dtype=jnp.int32)
    signed = jnp.where(positions < GRID // 2, positions, positions - GRID)
    return 2.0 * jnp.pi / GRID * signed.astype(jnp.float32)

def reference(planes, slowness, ref_slowness, freq_index):
    waves = wavenumbers()
    plane_waves = waves[:, None] ** 2 + waves[None, :] ** 2
    omegas = omega_step * freq_index.astype(jnp.float32)
    source = planes[:, 0] + 1j * planes[:, 1]
    receiver = planes[:, 2] + 1j * planes[:, 3]
    images = []
    for level in range(NZ):
        radicand = (omegas[:, None, None] * ref_slowness[level]) ** 2 - plane_waves[None]
        vertical = jnp.sqrt(jnp.maximum(radicand, 0.0)) * depth_step
        damping = jnp.exp(-jnp.sqrt(jnp.maximum(-radicand, 0.0)) * depth_step)
        source = jnp.fft.ifft2(jnp.fft.fft2(source) * (damping * jnp.cos(vertical) - 1j * damping * jnp.sin(vertical)))
        receiver = jnp.fft.ifft2(jnp.fft.fft2(receiver) * (damping * jnp.cos(vertical) + 1j * damping * jnp.sin(vertical)))
        screen_phase = omegas[:, None, None] * (slowness[level] - ref_slowness[level])[None] * depth_step
        source = source * (jnp.cos(screen_phase) - 1j * jnp.sin(screen_phase))
        receiver = receiver * (jnp.cos(screen_phase) + 1j * jnp.sin(screen_phase))
        images.append(lax.optimization_barrier(jnp.sum(source.real * receiver.real + source.imag * receiver.imag, axis=0)))
    leaving = jnp.stack([source.real, source.imag, receiver.real, receiver.imag], axis=1)
    return (jnp.stack(images), leaving)
```

```python
import functools

import jax
import jax.numpy as jnp
import numpy as np
from jax import lax
from jax.experimental import pallas as pl
from jax.experimental.pallas import tpu as pltpu
from jax.sharding import PartitionSpec as P

omega_step = 0.05
depth_step = 1.0
lanes = 128


def pair(table):
    high = table.astype(jnp.bfloat16)
    low = (table - high.astype(np.float64)).astype(jnp.bfloat16)
    return np.stack([high, low])


def real_form(points):
    product = np.outer(np.arange(points), np.arange(points)) % points
    angle = 2.0 * np.pi / points * product
    c, s = np.cos(angle), np.sin(angle)
    return pair(np.block([[c, -s], [s, c]])), pair(np.block([[c, s], [-s, c]]))


def twiddles(length, radix):
    points = length // radix
    angle = 2.0 * np.pi / length * np.outer(np.arange(radix), np.arange(points))
    return np.stack([np.cos(angle), -np.sin(angle)], axis=1).astype(np.float32)


def split(x):
    high = x.astype(jnp.bfloat16)
    return high, (x - high.astype(jnp.float32)).astype(jnp.bfloat16)


def dot(a, b):
    return jnp.dot(a, b, preferred_element_type=jnp.float32)


def times_table(x, table):
    high, low = split(x)
    return dot(high, table[0]) + dot(low, table[0]) + dot(high, table[1])


def table_times(table, x):
    high, low = split(x)
    return dot(table[0], high) + dot(table[0], low) + dot(table[1], high)


def scaled(value, factor):
    if value is None or factor == 0.0:
        return None
    if factor == 1.0:
        return value
    return -value if factor == -1.0 else value * factor


def plus(a, b):
    if a is None:
        return b
    return a if b is None else a + b


def small_transform(parts, sign):
    radix = len(parts)
    if radix == 1:
        return parts
    if radix % 2 == 0:
        half = radix // 2
        even = small_transform(parts[0::2], sign)
        odd = small_transform(parts[1::2], sign)
        first, second = [], []
        for r in range(half):
            angle = sign * 2.0 * np.pi * r / radix
            c, s = float(np.round(np.cos(angle), 15)), float(np.round(np.sin(angle), 15))
            ore, oim = odd[r]
            tre = plus(scaled(ore, c), scaled(oim, -s))
            tim = plus(scaled(oim, c), scaled(ore, s))
            ere, eim = even[r]
            first.append((ere + tre, eim + tim))
            second.append((ere - tre, eim - tim))
        return first + second
    raise ValueError("radix")


def turn(part, factor, conjugate):
    re, im = part
    fre, fim = factor
    if conjugate:
        return re * fre + im * fim, im * fre - re * fim
    return re * fre - im * fim, im * fre + re * fim


def rows_of(parts):
    return jnp.concatenate([jnp.concatenate(part, axis=1) for part in parts], axis=0)


def row_forward(cells, tw, table, points):
    stacked = []
    for parts in cells:
        for r, part in enumerate(small_transform(parts, -1.0)):
            factor = (tw[r, 0:1], tw[r, 1:2])
            stacked.append(part if r == 0 else turn(part, factor, False))
    return times_table(rows_of(stacked), table)


def row_inverse(ref, tw, table, radix, planes):
    rows, points = ref.shape[2], ref.shape[3]
    count = planes * radix
    stacked = jnp.concatenate(
        [ref[:, 0].reshape(count * rows, points), ref[:, 1].reshape(count * rows, points)], axis=1
    )
    out = times_table(stacked, table)
    cells = []
    for p in range(planes):
        parts = []
        for r in range(radix):
            at = (p * radix + r) * rows
            part = (out[at : at + rows, :points], out[at : at + rows, points:])
            parts.append(part if r == 0 else turn(part, (tw[r, 0:1], tw[r, 1:2]), True))
        cells.append(small_transform(parts, 1.0))
    return cells


def store_blocks(out_ref, value, count, rows, points):
    out_ref[:, 0] = value[:, :points].reshape(count, rows, points)
    out_ref[:, 1] = value[:, points:].reshape(count, rows, points)


def first_kernel(radix, freq_ref, planes_ref, tw, table, out_ref):
    rows, points = out_ref.shape[2], out_ref.shape[3]
    cells = []
    for p in range(2):
        cells.append(
            [
                (
                    planes_ref[0, 2 * p, :, m * points : (m + 1) * points],
                    planes_ref[0, 2 * p + 1, :, m * points : (m + 1) * points],
                )
                for m in range(radix)
            ]
        )
    value = row_forward(cells, tw, table, points)
    store_blocks(out_ref, value, 2 * radix, rows, points)


def column_kernel(radix, in_ref, hre, him, tw, forward, inverse, out_ref):
    count, _, rows, width = in_ref.shape
    points = count * rows // radix
    per = points // rows

    def block(m, part):
        return in_ref[m * per : (m + 1) * per, part].reshape(points, width)

    parts = small_transform([(block(m, 0), block(m, 1)) for m in range(radix)], -1.0)
    columns = []
    for r, part in enumerate(parts):
        if r > 0:
            factor = (tw[:, 2 * r : 2 * r + 1], tw[:, 2 * r + 1 : 2 * r + 2])
            part = turn(part, factor, False)
        columns.append(jnp.concatenate(part, axis=0))
    spectrum = table_times(forward, jnp.concatenate(columns, axis=1))
    columns = []
    for r in range(radix):
        at = slice(r * width, (r + 1) * width)
        part = turn((spectrum[:points, at], spectrum[points:, at]), (hre[r], him[r]), False)
        columns.append(jnp.concatenate(part, axis=0))
    back = table_times(inverse, jnp.concatenate(columns, axis=1))
    parts = []
    for r in range(radix):
        at = slice(r * width, (r + 1) * width)
        part = (back[:points, at], back[points:, at])
        if r > 0:
            factor = (tw[:, 2 * r : 2 * r + 1], tw[:, 2 * r + 1 : 2 * r + 2])
            part = turn(part, factor, True)
        parts.append(part)
    for m, (re, im) in enumerate(small_transform(parts, 1.0)):
        out_ref[m * per : (m + 1) * per, 0] = re.reshape(per, rows, width)
        out_ref[m * per : (m + 1) * per, 1] = im.reshape(per, rows, width)


def screened(cells, cos_ref, sin_ref, points):
    turned = ([], [])
    for m in range(len(cells[0])):
        at = slice(m * points, (m + 1) * points)
        factor = (cos_ref[:, at], sin_ref[:, at])
        turned[0].append(turn(cells[0][m], factor, True))
        turned[1].append(turn(cells[1][m], factor, False))
    return turned


def middle_kernel(radix, in_ref, cos_ref, sin_ref, tw, inverse, forward, out_ref, image_ref):
    rows, points = in_ref.shape[2], in_ref.shape[3]
    cells = screened(row_inverse(in_ref, tw, inverse, radix, 2), cos_ref, sin_ref, points)
    for m in range(radix):
        (sre, sim), (rre, rim) = cells[0][m], cells[1][m]
        image_ref[:, m * points : (m + 1) * points] = sre * rre + sim * rim
    value = row_forward(cells, tw, forward, points)
    store_blocks(out_ref, value, 2 * radix, rows, points)


def last_kernel(radix, in_ref, cos_ref, sin_ref, tw, inverse, leaving_ref, image_ref):
    points = in_ref.shape[3]
    cells = screened(row_inverse(in_ref, tw, inverse, radix, 2), cos_ref, sin_ref, points)
    for m in range(radix):
        at = slice(m * points, (m + 1) * points)
        (sre, sim), (rre, rim) = cells[0][m], cells[1][m]
        leaving_ref[0, 0, :, at] = sre
        leaving_ref[0, 1, :, at] = sim
        leaving_ref[0, 2, :, at] = rre
        leaving_ref[0, 3, :, at] = rim
        image_ref[:, at] = sre * rre + sim * rim


def signed_wave(positions, length):
    signed = jnp.where(positions < length // 2, positions, positions - length)
    return 2.0 * jnp.pi / length * signed.astype(jnp.float32)


def call(kernel, out_shapes):
    return pl.pallas_call(kernel, out_shape=[jax.ShapeDtypeStruct(s, jnp.float32) for s in out_shapes])


def shards(planes, slowness, ref_slowness, freq_index):
    _, _, rows, length = planes.shape
    ranks = lax.axis_size("row")
    radix = ranks // 2
    points = length // radix
    col_radix = length // lanes
    row_index, core = lax.axis_index("row"), lax.axis_index("depth")

    row_forward_table, row_inverse_table = real_form(points)
    col_inverse_table, col_forward_table = real_form(lanes)
    row_tw = twiddles(length, radix)
    col_tw = twiddles(length, col_radix).transpose(2, 0, 1).reshape(lanes, 2 * col_radix)

    omega = omega_step * freq_index[core].astype(jnp.float32)
    other = lax.ppermute(slowness, "depth", [(0, 1), (1, 0)])
    own_first = core == 0
    screens = [
        jnp.where(own_first, slowness[0], other[0]),
        jnp.where(own_first, other[0], slowness[0]),
    ]

    blocks = (ranks, 2, rows, points)
    spectra = pl.pallas_call(
        functools.partial(first_kernel, radix),
        grid_spec=pltpu.PrefetchScalarGridSpec(
            num_scalar_prefetch=1,
            grid=(1,),
            in_specs=[
                pl.BlockSpec((1,) + planes.shape[1:], lambda i, f: (f[0], 0, 0, 0)),
                pl.BlockSpec(row_tw.shape, lambda i, f: (0, 0, 0)),
                pl.BlockSpec(row_forward_table.shape, lambda i, f: (0, 0, 0)),
            ],
            out_specs=pl.BlockSpec(blocks, lambda i, f: (0, 0, 0, 0)),
        ),
        out_shape=jax.ShapeDtypeStruct(blocks, jnp.float32),
    )(core.astype(jnp.int32).reshape(1), planes, row_tw, row_forward_table)

    residue = row_index % radix
    sign = jnp.where(row_index < radix, -1.0, 1.0)
    col_wave = signed_wave(
        (jnp.arange(lanes, dtype=jnp.int32)[None, :] * col_radix)
        + jnp.arange(col_radix, dtype=jnp.int32)[:, None],
        length,
    )
    row_wave = signed_wave(jnp.arange(points, dtype=jnp.int32) * radix + residue, length)
    plane_waves = col_wave[:, :, None] ** 2 + row_wave[None, None, :] ** 2
    scale = 1.0 / (length * length)

    def exchange(x):
        return lax.all_to_all(x, "row", split_axis=0, concat_axis=0, tiled=True)

    images = []
    for level in range(2):
        radicand = (omega * ref_slowness[level]) ** 2 - plane_waves
        vertical = jnp.sqrt(jnp.maximum(radicand, 0.0)) * depth_step
        damping = scale * jnp.exp(-jnp.sqrt(jnp.maximum(-radicand, 0.0)) * depth_step)
        hre, him = damping * jnp.cos(vertical), sign * damping * jnp.sin(vertical)
        theta = omega * (screens[level] - ref_slowness[level]) * depth_step
        cos_theta, sin_theta = jnp.cos(theta), jnp.sin(theta)
        columns = exchange(spectra)
        (columns,) = call(functools.partial(column_kernel, col_radix), [blocks])(
            columns, hre, him, col_tw, col_forward_table, col_inverse_table
        )
        cells = exchange(columns)
        if level == 0:
            spectra, image = call(functools.partial(middle_kernel, radix), [blocks, (rows, length)])(
                cells, cos_theta, sin_theta, row_tw, row_inverse_table, row_forward_table
            )
        else:
            leaving, image = call(
                functools.partial(last_kernel, radix), [(1,) + planes.shape[1:], (rows, length)]
            )(cells, cos_theta, sin_theta, row_tw, row_inverse_table)
        images.append(image)
    keep = jnp.where(own_first, images[0], images[1])
    send = jnp.where(own_first, images[1], images[0])
    image = keep + lax.ppermute(send, "depth", [(0, 1), (1, 0)])
    return image[None], leaving


def solution(mesh):
    in_specs = (P("groups", None, "row", None), P("depth", "row", None), P(), P())
    out_specs = (P(("groups", "depth"), "row", None), P(("groups", "depth"), None, "row", None))
    return jax.shard_map(shards, mesh=mesh, in_specs=in_specs, out_specs=out_specs, check_vma=False)
```

```python
import functools

import jax
import jax.numpy as jnp
import numpy as np
from jax import lax
from jax.experimental import pallas as pl
from jax.experimental.pallas import tpu as pltpu
from jax.sharding import PartitionSpec as P

omega_step = 0.05
depth_step = 1.0
lanes = 128


def pair(table):
    high = table.astype(jnp.bfloat16)
    low = (table - high.astype(np.float64)).astype(jnp.bfloat16)
    return np.stack([high, low])


def real_form(points):
    product = np.outer(np.arange(points), np.arange(points)) % points
    angle = 2.0 * np.pi / points * product
    c, s = np.cos(angle), np.sin(angle)
    return pair(np.block([[c, -s], [s, c]])), pair(np.block([[c, s], [-s, c]]))


def twiddles(length, radix):
    points = length // radix
    angle = 2.0 * np.pi / length * np.outer(np.arange(radix), np.arange(points))
    return np.stack([np.cos(angle), -np.sin(angle)], axis=1).astype(np.float32)


def split(x):
    high = x.astype(jnp.bfloat16)
    return high, (x - high.astype(jnp.float32)).astype(jnp.bfloat16)


def dot(a, b):
    return jnp.dot(a, b, preferred_element_type=jnp.float32)


def times_table(x, table):
    high, low = split(x)
    return dot(high, table[0]) + dot(low, table[0]) + dot(high, table[1])


def table_times(table, x):
    high, low = split(x)
    return dot(table[0], high) + dot(table[0], low) + dot(table[1], high)


def scaled(value, factor):
    if value is None or factor == 0.0:
        return None
    if factor == 1.0:
        return value
    return -value if factor == -1.0 else value * factor


def plus(a, b):
    if a is None:
        return b
    return a if b is None else a + b


def small_transform(parts, sign):
    radix = len(parts)
    if radix == 1:
        return parts
    if radix % 2 == 0:
        half = radix // 2
        even = small_transform(parts[0::2], sign)
        odd = small_transform(parts[1::2], sign)
        first, second = [], []
        for r in range(half):
            angle = sign * 2.0 * np.pi * r / radix
            c, s = float(np.round(np.cos(angle), 15)), float(np.round(np.sin(angle), 15))
            ore, oim = odd[r]
            tre = plus(scaled(ore, c), scaled(oim, -s))
            tim = plus(scaled(oim, c), scaled(ore, s))
            ere, eim = even[r]
            first.append((ere + tre, eim + tim))
            second.append((ere - tre, eim - tim))
        return first + second
    raise ValueError("radix")


def turn(part, factor, conjugate):
    re, im = part
    fre, fim = factor
    if conjugate:
        return re * fre + im * fim, im * fre - re * fim
    return re * fre - im * fim, im * fre + re * fim


def rows_of(parts):
    return jnp.concatenate([jnp.concatenate(part, axis=1) for part in parts], axis=0)


def row_forward(cells, tw, table, points):
    stacked = []
    for parts in cells:
        for r, part in enumerate(small_transform(parts, -1.0)):
            factor = (tw[r, 0:1], tw[r, 1:2])
            stacked.append(part if r == 0 else turn(part, factor, False))
    return times_table(rows_of(stacked), table)


def row_inverse(ref, tw, table, radix, planes):
    rows, points = ref.shape[2], ref.shape[3]
    count = planes * radix
    stacked = jnp.concatenate(
        [ref[:, 0].reshape(count * rows, points), ref[:, 1].reshape(count * rows, points)], axis=1
    )
    out = times_table(stacked, table)
    cells = []
    for p in range(planes):
        parts = []
        for r in range(radix):
            at = (p * radix + r) * rows
            part = (out[at : at + rows, :points], out[at : at + rows, points:])
            parts.append(part if r == 0 else turn(part, (tw[r, 0:1], tw[r, 1:2]), True))
        cells.append(small_transform(parts, 1.0))
    return cells


def store_blocks(out_ref, value, count, rows, points):
    out_ref[:, 0] = value[:, :points].reshape(count, rows, points)
    out_ref[:, 1] = value[:, points:].reshape(count, rows, points)


def half_transform(parts, odd):
    half = len(parts) // 2
    folded = []
    for m in range(half):
        (are, aim), (bre, bim) = parts[m], parts[m + half]
        if not odd:
            folded.append((are + bre, aim + bim))
            continue
        re, im = are - bre, aim - bim
        angle = -2.0 * np.pi * m / len(parts)
        c, s = float(np.round(np.cos(angle), 15)), float(np.round(np.sin(angle), 15))
        folded.append((plus(scaled(re, c), scaled(im, -s)), plus(scaled(im, c), scaled(re, s))))
    return small_transform(folded, -1.0)


def first_kernel(radix, planes_ref, tw, table, out_ref):
    count, _, rows, points = out_ref.shape
    for core in range(2):

        @pl.when(lax.axis_index("depth") == core)
        def _():
            stacked = []
            for p in range(planes_ref.shape[0] * 2):
                f, c = p // 2, 2 * (p % 2)
                parts = [
                    tuple(planes_ref[f, c + i, :, m * points : (m + 1) * points] for i in range(2))
                    for m in range(radix)
                ]
                for y, part in enumerate(half_transform(parts, core == 1)):
                    r = 2 * y + core
                    stacked.append(part if r == 0 else turn(part, (tw[r, 0:1], tw[r, 1:2]), False))
            value = times_table(rows_of(stacked), table)
            store_blocks(out_ref, value, count, rows, points)


def residue_of():
    per_plane = lax.axis_size("row") // 4
    return lax.axis_index("depth") + 2 * lax.rem(lax.axis_index("row"), per_plane)


def spread(held, out_refs):
    own = residue_of()
    for step, ref in enumerate(out_refs):
        ref[...] = held[own ^ step]


def collect(in_refs, held):
    own = residue_of()
    for step, ref in enumerate(in_refs):
        held[own ^ step] = ref[...]


def columns_to_quarters(col_radix, in_ref, hre, him, tw, forward, inverse, *rest):
    out_refs, held = rest[:-1], rest[-1]
    column_kernel(col_radix, in_ref, hre, him, tw, forward, inverse, held)
    spread(held, out_refs)


def quarters_to_columns(col_radix, radix, *refs):
    in_refs, (hre, him, tw, forward, inverse, out_ref, held) = refs[:radix], refs[radix:]
    collect(in_refs, held)
    column_kernel(col_radix, held, hre, him, tw, forward, inverse, out_ref)


def middle_kernel(radix, *refs):
    in_refs, (cos_ref, sin_ref, tw, inverse, forward) = refs[:radix], refs[radix : radix + 5]
    out_refs, (keep_ref, send_ref, held, field) = refs[radix + 5 : 2 * radix + 5], refs[2 * radix + 5 :]
    rows, points = held.shape[2], held.shape[3]
    collect(in_refs, held)
    (cells,) = row_inverse(held, tw, inverse, radix, 1)
    turned = []
    for m in range(radix):
        at = slice(m * points, (m + 1) * points)
        part = turn(cells[m], (cos_ref[:, at], sin_ref[:, at]), False)
        for half in range(2):
            for i in range(2):
                field[half, i, :, at] = part[i][half * rows // 2 : (half + 1) * rows // 2]
        turned.append(part)
    mine = lax.rem(lax.axis_index("row") // (lax.axis_size("row") // 4), 2)
    keep_ref[...] = field[mine]
    send_ref[...] = field[1 - mine]
    value = row_forward([turned], tw, forward, points)
    store_blocks(held, value, radix, rows, points)
    spread(held, out_refs)


def column_kernel(radix, in_ref, hre, him, tw, forward, inverse, out_ref):
    count, _, rows, width = in_ref.shape
    points = count * rows // radix
    per = points // rows
    out_rows = out_ref.shape[2]
    out_per = points // out_rows

    def block(m, part):
        return in_ref[m * per : (m + 1) * per, part].reshape(points, width)

    parts = small_transform([(block(m, 0), block(m, 1)) for m in range(radix)], -1.0)
    columns = []
    for r, part in enumerate(parts):
        if r > 0:
            factor = (tw[:, 2 * r : 2 * r + 1], tw[:, 2 * r + 1 : 2 * r + 2])
            part = turn(part, factor, False)
        columns.append(jnp.concatenate(part, axis=0))
    spectrum = table_times(forward, jnp.concatenate(columns, axis=1))
    columns = []
    for r in range(radix):
        at = slice(r * width, (r + 1) * width)
        part = turn((spectrum[:points, at], spectrum[points:, at]), (hre[r], him[r]), False)
        columns.append(jnp.concatenate(part, axis=0))
    back = table_times(inverse, jnp.concatenate(columns, axis=1))
    parts = []
    for r in range(radix):
        at = slice(r * width, (r + 1) * width)
        part = (back[:points, at], back[points:, at])
        if r > 0:
            factor = (tw[:, 2 * r : 2 * r + 1], tw[:, 2 * r + 1 : 2 * r + 2])
            part = turn(part, factor, True)
        parts.append(part)
    for m, (re, im) in enumerate(small_transform(parts, 1.0)):
        out_ref[m * out_per : (m + 1) * out_per, 0] = re.reshape(out_per, out_rows, width)
        out_ref[m * out_per : (m + 1) * out_per, 1] = im.reshape(out_per, out_rows, width)


def screened(cells, cos_ref, sin_ref, points):
    turned = ([], [])
    for m in range(len(cells[0])):
        at = slice(m * points, (m + 1) * points)
        factor = (cos_ref[:, at], sin_ref[:, at])
        turned[0].append(turn(cells[0][m], factor, True))
        turned[1].append(turn(cells[1][m], factor, False))
    return turned


def last_kernel(radix, in_ref, got_ref, cos_ref, sin_ref, tw, inverse, leaving_ref, image_ref, held):
    points = in_ref.shape[3]
    core = lax.axis_index("depth")
    per_plane = radix // 2
    for p in range(2):
        for y in range(per_plane):
            at = p * radix + 2 * y
            held[at + core] = in_ref[core * radix + p * per_plane + y]
            held[at + 1 - core] = got_ref[p * per_plane + y]
    cells = screened(row_inverse(held, tw, inverse, radix, 2), cos_ref, sin_ref, points)
    for m in range(radix):
        at = slice(m * points, (m + 1) * points)
        (sre, sim), (rre, rim) = cells[0][m], cells[1][m]
        leaving_ref[0, 0, :, at] = sre
        leaving_ref[0, 1, :, at] = sim
        leaving_ref[0, 2, :, at] = rre
        leaving_ref[0, 3, :, at] = rim
        image_ref[:, at] = sre * rre + sim * rim


def signed_wave(positions, length):
    signed = jnp.where(positions < length // 2, positions, positions - length)
    return 2.0 * jnp.pi / length * signed.astype(jnp.float32)


def call(kernel, out_shapes, scratch):
    return pl.pallas_call(
        kernel,
        out_shape=[jax.ShapeDtypeStruct(s, jnp.float32) for s in out_shapes],
        scratch_shapes=[pltpu.VMEM(s, jnp.float32) for s in scratch],
    )


def shards(planes, slowness, ref_slowness, freq_index):
    _, _, rows, length = planes.shape
    ranks = lax.axis_size("row")
    radix = ranks // 2
    per_plane = radix // 2
    points = length // radix
    col_radix = length // lanes
    row_index, core = lax.axis_index("row"), lax.axis_index("depth")
    own_first = core == 0

    row_forward_table, row_inverse_table = real_form(points)
    col_inverse_table, col_forward_table = real_form(lanes)
    row_tw = twiddles(length, radix)
    col_tw = twiddles(length, col_radix).transpose(2, 0, 1).reshape(lanes, 2 * col_radix)
    swap = [(0, 1), (1, 0)]
    both = ("depth", "row")

    def flat(c, r):
        return c * ranks + r

    def inner(arrays):
        got = [arrays[0]] + [None] * (radix - 1)
        for step in list(range(2, radix)) + [1]:
            pairs = [
                (flat(c, r), flat(c ^ (step & 1), r ^ (step >> 1))) for c in range(2) for r in range(ranks)
            ]
            got[step] = lax.ppermute(arrays[step], both, pairs)
        return got

    def exchange(x):
        return lax.all_to_all(x, "row", split_axis=0, concat_axis=0, tiled=True)

    def twin(x):
        return lax.ppermute(x, "row", [(r, r ^ per_plane) for r in range(ranks)])

    plane = row_index // per_plane
    residue = residue_of()
    sign = jnp.where(plane % 2 == 0, -1.0, 1.0)
    omegas = omega_step * freq_index.astype(jnp.float32)
    omega = omegas[plane // 2]

    other = lax.ppermute(slowness, "depth", swap)
    blocks = (ranks, 2, rows, points)
    quarter = (2, 2 * rows, points)
    half_field = (2, rows, length)
    (spectra,) = call(functools.partial(first_kernel, radix), [blocks], [])(
        planes, row_tw, row_forward_table
    )
    first_slow = jnp.where(own_first, slowness[0], other[0])
    last_slow = jnp.where(own_first, other[0], slowness[0])
    pairs = [
        (flat(f, b), flat((b // 2) % 2, (2 * f + b % 2) * per_plane + b // 4))
        for f in range(2)
        for b in range(ranks)
    ]
    near = lax.ppermute(first_slow, both, pairs)
    far = twin(near)

    col_wave = signed_wave(
        (jnp.arange(lanes, dtype=jnp.int32)[None, :] * col_radix)
        + jnp.arange(col_radix, dtype=jnp.int32)[:, None],
        length,
    )
    row_wave = signed_wave(jnp.arange(points, dtype=jnp.int32) * radix + residue, length)
    plane_waves = col_wave[:, :, None] ** 2 + row_wave[None, None, :] ** 2
    scale = 1.0 / (length * length)
    propagators = []
    for level in range(2):
        radicand = (omega * ref_slowness[level]) ** 2 - plane_waves
        vertical = jnp.sqrt(jnp.maximum(radicand, 0.0)) * depth_step
        damping = scale * jnp.exp(-jnp.sqrt(jnp.maximum(-radicand, 0.0)) * depth_step)
        propagators.append((damping * jnp.cos(vertical), sign * damping * jnp.sin(vertical)))

    columns = exchange(spectra)
    quarters = call(
        functools.partial(columns_to_quarters, col_radix), [quarter] * radix, [(radix,) + quarter]
    )(columns, *propagators[0], col_tw, col_forward_table, col_inverse_table)
    quarters = inner(quarters)

    slow = jnp.where(plane % 2 == 0, jnp.concatenate([near, far]), jnp.concatenate([far, near]))
    theta = omega * (slow - ref_slowness[0]) * depth_step
    *quarters, keep, send = call(
        functools.partial(middle_kernel, radix),
        [quarter] * radix + [half_field] * 2,
        [(radix,) + quarter, (2,) + half_field],
    )(*quarters, jnp.cos(theta), sign * jnp.sin(theta), row_tw, row_inverse_table, row_forward_table)
    quarters = inner(quarters)
    got = twin(send)
    (columns,) = call(
        functools.partial(quarters_to_columns, col_radix, radix), [blocks], [(radix,) + quarter]
    )(*quarters, *propagators[1], col_tw, col_forward_table, col_inverse_table)
    cells = exchange(columns)

    share = keep[0] * got[0] + keep[1] * got[1]
    first_image = 0.0
    for f in range(2):
        pairs = [
            (flat(c, (2 * f + h) * per_plane + y), flat(0, 2 * (c + 2 * y) + h))
            for c in range(2)
            for h in range(2)
            for y in range(per_plane)
        ]
        first_image = first_image + lax.ppermute(share, both, pairs)

    across = lax.ppermute(lax.dynamic_slice_in_dim(cells, (1 - core) * radix, radix), "depth", swap)
    theta = omegas[core] * (last_slow - ref_slowness[1]) * depth_step
    leaving, share = call(
        functools.partial(last_kernel, radix),
        [(1,) + planes.shape[1:], (rows, length)],
        [(2 * radix,) + blocks[1:]],
    )(cells, across, jnp.cos(theta), jnp.sin(theta), row_tw, row_inverse_table)
    last_image = share + lax.ppermute(share, "depth", [(0, 1)])
    return jnp.where(own_first, first_image, last_image)[None], leaving


def solution(mesh):
    in_specs = (P("groups", None, "row", None), P("depth", "row", None), P(), P())
    out_specs = (P(("groups", "depth"), "row", None), P(("groups", "depth"), None, "row", None))
    return jax.shard_map(shards, mesh=mesh, in_specs=in_specs, out_specs=out_specs, check_vma=False)
```

```python
import functools

import jax
import jax.numpy as jnp
import numpy as np
from jax import lax
from jax.experimental import pallas as pl
from jax.experimental.pallas import tpu as pltpu
from jax.sharding import PartitionSpec as P

omega_step = 0.05
depth_step = 1.0
lanes = 128


def pair(table):
    high = table.astype(jnp.bfloat16)
    low = (table - high.astype(np.float64)).astype(jnp.bfloat16)
    return np.stack([high, low])


def real_form(points):
    product = np.outer(np.arange(points), np.arange(points)) % points
    angle = 2.0 * np.pi / points * product
    c, s = np.cos(angle), np.sin(angle)
    return pair(np.block([[c, -s], [s, c]])), pair(np.block([[c, s], [-s, c]]))


def twiddles(length, radix):
    points = length // radix
    angle = 2.0 * np.pi / length * np.outer(np.arange(radix), np.arange(points))
    return np.stack([np.cos(angle), -np.sin(angle)], axis=1).astype(np.float32)


def split(x):
    high = x.astype(jnp.bfloat16)
    return high, (x - high.astype(jnp.float32)).astype(jnp.bfloat16)


def dot(a, b):
    return jnp.dot(a, b, preferred_element_type=jnp.float32)


def times_table(x, table):
    high, low = split(x)
    return dot(high, table[0]) + dot(low, table[0]) + dot(high, table[1])


def table_times(table, x):
    high, low = split(x)
    return dot(table[0], high) + dot(table[0], low) + dot(table[1], high)


def scaled(value, factor):
    if value is None or factor == 0.0:
        return None
    if factor == 1.0:
        return value
    return -value if factor == -1.0 else value * factor


def plus(a, b):
    if a is None:
        return b
    return a if b is None else a + b


def small_transform(parts, sign):
    radix = len(parts)
    if radix == 1:
        return parts
    if radix % 2 == 0:
        half = radix // 2
        even = small_transform(parts[0::2], sign)
        odd = small_transform(parts[1::2], sign)
        first, second = [], []
        for r in range(half):
            angle = sign * 2.0 * np.pi * r / radix
            c, s = float(np.round(np.cos(angle), 15)), float(np.round(np.sin(angle), 15))
            ore, oim = odd[r]
            tre = plus(scaled(ore, c), scaled(oim, -s))
            tim = plus(scaled(oim, c), scaled(ore, s))
            ere, eim = even[r]
            first.append((ere + tre, eim + tim))
            second.append((ere - tre, eim - tim))
        return first + second
    raise ValueError("radix")


def turn(part, factor, conjugate):
    re, im = part
    fre, fim = factor
    if conjugate:
        return re * fre + im * fim, im * fre - re * fim
    return re * fre - im * fim, im * fre + re * fim


def rows_of(parts):
    return jnp.concatenate([jnp.concatenate(part, axis=1) for part in parts], axis=0)


def row_forward(cells, tw, table, points):
    stacked = []
    for parts in cells:
        for r, part in enumerate(small_transform(parts, -1.0)):
            factor = (tw[r, 0:1], tw[r, 1:2])
            stacked.append(part if r == 0 else turn(part, factor, False))
    return times_table(rows_of(stacked), table)


def row_inverse(ref, tw, table, radix, planes):
    rows, points = ref.shape[2], ref.shape[3]
    count = planes * radix
    stacked = jnp.concatenate(
        [ref[:, 0].reshape(count * rows, points), ref[:, 1].reshape(count * rows, points)], axis=1
    )
    out = times_table(stacked, table)
    cells = []
    for p in range(planes):
        parts = []
        for r in range(radix):
            at = (p * radix + r) * rows
            part = (out[at : at + rows, :points], out[at : at + rows, points:])
            parts.append(part if r == 0 else turn(part, (tw[r, 0:1], tw[r, 1:2]), True))
        cells.append(small_transform(parts, 1.0))
    return cells


def store_blocks(out_ref, value, count, rows, points):
    out_ref[:, 0] = value[:, :points].reshape(count, rows, points)
    out_ref[:, 1] = value[:, points:].reshape(count, rows, points)


def half_transform(parts, odd):
    half = len(parts) // 2
    folded = []
    for m in range(half):
        (are, aim), (bre, bim) = parts[m], parts[m + half]
        if not odd:
            folded.append((are + bre, aim + bim))
            continue
        re, im = are - bre, aim - bim
        angle = -2.0 * np.pi * m / len(parts)
        c, s = float(np.round(np.cos(angle), 15)), float(np.round(np.sin(angle), 15))
        folded.append((plus(scaled(re, c), scaled(im, -s)), plus(scaled(im, c), scaled(re, s))))
    return small_transform(folded, -1.0)


def first_kernel(radix, planes_ref, tw, table, out_ref):
    count, _, rows, points = out_ref.shape
    for core in range(2):

        @pl.when(lax.axis_index("depth") == core)
        def _():
            stacked = []
            for p in range(planes_ref.shape[0] * 2):
                f, c = p // 2, 2 * (p % 2)
                parts = [
                    tuple(planes_ref[f, c + i, :, m * points : (m + 1) * points] for i in range(2))
                    for m in range(radix)
                ]
                for y, part in enumerate(half_transform(parts, core == 1)):
                    r = 2 * y + core
                    stacked.append(part if r == 0 else turn(part, (tw[r, 0:1], tw[r, 1:2]), False))
            value = times_table(rows_of(stacked), table)
            store_blocks(out_ref, value, count, rows, points)


def residue_of():
    per_plane = lax.axis_size("row") // 4
    return lax.axis_index("depth") + 2 * lax.rem(lax.axis_index("row"), per_plane)


def spread(held, out_refs):
    own = residue_of()
    for step, ref in enumerate(out_refs):
        ref[...] = held[own ^ step]


def collect(in_refs, held):
    own = residue_of()
    for step, ref in enumerate(in_refs):
        held[own ^ step] = ref[...]


def columns_to_quarters(col_radix, in_ref, hre, him, tw, forward, inverse, *rest):
    out_refs, held = rest[:-1], rest[-1]
    column_kernel(col_radix, in_ref, hre, him, tw, forward, inverse, held)
    spread(held, out_refs)


def quarters_to_columns(col_radix, radix, *refs):
    in_refs, refs = refs[:radix], refs[radix:]
    keep_ref, got_ref, hre, him, tw, forward, inverse, out_ref, share_ref, held = refs
    share_ref[...] = keep_ref[0] * got_ref[0] + keep_ref[1] * got_ref[1]
    collect(in_refs, held)
    column_kernel(col_radix, held, hre, him, tw, forward, inverse, out_ref)


def middle_kernel(radix, *refs):
    in_refs, (cos_ref, sin_ref, tw, inverse, forward) = refs[:radix], refs[radix : radix + 5]
    out_refs, (keep_ref, send_ref, held, field) = refs[radix + 5 : 2 * radix + 5], refs[2 * radix + 5 :]
    rows, points = held.shape[2], held.shape[3]
    collect(in_refs, held)
    (cells,) = row_inverse(held, tw, inverse, radix, 1)
    turned = []
    for m in range(radix):
        at = slice(m * points, (m + 1) * points)
        part = turn(cells[m], (cos_ref[:, at], sin_ref[:, at]), False)
        for half in range(2):
            for i in range(2):
                field[half, i, :, at] = part[i][half * rows // 2 : (half + 1) * rows // 2]
        turned.append(part)
    mine = lax.rem(lax.axis_index("row") // (lax.axis_size("row") // 4), 2)
    keep_ref[...] = field[mine]
    send_ref[...] = field[1 - mine]
    value = row_forward([turned], tw, forward, points)
    store_blocks(held, value, radix, rows, points)
    spread(held, out_refs)


def column_kernel(radix, in_ref, hre, him, tw, forward, inverse, out_ref):
    count, _, rows, width = in_ref.shape
    points = count * rows // radix
    per = points // rows
    out_rows = out_ref.shape[2]
    out_per = points // out_rows

    def block(m, part):
        return in_ref[m * per : (m + 1) * per, part].reshape(points, width)

    parts = small_transform([(block(m, 0), block(m, 1)) for m in range(radix)], -1.0)
    columns = []
    for r, part in enumerate(parts):
        if r > 0:
            factor = (tw[:, 2 * r : 2 * r + 1], tw[:, 2 * r + 1 : 2 * r + 2])
            part = turn(part, factor, False)
        columns.append(jnp.concatenate(part, axis=0))
    spectrum = table_times(forward, jnp.concatenate(columns, axis=1))
    columns = []
    for r in range(radix):
        at = slice(r * width, (r + 1) * width)
        part = turn((spectrum[:points, at], spectrum[points:, at]), (hre[r], him[r]), False)
        columns.append(jnp.concatenate(part, axis=0))
    back = table_times(inverse, jnp.concatenate(columns, axis=1))
    parts = []
    for r in range(radix):
        at = slice(r * width, (r + 1) * width)
        part = (back[:points, at], back[points:, at])
        if r > 0:
            factor = (tw[:, 2 * r : 2 * r + 1], tw[:, 2 * r + 1 : 2 * r + 2])
            part = turn(part, factor, True)
        parts.append(part)
    for m, (re, im) in enumerate(small_transform(parts, 1.0)):
        out_ref[m * out_per : (m + 1) * out_per, 0] = re.reshape(out_per, out_rows, width)
        out_ref[m * out_per : (m + 1) * out_per, 1] = im.reshape(out_per, out_rows, width)


def screened(cells, cos_ref, sin_ref, points):
    turned = ([], [])
    for m in range(len(cells[0])):
        at = slice(m * points, (m + 1) * points)
        factor = (cos_ref[:, at], sin_ref[:, at])
        turned[0].append(turn(cells[0][m], factor, True))
        turned[1].append(turn(cells[1][m], factor, False))
    return turned


def last_kernel(
    radix, in_ref, got_ref, first_ref, second_ref, cos_ref, sin_ref, tw, inverse, leaving_ref, image_ref, base_ref, held
):
    points = in_ref.shape[3]
    core = lax.axis_index("depth")
    per_plane = radix // 2
    for p in range(2):
        for y in range(per_plane):
            at = p * radix + 2 * y
            held[at + core] = in_ref[core * radix + p * per_plane + y]
            held[at + 1 - core] = got_ref[p * per_plane + y]
    cells = screened(row_inverse(held, tw, inverse, radix, 2), cos_ref, sin_ref, points)
    for m in range(radix):
        at = slice(m * points, (m + 1) * points)
        (sre, sim), (rre, rim) = cells[0][m], cells[1][m]
        leaving_ref[0, 0, :, at] = sre
        leaving_ref[0, 1, :, at] = sim
        leaving_ref[0, 2, :, at] = rre
        leaving_ref[0, 3, :, at] = rim
        image_ref[:, at] = sre * rre + sim * rim
    base_ref[...] = image_ref[...]

    @pl.when(core == 0)
    def _():
        base_ref[...] = first_ref[...] + second_ref[...]


def signed_wave(positions, length):
    signed = jnp.where(positions < length // 2, positions, positions - length)
    return 2.0 * jnp.pi / length * signed.astype(jnp.float32)


def call(kernel, out_shapes, scratch, args, held_args=True):
    vmem = pl.BlockSpec(memory_space=pltpu.VMEM)
    return pl.pallas_call(
        kernel,
        in_specs=[vmem] * len(args),
        out_specs=[vmem] * len(out_shapes),
        out_shape=[pltpu.VMEM(s, jnp.float32) for s in out_shapes],
        scratch_shapes=[pltpu.VMEM(s, jnp.float32) for s in scratch],
    )(*[pltpu.with_memory_space_constraint(a, pltpu.VMEM) if held_args else a for a in args])


def shards(planes, slowness, ref_slowness, freq_index):
    _, _, rows, length = planes.shape
    ranks = lax.axis_size("row")
    radix = ranks // 2
    per_plane = radix // 2
    points = length // radix
    col_radix = length // lanes
    row_index, core = lax.axis_index("row"), lax.axis_index("depth")
    own_first = core == 0

    row_forward_table, row_inverse_table = real_form(points)
    col_inverse_table, col_forward_table = real_form(lanes)
    row_tw = twiddles(length, radix)
    col_tw = twiddles(length, col_radix).transpose(2, 0, 1).reshape(lanes, 2 * col_radix)
    swap = [(0, 1), (1, 0)]
    both = ("depth", "row")

    def flat(c, r):
        return c * ranks + r

    def inner(arrays):
        got = [arrays[0]] + [None] * (radix - 1)
        for step in list(range(2, radix)) + [1]:
            pairs = [
                (flat(c, r), flat(c ^ (step & 1), r ^ (step >> 1))) for c in range(2) for r in range(ranks)
            ]
            got[step] = lax.ppermute(arrays[step], both, pairs)
        return got

    def exchange(x):
        return lax.all_to_all(x, "row", split_axis=0, concat_axis=0, tiled=True)

    def twin(x):
        return lax.ppermute(x, "row", [(r, r ^ per_plane) for r in range(ranks)])

    plane = row_index // per_plane
    residue = residue_of()
    sign = jnp.where(plane % 2 == 0, -1.0, 1.0)
    omegas = omega_step * freq_index.astype(jnp.float32)
    omega = omegas[plane // 2]

    other = lax.ppermute(slowness, "depth", swap)
    blocks = (ranks, 2, rows, points)
    quarter = (2, 2 * rows, points)
    half_field = (2, rows, length)
    (spectra,) = call(
        functools.partial(first_kernel, radix),
        [blocks],
        [],
        (planes, row_tw, row_forward_table),
        held_args=False,
    )
    first_slow = jnp.where(own_first, slowness[0], other[0])
    last_slow = jnp.where(own_first, other[0], slowness[0])
    pairs = [
        (flat(f, b), flat((b // 2) % 2, (2 * f + b % 2) * per_plane + b // 4))
        for f in range(2)
        for b in range(ranks)
    ]
    near = lax.ppermute(first_slow, both, pairs)
    col_wave = signed_wave(
        (jnp.arange(lanes, dtype=jnp.int32)[None, :] * col_radix)
        + jnp.arange(col_radix, dtype=jnp.int32)[:, None],
        length,
    )
    row_wave = signed_wave(jnp.arange(points, dtype=jnp.int32) * radix + residue, length)
    plane_waves = col_wave[:, :, None] ** 2 + row_wave[None, None, :] ** 2
    scale = 1.0 / (length * length)
    propagators = []
    for level in range(2):
        radicand = (omega * ref_slowness[level]) ** 2 - plane_waves
        vertical = jnp.sqrt(jnp.maximum(radicand, 0.0)) * depth_step
        damping = scale * jnp.exp(-jnp.sqrt(jnp.maximum(-radicand, 0.0)) * depth_step)
        propagators.append((damping * jnp.cos(vertical), sign * damping * jnp.sin(vertical)))

    near, propagators = lax.optimization_barrier((near, propagators))
    far = twin(near)
    columns = exchange(spectra)
    quarters = call(
        functools.partial(columns_to_quarters, col_radix),
        [quarter] * radix,
        [(radix,) + quarter],
        (columns, *propagators[0], col_tw, col_forward_table, col_inverse_table),
    )
    quarters = inner(quarters)

    slow = jnp.where(plane % 2 == 0, jnp.concatenate([near, far]), jnp.concatenate([far, near]))
    theta = omega * (slow - ref_slowness[0]) * depth_step
    *quarters, keep, send = call(
        functools.partial(middle_kernel, radix),
        [quarter] * radix + [half_field] * 2,
        [(radix,) + quarter, (2,) + half_field],
        (*quarters, jnp.cos(theta), sign * jnp.sin(theta), row_tw, row_inverse_table, row_forward_table),
    )
    quarters = inner(quarters)
    got = twin(send)
    columns, share = call(
        functools.partial(quarters_to_columns, col_radix, radix),
        [blocks, (rows, length)],
        [(radix,) + quarter],
        (*quarters, keep, got, *propagators[1], col_tw, col_forward_table, col_inverse_table),
    )
    cells = exchange(columns)

    shares = []
    for f in range(2):
        pairs = [
            (flat(c, (2 * f + h) * per_plane + y), flat(0, 2 * (c + 2 * y) + h))
            for c in range(2)
            for h in range(2)
            for y in range(per_plane)
        ]
        shares.append(lax.ppermute(share, both, pairs))

    cells, *shares = lax.optimization_barrier((cells, *shares))
    across = lax.ppermute(lax.dynamic_slice_in_dim(cells, (1 - core) * radix, radix), "depth", swap)
    theta = omegas[core] * (last_slow - ref_slowness[1]) * depth_step
    leaving, share, base = call(
        functools.partial(last_kernel, radix),
        [(1,) + planes.shape[1:], (rows, length), (rows, length)],
        [(2 * radix,) + blocks[1:]],
        (cells, across, *shares, jnp.cos(theta), jnp.sin(theta), row_tw, row_inverse_table),
    )
    image = base + lax.ppermute(share, "depth", [(0, 1)])
    return image[None], leaving


def solution(mesh):
    in_specs = (P("groups", None, "row", None), P("depth", "row", None), P(), P())
    out_specs = (P(("groups", "depth"), "row", None), P(("groups", "depth"), None, "row", None))
    return jax.shard_map(shards, mesh=mesh, in_specs=in_specs, out_specs=out_specs, check_vma=False)
```

```python
import functools

import jax
import jax.numpy as jnp
import numpy as np
from jax import lax
from jax.experimental import pallas as pl
from jax.experimental.pallas import tpu as pltpu
from jax.sharding import PartitionSpec as P


omega_step = 0.05
depth_step = 1.0
lanes = 128


def pair(table):
    high = table.astype(jnp.bfloat16)
    low = (table - high.astype(np.float64)).astype(jnp.bfloat16)
    return np.stack([high, low])


def real_form(points):
    product = np.outer(np.arange(points), np.arange(points)) % points
    angle = 2.0 * np.pi / points * product
    c, s = np.cos(angle), np.sin(angle)
    return pair(np.block([[c, -s], [s, c]])), pair(np.block([[c, s], [-s, c]]))


def twiddles(length, radix):
    points = length // radix
    angle = 2.0 * np.pi / length * np.outer(np.arange(radix), np.arange(points))
    return np.stack([np.cos(angle), -np.sin(angle)], axis=1).astype(np.float32)


def split(x):
    high = x.astype(jnp.bfloat16)
    return high, (x - high.astype(jnp.float32)).astype(jnp.bfloat16)


def dot(a, b):
    return jnp.dot(a, b, preferred_element_type=jnp.float32)


def times_table(x, table):
    high, low = split(x)
    return dot(high, table[0]) + dot(low, table[0]) + dot(high, table[1])


def table_times(table, x):
    high, low = split(x)
    return dot(table[0], high) + dot(table[0], low) + dot(table[1], high)


def scaled(value, factor):
    if value is None or factor == 0.0:
        return None
    if factor == 1.0:
        return value
    return -value if factor == -1.0 else value * factor


def plus(a, b):
    if a is None:
        return b
    return a if b is None else a + b


def small_transform(parts, sign):
    radix = len(parts)
    if radix == 1:
        return parts
    if radix % 2 == 0:
        half = radix // 2
        even = small_transform(parts[0::2], sign)
        odd = small_transform(parts[1::2], sign)
        first, second = [], []
        for r in range(half):
            angle = sign * 2.0 * np.pi * r / radix
            c, s = float(np.round(np.cos(angle), 15)), float(np.round(np.sin(angle), 15))
            ore, oim = odd[r]
            tre = plus(scaled(ore, c), scaled(oim, -s))
            tim = plus(scaled(oim, c), scaled(ore, s))
            ere, eim = even[r]
            first.append((ere + tre, eim + tim))
            second.append((ere - tre, eim - tim))
        return first + second
    raise ValueError("radix")


def turn(part, factor, conjugate):
    re, im = part
    fre, fim = factor
    if conjugate:
        return re * fre + im * fim, im * fre - re * fim
    return re * fre - im * fim, im * fre + re * fim


def rows_of(parts):
    return jnp.concatenate([jnp.concatenate(part, axis=1) for part in parts], axis=0)


def row_forward(cells, tw, table):
    stacked = []
    for parts in cells:
        for r, part in enumerate(small_transform(parts, -1.0)):
            factor = (tw[r, 0:1], tw[r, 1:2])
            stacked.append(part if r == 0 else turn(part, factor, False))
    return times_table(rows_of(stacked), table)


def row_inverse(ref, tw, table, radix, planes):
    rows, points = ref.shape[2], ref.shape[3]
    count = planes * radix
    stacked = jnp.concatenate(
        [ref[:, 0].reshape(count * rows, points), ref[:, 1].reshape(count * rows, points)], axis=1
    )
    out = times_table(stacked, table)
    cells = []
    for p in range(planes):
        parts = []
        for r in range(radix):
            at = (p * radix + r) * rows
            part = (out[at : at + rows, :points], out[at : at + rows, points:])
            parts.append(part if r == 0 else turn(part, (tw[r, 0:1], tw[r, 1:2]), True))
        cells.append(small_transform(parts, 1.0))
    return cells


def store_blocks(out_ref, value, count, rows, points):
    out_ref[:, 0] = value[:, :points].reshape(count, rows, points)
    out_ref[:, 1] = value[:, points:].reshape(count, rows, points)


def half_transform(parts, odd):
    half = len(parts) // 2
    folded = []
    for m in range(half):
        (are, aim), (bre, bim) = parts[m], parts[m + half]
        if not odd:
            folded.append((are + bre, aim + bim))
            continue
        re, im = are - bre, aim - bim
        angle = -2.0 * np.pi * m / len(parts)
        c, s = float(np.round(np.cos(angle), 15)), float(np.round(np.sin(angle), 15))
        folded.append((plus(scaled(re, c), scaled(im, -s)), plus(scaled(im, c), scaled(re, s))))
    return small_transform(folded, -1.0)


def first_kernel(radix, planes_ref, tw, table, out_ref):
    count, _, rows, points = out_ref.shape
    for core in range(2):

        @pl.when(lax.axis_index("depth") == core)
        def _():
            stacked = []
            for p in range(planes_ref.shape[0] * 2):
                f, c = p // 2, 2 * (p % 2)
                parts = [
                    tuple(planes_ref[f, c + i, :, m * points : (m + 1) * points] for i in range(2))
                    for m in range(radix)
                ]
                for y, part in enumerate(half_transform(parts, core == 1)):
                    r = 2 * y + core
                    stacked.append(part if r == 0 else turn(part, (tw[r, 0:1], tw[r, 1:2]), False))
            value = times_table(rows_of(stacked), table)
            store_blocks(out_ref, value, count, rows, points)


def residue_of():
    per_plane = lax.axis_size("row") // 4
    return lax.axis_index("depth") + 2 * lax.rem(lax.axis_index("row"), per_plane)


def spread(held, out_refs):
    own = residue_of()
    for step, ref in enumerate(out_refs):
        ref[...] = held[own ^ step]


def collect(in_refs, held):
    own = residue_of()
    for step, ref in enumerate(in_refs):
        held[own ^ step] = ref[...]


def quarter_place(block, ranks):
    per_plane = ranks // 4
    step, place = block // per_plane, block % per_plane
    return step // 2 + 2 * place, step % 2


class Blocks:
    def __init__(self, ref, ranks, rows):
        self.ref, self.ranks, self.rows = ref, ranks, rows

    def at(self, block, part):
        return block, part


class Quarters(Blocks):
    def at(self, block, part):
        quarter, half = quarter_place(block, self.ranks)
        return quarter, part, slice(half * self.rows, (half + 1) * self.rows)


def columns_to_quarters(col_radix, in_ref, hre, him, tw, forward, inverse, *rest):
    out_refs, held = rest[:-1], rest[-1]
    ranks, rows = in_ref.shape[0], in_ref.shape[2]
    source, target = Blocks(in_ref, ranks, rows), Quarters(held, ranks, rows)
    column_kernel(col_radix, source, hre, him, tw, forward, inverse, target)
    spread(held, out_refs)


def quarters_to_columns(col_radix, radix, *refs):
    in_refs, (hre, him, tw, forward, inverse, out_ref, held) = refs[:radix], refs[radix:]
    ranks, rows = out_ref.shape[0], out_ref.shape[2]
    collect(in_refs, held)
    source, target = Quarters(held, ranks, rows), Blocks(out_ref, ranks, rows)
    column_kernel(col_radix, source, hre, him, tw, forward, inverse, target)


def middle_kernel(radix, *refs):
    in_refs, refs = refs[:radix], refs[radix:]
    (near_cos, near_sin, far_cos, far_sin, tw, inverse, forward), refs = refs[:7], refs[7:]
    out_refs, (keep_ref, send_ref, held, field, screen) = refs[:radix], refs[radix:]
    rows, points = held.shape[2], held.shape[3]
    mine = lax.rem(lax.axis_index("row") // (lax.axis_size("row") // 4), 2)
    for half, pair_refs in ((mine, (near_cos, near_sin)), (1 - mine, (far_cos, far_sin))):
        for i, ref in enumerate(pair_refs):
            screen[i, half] = ref[...]
    collect(in_refs, held)
    (cells,) = row_inverse(held, tw, inverse, radix, 1)
    turned = []
    for m in range(radix):
        at = slice(m * points, (m + 1) * points)
        factor = [screen[i, :, :, at].reshape(rows, points) for i in range(2)]
        part = turn(cells[m], factor, False)
        for half in range(2):
            for i in range(2):
                field[half, i, :, at] = part[i][half * rows // 2 : (half + 1) * rows // 2]
        turned.append(part)
    keep_ref[...] = field[mine]
    send_ref[...] = field[1 - mine]
    value = row_forward([turned], tw, forward)
    store_blocks(held, value, radix, rows, points)
    spread(held, out_refs)


def column_kernel(radix, source, hre, him, tw, forward, inverse, target):
    points, width = hre.shape[1], hre.shape[2]
    rows = source.rows
    per = points // rows

    def block(m, part):
        pieces = [source.ref[source.at(m * per + i, part)] for i in range(per)]
        return jnp.concatenate(pieces, axis=0)

    parts = small_transform([(block(m, 0), block(m, 1)) for m in range(radix)], -1.0)
    columns = []
    for r, part in enumerate(parts):
        if r > 0:
            factor = (tw[:, 2 * r : 2 * r + 1], tw[:, 2 * r + 1 : 2 * r + 2])
            part = turn(part, factor, False)
        columns.append(jnp.concatenate(part, axis=0))
    spectrum = table_times(forward, jnp.concatenate(columns, axis=1))
    columns = []
    for r in range(radix):
        at = slice(r * width, (r + 1) * width)
        part = turn((spectrum[:points, at], spectrum[points:, at]), (hre[r], him[r]), False)
        columns.append(jnp.concatenate(part, axis=0))
    back = table_times(inverse, jnp.concatenate(columns, axis=1))
    parts = []
    for r in range(radix):
        at = slice(r * width, (r + 1) * width)
        part = (back[:points, at], back[points:, at])
        if r > 0:
            factor = (tw[:, 2 * r : 2 * r + 1], tw[:, 2 * r + 1 : 2 * r + 2])
            part = turn(part, factor, True)
        parts.append(part)
    for m, (re, im) in enumerate(small_transform(parts, 1.0)):
        for i in range(per):
            at = slice(i * rows, (i + 1) * rows)
            target.ref[target.at(m * per + i, 0)] = re[at]
            target.ref[target.at(m * per + i, 1)] = im[at]


def screened(cells, cos_ref, sin_ref, points):
    turned = ([], [])
    for m in range(len(cells[0])):
        at = slice(m * points, (m + 1) * points)
        factor = (cos_ref[:, at], sin_ref[:, at])
        turned[0].append(turn(cells[0][m], factor, True))
        turned[1].append(turn(cells[1][m], factor, False))
    return turned


def last_kernel(
    radix, in_ref, got_ref, cos_ref, sin_ref, tw, inverse, leaving_ref, image_ref, base_ref, held
):
    points = in_ref.shape[3]
    core = lax.axis_index("depth")
    per_plane = radix // 2
    for p in range(2):
        for y in range(per_plane):
            at = p * radix + 2 * y
            held[at + core] = in_ref[core * radix + p * per_plane + y]
            held[at + 1 - core] = got_ref[p * per_plane + y]
    cells = screened(row_inverse(held, tw, inverse, radix, 2), cos_ref, sin_ref, points)
    for m in range(radix):
        at = slice(m * points, (m + 1) * points)
        (sre, sim), (rre, rim) = cells[0][m], cells[1][m]
        leaving_ref[0, 0, :, at] = sre
        leaving_ref[0, 1, :, at] = sim
        leaving_ref[0, 2, :, at] = rre
        leaving_ref[0, 3, :, at] = rim
        image_ref[:, at] = sre * rre + sim * rim
    base_ref[...] = jnp.where(core == 0, 0.0, image_ref[...])


def signed_wave(positions, length):
    signed = jnp.where(positions < length // 2, positions, positions - length)
    return 2.0 * jnp.pi / length * signed.astype(jnp.float32)


def call(kernel, out_shapes, scratch, args, held_args=True):
    vmem = pl.BlockSpec(memory_space=pltpu.VMEM)
    return pl.pallas_call(
        kernel,
        in_specs=[vmem] * len(args),
        out_specs=[vmem] * len(out_shapes),
        out_shape=[pltpu.VMEM(s, jnp.float32) for s in out_shapes],
        scratch_shapes=[pltpu.VMEM(s, jnp.float32) for s in scratch],
    )(*[pltpu.with_memory_space_constraint(a, pltpu.VMEM) if held_args else a for a in args])


def shards(planes, slowness, ref_slowness, freq_index):
    _, _, rows, length = planes.shape
    ranks = lax.axis_size("row")
    radix = ranks // 2
    per_plane = radix // 2
    points = length // radix
    col_radix = length // lanes
    row_index, core = lax.axis_index("row"), lax.axis_index("depth")
    own_first = core == 0

    row_forward_table, row_inverse_table = real_form(points)
    col_inverse_table, col_forward_table = real_form(lanes)
    row_tw = twiddles(length, radix)
    col_tw = twiddles(length, col_radix).transpose(2, 0, 1).reshape(lanes, 2 * col_radix)
    swap = [(0, 1), (1, 0)]
    both = ("depth", "row")

    def flat(c, r):
        return c * ranks + r

    def inner(arrays):
        got = [arrays[0]] + [None] * (radix - 1)
        for step in list(range(2, radix)) + [1]:
            pairs = [
                (flat(c, r), flat(c ^ (step & 1), r ^ (step >> 1))) for c in range(2) for r in range(ranks)
            ]
            got[step] = lax.ppermute(arrays[step], both, pairs)
        return got

    def exchange(x):
        return lax.all_to_all(x, "row", split_axis=0, concat_axis=0, tiled=True)

    def twin(x):
        return lax.ppermute(x, "row", [(r, r ^ per_plane) for r in range(ranks)])

    plane = row_index // per_plane
    residue = residue_of()
    sign = jnp.where(plane % 2 == 0, -1.0, 1.0)
    omegas = omega_step * freq_index.astype(jnp.float32)
    omega = omegas[plane // 2]

    other = lax.ppermute(slowness, "depth", swap)
    blocks = (ranks, 2, rows, points)
    quarter = (2, 2 * rows, points)
    half_field = (2, rows, length)
    (spectra,) = call(
        functools.partial(first_kernel, radix),
        [blocks],
        [],
        (planes, row_tw, row_forward_table),
        held_args=False,
    )
    first_slow = jnp.where(own_first, slowness[0], other[0])
    last_slow = jnp.where(own_first, other[0], slowness[0])

    col_wave = signed_wave(
        (jnp.arange(lanes, dtype=jnp.int32)[None, :] * col_radix)
        + jnp.arange(col_radix, dtype=jnp.int32)[:, None],
        length,
    )
    row_wave = signed_wave(jnp.arange(points, dtype=jnp.int32) * radix + residue, length)
    plane_waves = col_wave[:, :, None] ** 2 + row_wave[None, None, :] ** 2
    scale = 1.0 / (length * length)

    def propagator(slow_ref):
        radicand = (omega * slow_ref) ** 2 - plane_waves
        vertical = jnp.sqrt(jnp.maximum(radicand, 0.0)) * depth_step
        damping = scale * jnp.exp(-jnp.sqrt(jnp.maximum(-radicand, 0.0)) * depth_step)
        return damping * jnp.cos(vertical), sign * damping * jnp.sin(vertical)

    def screen(slow, slow_ref, frequency, turned):
        theta = frequency * (slow - slow_ref) * depth_step
        return jnp.cos(theta), turned * jnp.sin(theta)

    first_propagator = propagator(ref_slowness[0])
    columns = exchange(spectra)
    columns, first_slow = lax.optimization_barrier((columns, first_slow))
    pairs = []
    for f in range(2):
        for b in range(ranks):
            (quarter_at, half) = quarter_place(b, ranks)
            pairs.append(
                (flat(f, b), flat(quarter_at % 2, (2 * f + half) * per_plane + quarter_at // 2))
            )
    near = lax.ppermute(first_slow, both, pairs)
    far = twin(near)
    quarters = call(
        functools.partial(columns_to_quarters, col_radix),
        [quarter] * radix,
        [(radix,) + quarter],
        (columns, *first_propagator, col_tw, col_forward_table, col_inverse_table),
    )
    quarters = inner(quarters)

    screens = screen(near, ref_slowness[0], omega, sign) + screen(far, ref_slowness[0], omega, sign)
    *quarters, keep, send = call(
        functools.partial(middle_kernel, radix),
        [quarter] * radix + [half_field] * 2,
        [(radix,) + quarter, (2,) + half_field, (2,) + half_field],
        (*quarters, *screens, row_tw, row_inverse_table, row_forward_table),
    )
    quarters = inner(quarters)
    got = twin(send)
    keep, last_ref = lax.optimization_barrier((keep, ref_slowness[1]))
    (columns,) = call(
        functools.partial(quarters_to_columns, col_radix, radix),
        [blocks],
        [(radix,) + quarter],
        (*quarters, *propagator(last_ref), col_tw, col_forward_table, col_inverse_table),
    )
    columns, last_slow = lax.optimization_barrier((columns, last_slow))
    cells = exchange(columns)
    share = keep[0] * got[0] + keep[1] * got[1]
    last_screen = screen(last_slow, ref_slowness[1], omegas[core], 1.0)

    cells, share = lax.optimization_barrier((cells, share))
    across = lax.ppermute(
        lax.dynamic_slice_in_dim(cells, (1 - core) * radix, radix), "depth", swap
    )
    image = 0.0
    for f in range(2):
        pairs = []
        for b in range(ranks):
            (quarter_at, half) = quarter_place(b, ranks)
            source = flat(quarter_at % 2, (2 * f + half) * per_plane + quarter_at // 2)
            pairs.append((source, flat(0, b)))
        image = image + lax.ppermute(share, both, pairs)
    leaving, share, base = call(
        functools.partial(last_kernel, radix),
        [(1,) + planes.shape[1:], (rows, length), (rows, length)],
        [(2 * radix,) + blocks[1:]],
        (
            cells,
            across,
            *last_screen,
            row_tw,
            row_inverse_table,
        ),
    )
    image = image + base + lax.ppermute(share, "depth", [(0, 1)])
    return image[None], leaving


def solution(mesh):
    in_specs = (P("groups", None, "row", None), P("depth", "row", None), P(), P())
    out_specs = (P(("groups", "depth"), "row", None), P(("groups", "depth"), None, "row", None))
    return jax.shard_map(shards, mesh=mesh, in_specs=in_specs, out_specs=out_specs, check_vma=False)
```

```python
import functools

import jax
import jax.numpy as jnp
import numpy as np
from jax import lax
from jax.experimental import pallas as pl
from jax.experimental.pallas import tpu as pltpu
from jax.sharding import PartitionSpec as P


omega_step = 0.05
depth_step = 1.0
lanes = 128
kernel_vmem = 24 << 20


def pair(table):
    high = table.astype(jnp.bfloat16)
    low = (table - high.astype(np.float64)).astype(jnp.bfloat16)
    return np.stack([high, low])


def real_form(points):
    product = np.outer(np.arange(points), np.arange(points)) % points
    angle = 2.0 * np.pi / points * product
    c, s = np.cos(angle), np.sin(angle)
    return pair(np.block([[c, -s], [s, c]])), pair(np.block([[c, s], [-s, c]]))


def twiddles(length, radix):
    points = length // radix
    angle = 2.0 * np.pi / length * np.outer(np.arange(radix), np.arange(points))
    return np.stack([np.cos(angle), -np.sin(angle)], axis=1).astype(np.float32)


def split(x):
    high = x.astype(jnp.bfloat16)
    return high, (x - high.astype(jnp.float32)).astype(jnp.bfloat16)


def dot(a, b):
    return jnp.dot(a, b, preferred_element_type=jnp.float32)


def times_table(x, table):
    high, low = split(x)
    return dot(high, table[0]) + dot(low, table[0]) + dot(high, table[1])


def table_times(table, x):
    high, low = split(x)
    return dot(table[0], high) + dot(table[0], low) + dot(table[1], high)


def scaled(value, factor):
    if value is None or factor == 0.0:
        return None
    if factor == 1.0:
        return value
    return -value if factor == -1.0 else value * factor


def plus(a, b):
    if a is None:
        return b
    return a if b is None else a + b


def small_transform(parts, sign):
    radix = len(parts)
    if radix == 1:
        return parts
    if radix % 2 == 0:
        half = radix // 2
        even = small_transform(parts[0::2], sign)
        odd = small_transform(parts[1::2], sign)
        first, second = [], []
        for r in range(half):
            angle = sign * 2.0 * np.pi * r / radix
            c, s = float(np.round(np.cos(angle), 15)), float(np.round(np.sin(angle), 15))
            ore, oim = odd[r]
            tre = plus(scaled(ore, c), scaled(oim, -s))
            tim = plus(scaled(oim, c), scaled(ore, s))
            ere, eim = even[r]
            first.append((ere + tre, eim + tim))
            second.append((ere - tre, eim - tim))
        return first + second
    raise ValueError("radix")


def turn(part, factor, conjugate):
    re, im = part
    fre, fim = factor
    if conjugate:
        return re * fre + im * fim, im * fre - re * fim
    return re * fre - im * fim, im * fre + re * fim


def rows_of(parts):
    return jnp.concatenate([jnp.concatenate(part, axis=1) for part in parts], axis=0)


def row_forward(cells, tw, table):
    stacked = []
    for parts in cells:
        for r, part in enumerate(small_transform(parts, -1.0)):
            factor = (tw[r, 0:1], tw[r, 1:2])
            stacked.append(part if r == 0 else turn(part, factor, False))
    return times_table(rows_of(stacked), table)


def row_inverse(ref, tw, table, radix, planes):
    rows, points = ref.shape[2], ref.shape[3]
    count = planes * radix
    stacked = jnp.concatenate(
        [ref[:, 0].reshape(count * rows, points), ref[:, 1].reshape(count * rows, points)], axis=1
    )
    out = times_table(stacked, table)
    cells = []
    for p in range(planes):
        parts = []
        for r in range(radix):
            at = (p * radix + r) * rows
            part = (out[at : at + rows, :points], out[at : at + rows, points:])
            parts.append(part if r == 0 else turn(part, (tw[r, 0:1], tw[r, 1:2]), True))
        cells.append(small_transform(parts, 1.0))
    return cells


def store_blocks(out_ref, value, count, rows, points):
    out_ref[:, 0] = value[:, :points].reshape(count, rows, points)
    out_ref[:, 1] = value[:, points:].reshape(count, rows, points)


def first_kernel(radix, core_ref, planes_ref, tw, table, out_ref):
    count, _, rows, points = out_ref.shape
    parts = [
        tuple(planes_ref[0, i, :, m * points : (m + 1) * points] for i in range(2)) for m in range(radix)
    ]
    value = row_forward([parts], tw, table)
    store_blocks(out_ref, value, count, rows, points)


def residue_of():
    return lax.rem(lax.axis_index("row"), lax.axis_size("row") // 2)


def frequency_of():
    return lax.axis_index("row") // (lax.axis_size("row") // 2)


def spread(held, out_refs):
    own = residue_of()
    for step, ref in enumerate(out_refs):
        ref[...] = held[own ^ step]


def collect(in_refs, held):
    own = residue_of()
    for step, ref in enumerate(in_refs):
        held[own ^ step] = ref[...]


def quarter_place(block, ranks):
    return block % (ranks // 2), block // (ranks // 2)


class Blocks:
    def __init__(self, ref, ranks, rows):
        self.ref, self.ranks, self.rows = ref, ranks, rows

    def at(self, block, part):
        return block, part


class Quarters(Blocks):
    def at(self, block, part):
        quarter, half = quarter_place(block, self.ranks)
        return quarter, part, slice(half * self.rows, (half + 1) * self.rows)


def columns_to_quarters(col_radix, in_ref, hre, him, tw, forward, inverse, *rest):
    out_refs, held = rest[:-1], rest[-1]
    ranks, rows = in_ref.shape[0], in_ref.shape[2]
    source, target = Blocks(in_ref, ranks, rows), Quarters(held, ranks, rows)
    column_kernel(col_radix, source, hre, him, tw, forward, inverse, target)
    spread(held, out_refs)


def quarters_to_columns(col_radix, radix, *refs):
    in_refs, (hre, him, tw, forward, inverse, out_ref, held) = refs[:radix], refs[radix:]
    ranks, rows = out_ref.shape[0], out_ref.shape[2]
    collect(in_refs, held)
    source, target = Quarters(held, ranks, rows), Blocks(out_ref, ranks, rows)
    column_kernel(col_radix, source, hre, him, tw, forward, inverse, target)


def middle_kernel(radix, *refs):
    in_refs, refs = refs[:radix], refs[radix:]
    (own_cos, own_sin, far_cos, far_sin, tw, inverse, forward), refs = refs[:7], refs[7:]
    out_refs, (keep_ref, send_ref, held, field, screen) = refs[:radix], refs[radix:]
    rows, points = held.shape[2], held.shape[3]
    mine = frequency_of()
    for half, pair_refs in ((mine, (own_cos, own_sin)), (1 - mine, (far_cos, far_sin))):
        for i, ref in enumerate(pair_refs):
            screen[i, half] = ref[...]
    collect(in_refs, held)
    (cells,) = row_inverse(held, tw, inverse, radix, 1)
    turned = []
    for m in range(radix):
        at = slice(m * points, (m + 1) * points)
        factor = [screen[i, :, :, at].reshape(rows, points) for i in range(2)]
        part = turn(cells[m], factor, False)
        for half in range(2):
            for i in range(2):
                field[half, i, :, at] = part[i][half * rows // 2 : (half + 1) * rows // 2]
        turned.append(part)
    kept = mine ^ lax.axis_index("depth")
    keep_ref[...] = field[kept]
    send_ref[...] = field[1 - kept]
    value = row_forward([turned], tw, forward)
    store_blocks(held, value, radix, rows, points)
    spread(held, out_refs)


def column_kernel(radix, source, hre, him, tw, forward, inverse, target):
    points, width = hre.shape[1], hre.shape[2]
    rows = source.rows
    per = points // rows

    def block(m, part):
        pieces = [source.ref[source.at(m * per + i, part)] for i in range(per)]
        return jnp.concatenate(pieces, axis=0)

    parts = small_transform([(block(m, 0), block(m, 1)) for m in range(radix)], -1.0)
    columns = []
    for r, part in enumerate(parts):
        if r > 0:
            factor = (tw[:, 2 * r : 2 * r + 1], tw[:, 2 * r + 1 : 2 * r + 2])
            part = turn(part, factor, False)
        columns.append(jnp.concatenate(part, axis=0))
    spectrum = table_times(forward, jnp.concatenate(columns, axis=1))
    columns = []
    for r in range(radix):
        at = slice(r * width, (r + 1) * width)
        part = turn((spectrum[:points, at], spectrum[points:, at]), (hre[r], him[r]), False)
        columns.append(jnp.concatenate(part, axis=0))
    back = table_times(inverse, jnp.concatenate(columns, axis=1))
    parts = []
    for r in range(radix):
        at = slice(r * width, (r + 1) * width)
        part = (back[:points, at], back[points:, at])
        if r > 0:
            factor = (tw[:, 2 * r : 2 * r + 1], tw[:, 2 * r + 1 : 2 * r + 2])
            part = turn(part, factor, True)
        parts.append(part)
    for m, (re, im) in enumerate(small_transform(parts, 1.0)):
        for i in range(per):
            at = slice(i * rows, (i + 1) * rows)
            target.ref[target.at(m * per + i, 0)] = re[at]
            target.ref[target.at(m * per + i, 1)] = im[at]


def middle_kernel(radix, *refs):
    in_refs, refs = refs[:radix], refs[radix:]
    (own_cos, own_sin, far_cos, far_sin, tw, inverse, forward), refs = refs[:7], refs[7:]
    out_refs, (keep_ref, send_ref, held, field, screen) = refs[:radix], refs[radix:]
    rows, points = held.shape[2], held.shape[3]
    mine = frequency_of()
    for half, pair_refs in ((mine, (own_cos, own_sin)), (1 - mine, (far_cos, far_sin))):
        for i, ref in enumerate(pair_refs):
            screen[i, half] = ref[...]
    collect(in_refs, held)
    (cells,) = row_inverse(held, tw, inverse, radix, 1)
    turned = []
    for m in range(radix):
        at = slice(m * points, (m + 1) * points)
        factor = [screen[i, :, :, at].reshape(rows, points) for i in range(2)]
        part = turn(cells[m], factor, False)
        for half in range(2):
            for i in range(2):
                field[half, i, :, at] = part[i][half * rows // 2 : (half + 1) * rows // 2]
        turned.append(part)
    kept = mine ^ lax.axis_index("depth")
    keep_ref[...] = field[kept]
    send_ref[...] = field[1 - kept]
    value = row_forward([turned], tw, forward)
    store_blocks(held, value, radix, rows, points)
    spread(held, out_refs)


def column_kernel(radix, source, hre, him, tw, forward, inverse, target):
    points, width = hre.shape[1], hre.shape[2]
    rows = source.rows
    per = points // rows

    def block(m, part):
        pieces = [source.ref[source.at(m * per + i, part)] for i in range(per)]
        return jnp.concatenate(pieces, axis=0)

    parts = small_transform([(block(m, 0), block(m, 1)) for m in range(radix)], -1.0)
    columns = []
    for r, part in enumerate(parts):
        if r > 0:
            factor = (tw[:, 2 * r : 2 * r + 1], tw[:, 2 * r + 1 : 2 * r + 2])
            part = turn(part, factor, False)
        columns.append(jnp.concatenate(part, axis=0))
    spectrum = table_times(forward, jnp.concatenate(columns, axis=1))
    columns = []
    for r in range(radix):
        at = slice(r * width, (r + 1) * width)
        part = turn((spectrum[:points, at], spectrum[points:, at]), (hre[r], him[r]), False)
        columns.append(jnp.concatenate(part, axis=0))
    back = table_times(inverse, jnp.concatenate(columns, axis=1))
    parts = []
    for r in range(radix):
        at = slice(r * width, (r + 1) * width)
        part = (back[:points, at], back[points:, at])
        if r > 0:
            factor = (tw[:, 2 * r : 2 * r + 1], tw[:, 2 * r + 1 : 2 * r + 2])
            part = turn(part, factor, True)
        parts.append(part)
    for m, (re, im) in enumerate(small_transform(parts, 1.0)):
        for i in range(per):
            at = slice(i * rows, (i + 1) * rows)
            target.ref[target.at(m * per + i, 0)] = re[at]
            target.ref[target.at(m * per + i, 1)] = im[at]


def last_kernel(radix, in_ref, *refs):
    screens, (tw, inverse, out_ref) = refs[:4], refs[4:]
    points = in_ref.shape[3]
    for f, parts in enumerate(row_inverse(in_ref, tw, inverse, radix, 2)):
        for m, part in enumerate(parts):
            at = slice(m * points, (m + 1) * points)
            factor = (screens[2 * f][:, at], screens[2 * f + 1][:, at])
            re, im = turn(part, factor, False)
            out_ref[f, 0, :, at] = re
            out_ref[f, 1, :, at] = im


def output_kernel(own_ref, got_ref, share_ref, more_ref, image_ref, leaving_ref):
    for core, (source, receiver) in enumerate(((own_ref, got_ref), (got_ref, own_ref))):

        @pl.when(lax.axis_index("depth") == core)
        def _():
            leaving_ref[0, 0:2] = source[core]
            leaving_ref[0, 2:4] = receiver[core]
            if core == 0:
                image_ref[0] = share_ref[...] + more_ref[...]
            else:
                terms = [source[f, i] * receiver[f, i] for f in range(2) for i in range(2)]
                image_ref[0] = (terms[0] + terms[1]) + (terms[2] + terms[3])


def signed_wave(positions, length):
    signed = jnp.where(positions < length // 2, positions, positions - length)
    return 2.0 * jnp.pi / length * signed.astype(jnp.float32)


def call(kernel, out_shapes, scratch, args, held=True):
    vmem = pl.BlockSpec(memory_space=pltpu.VMEM)
    shape = pltpu.VMEM if held else jax.ShapeDtypeStruct
    return pl.pallas_call(
        kernel,
        in_specs=[vmem] * len(args),
        out_specs=[vmem] * len(out_shapes),
        out_shape=[shape(s, jnp.float32) for s in out_shapes],
        scratch_shapes=[pltpu.VMEM(s, jnp.float32) for s in scratch],
        compiler_params=pltpu.CompilerParams(vmem_limit_bytes=kernel_vmem),
    )(*[pltpu.with_memory_space_constraint(a, pltpu.VMEM) for a in args])


def shards(planes, slowness, ref_slowness, freq_index):
    freqs, _, rows, length = planes.shape
    ranks = lax.axis_size("row")
    radix = ranks // 2
    points = length // radix
    col_radix = length // lanes
    core = lax.axis_index("depth")

    row_forward_table, row_inverse_table = real_form(points)
    col_inverse_table, col_forward_table = real_form(lanes)
    row_tw = twiddles(length, radix)
    col_tw = twiddles(length, col_radix).transpose(2, 0, 1).reshape(lanes, 2 * col_radix)
    swap = [(0, 1), (1, 0)]
    both = ("depth", "row")

    def flat(c, r):
        return c * ranks + r

    def inner(arrays):
        got = [arrays[0]]
        for step in range(1, radix):
            got.append(lax.ppermute(arrays[step], "row", [(r, r ^ step) for r in range(ranks)]))
        return got

    def exchange(x):
        return lax.all_to_all(x, "row", split_axis=0, concat_axis=0, tiled=True)

    residue = residue_of()
    sign = jnp.where(core == 0, -1.0, 1.0)
    omegas = omega_step * freq_index.astype(jnp.float32)
    omega = omegas[frequency_of()]
    tied_tw = row_tw + 0.0 * omega

    far = lax.ppermute(slowness[0], both, [(flat(0, r), flat(0, r ^ radix)) for r in range(ranks)])
    other = lax.ppermute(slowness, "depth", swap)
    blocks = (ranks, 2, rows, points)
    quarter = (2, 2 * rows, points)
    half_field = (2, rows, length)
    per_freq = (ranks // freqs,) + blocks[1:]
    spectra = pl.pallas_call(
        functools.partial(first_kernel, radix),
        grid_spec=pltpu.PrefetchScalarGridSpec(
            num_scalar_prefetch=1,
            grid=(freqs,),
            in_specs=[
                pl.BlockSpec((1, 2, rows, length), lambda f, c: (f, c[0], 0, 0)),
                pl.BlockSpec(row_tw.shape, lambda f, c: (0, 0, 0)),
                pl.BlockSpec(row_forward_table.shape, lambda f, c: (0, 0, 0)),
            ],
            out_specs=pl.BlockSpec(per_freq, lambda f, c: (f, 0, 0, 0)),
        ),
        out_shape=jax.ShapeDtypeStruct(blocks, jnp.float32),
    )(core.astype(jnp.int32).reshape(1), planes, row_tw, row_forward_table)

    col_wave = signed_wave(
        (jnp.arange(lanes, dtype=jnp.int32)[None, :] * col_radix)
        + jnp.arange(col_radix, dtype=jnp.int32)[:, None],
        length,
    )
    row_wave = signed_wave(jnp.arange(points, dtype=jnp.int32) * radix + residue, length)
    plane_waves = col_wave[:, :, None] ** 2 + row_wave[None, None, :] ** 2
    scale = 1.0 / (length * length)

    squares = [(omega * ref_slowness[level]) ** 2 for level in range(2)]

    def propagator(square):
        radicand = square - plane_waves
        vertical = jnp.sqrt(jnp.maximum(radicand, 0.0)) * depth_step
        damping = scale * jnp.exp(-jnp.sqrt(jnp.maximum(-radicand, 0.0)) * depth_step)
        return damping * jnp.cos(vertical), sign * damping * jnp.sin(vertical)

    def screen(slow, slow_ref, frequency):
        theta = frequency * (slow - slow_ref) * depth_step
        return jnp.cos(theta), sign * jnp.sin(theta)

    propagator_a = propagator(squares[0])
    sent = lax.ppermute(far, "depth", [(0, 1)])
    first_slow = jnp.where(core == 0, slowness[0], other[0])
    screens_a = screen(first_slow, ref_slowness[0], omega)
    screens_a += screen(jnp.where(core == 0, far, sent), ref_slowness[0], omega)
    columns = exchange(spectra)
    quarters = call(
        functools.partial(columns_to_quarters, col_radix),
        [quarter] * radix,
        [(radix,) + quarter],
        (columns, *propagator_a, col_tw, col_forward_table, col_inverse_table),
    )
    first, square = lax.optimization_barrier((quarters[0], squares[1]))
    quarters = [first, *quarters[1:]]
    quarters = inner(quarters)
    propagator_b = propagator(square)
    *quarters, keep, send = call(
        functools.partial(middle_kernel, radix),
        [quarter] * radix + [half_field] * 2,
        [(radix,) + quarter, (2,) + half_field, (2,) + half_field],
        (*quarters, *screens_a, tied_tw, row_inverse_table, row_forward_table),
    )
    quarters = inner(quarters)
    got = lax.ppermute(send, "depth", swap)
    share = keep[0] * got[0] + keep[1] * got[1]
    more = lax.ppermute(share, both, [(flat(1, r), flat(0, r ^ radix)) for r in range(ranks)])
    (columns,) = call(
        functools.partial(quarters_to_columns, col_radix, radix),
        [blocks],
        [(radix,) + quarter],
        (*quarters, *propagator_b, col_tw, col_forward_table, col_inverse_table),
    )
    cells = exchange(columns)
    last_slow = jnp.where(core == 0, other[0], slowness[0])
    screens_b = [x for f in range(2) for x in screen(last_slow, ref_slowness[1], omegas[f])]
    (fields,) = call(
        functools.partial(last_kernel, radix),
        [(freqs,) + half_field],
        [],
        (cells, *screens_b, tied_tw, row_inverse_table),
    )
    swapped = lax.ppermute(fields, "depth", swap)
    image, leaving = call(
        output_kernel,
        [(1, rows, length), (1,) + planes.shape[1:]],
        [],
        (fields, swapped, share, more),
        held=False,
    )
    return image, leaving


def solution(mesh):
    in_specs = (P("groups", None, "row", None), P("depth", "row", None), P(), P())
    out_specs = (P(("groups", "depth"), "row", None), P(("groups", "depth"), None, "row", None))
    return jax.shard_map(shards, mesh=mesh, in_specs=in_specs, out_specs=out_specs, check_vma=False)
```

```python
import functools

import jax
import jax.numpy as jnp
import numpy as np
from jax import lax
from jax.experimental import pallas as pl
from jax.experimental.pallas import tpu as pltpu
from jax.sharding import PartitionSpec as P


omega_step = 0.05
depth_step = 1.0
lanes = 128
kernel_vmem = 24 << 20


def pair(table):
    high = table.astype(jnp.bfloat16)
    low = (table - high.astype(np.float64)).astype(jnp.bfloat16)
    return np.stack([high, low])


def real_form(points):
    product = np.outer(np.arange(points), np.arange(points)) % points
    angle = 2.0 * np.pi / points * product
    c, s = np.cos(angle), np.sin(angle)
    return pair(np.block([[c, -s], [s, c]])), pair(np.block([[c, s], [-s, c]]))


def twiddles(length, radix):
    points = length // radix
    angle = 2.0 * np.pi / length * np.outer(np.arange(radix), np.arange(points))
    return np.stack([np.cos(angle), -np.sin(angle)], axis=1).astype(np.float32)


def split(x):
    high = x.astype(jnp.bfloat16)
    return high, (x - high.astype(jnp.float32)).astype(jnp.bfloat16)


def dot(a, b):
    return jnp.dot(a, b, preferred_element_type=jnp.float32)


def times_table(x, table):
    high, low = split(x)
    return dot(high, table[0]) + dot(low, table[0]) + dot(high, table[1])


def table_times(table, x):
    high, low = split(x)
    return dot(table[0], high) + dot(table[0], low) + dot(table[1], high)


def scaled(value, factor):
    if value is None or factor == 0.0:
        return None
    if factor == 1.0:
        return value
    return -value if factor == -1.0 else value * factor


def plus(a, b):
    if a is None:
        return b
    return a if b is None else a + b


def small_transform(parts, sign):
    radix = len(parts)
    if radix == 1:
        return parts
    if radix % 2 == 0:
        half = radix // 2
        even = small_transform(parts[0::2], sign)
        odd = small_transform(parts[1::2], sign)
        first, second = [], []
        for r in range(half):
            angle = sign * 2.0 * np.pi * r / radix
            c, s = float(np.round(np.cos(angle), 15)), float(np.round(np.sin(angle), 15))
            ore, oim = odd[r]
            tre = plus(scaled(ore, c), scaled(oim, -s))
            tim = plus(scaled(oim, c), scaled(ore, s))
            ere, eim = even[r]
            first.append((ere + tre, eim + tim))
            second.append((ere - tre, eim - tim))
        return first + second
    raise ValueError("radix")


def turn(part, factor, conjugate):
    re, im = part
    fre, fim = factor
    if conjugate:
        return re * fre + im * fim, im * fre - re * fim
    return re * fre - im * fim, im * fre + re * fim


def rows_of(parts):
    return jnp.concatenate([jnp.concatenate(part, axis=1) for part in parts], axis=0)


def row_forward(cells, tw, table):
    stacked = []
    for parts in cells:
        for r, part in enumerate(small_transform(parts, -1.0)):
            factor = (tw[r, 0:1], tw[r, 1:2])
            stacked.append(part if r == 0 else turn(part, factor, False))
    return times_table(rows_of(stacked), table)


def row_inverse(ref, tw, table, radix, planes):
    rows, points = ref.shape[2], ref.shape[3]
    count = planes * radix
    stacked = jnp.concatenate(
        [ref[:, 0].reshape(count * rows, points), ref[:, 1].reshape(count * rows, points)], axis=1
    )
    out = times_table(stacked, table)
    cells = []
    for p in range(planes):
        parts = []
        for r in range(radix):
            at = (p * radix + r) * rows
            part = (out[at : at + rows, :points], out[at : at + rows, points:])
            parts.append(part if r == 0 else turn(part, (tw[r, 0:1], tw[r, 1:2]), True))
        cells.append(small_transform(parts, 1.0))
    return cells


def store_blocks(out_ref, value, count, rows, points):
    out_ref[:, 0] = value[:, :points].reshape(count, rows, points)
    out_ref[:, 1] = value[:, points:].reshape(count, rows, points)


def first_kernel(radix, core_ref, planes_ref, tw, table, out_ref):
    count, _, rows, points = out_ref.shape
    parts = [
        tuple(planes_ref[0, i, :, m * points : (m + 1) * points] for i in range(2)) for m in range(radix)
    ]
    value = row_forward([parts], tw, table)
    store_blocks(out_ref, value, count, rows, points)


def residue_of():
    return lax.rem(lax.axis_index("row"), lax.axis_size("row") // 2)


def frequency_of():
    return lax.axis_index("row") // (lax.axis_size("row") // 2)


def spread(held, out_refs):
    own = residue_of()
    for step, ref in enumerate(out_refs):
        ref[...] = held[own ^ step]


def collect(in_refs, held):
    own = residue_of()
    for step, ref in enumerate(in_refs):
        held[own ^ step] = ref[...]


def quarter_place(block, ranks):
    return block % (ranks // 2), block // (ranks // 2)


class Blocks:
    def __init__(self, ref, ranks, rows):
        self.ref, self.ranks, self.rows = ref, ranks, rows

    def at(self, block, part):
        return block, part


class Quarters(Blocks):
    def at(self, block, part):
        quarter, half = quarter_place(block, self.ranks)
        return quarter, part, slice(half * self.rows, (half + 1) * self.rows)


def columns_to_quarters(col_radix, in_ref, hre, him, tw, forward, inverse, *rest):
    out_refs, held = rest[:-1], rest[-1]
    ranks, rows = in_ref.shape[0], in_ref.shape[2]
    source, target = Blocks(in_ref, ranks, rows), Quarters(held, ranks, rows)
    column_kernel(col_radix, source, hre, him, tw, forward, inverse, target)
    spread(held, out_refs)


def quarters_to_columns(col_radix, radix, *refs):
    in_refs, (hre, him, tw, forward, inverse, out_ref, held) = refs[:radix], refs[radix:]
    ranks, rows = out_ref.shape[0], out_ref.shape[2]
    collect(in_refs, held)
    source, target = Quarters(held, ranks, rows), Blocks(out_ref, ranks, rows)
    column_kernel(col_radix, source, hre, him, tw, forward, inverse, target)


def middle_kernel(radix, *refs):
    in_refs, refs = refs[:radix], refs[radix:]
    (own_cos, own_sin, far_cos, far_sin, tw, inverse, forward), refs = refs[:7], refs[7:]
    out_refs, (keep_ref, send_ref, held, field, screen) = refs[:radix], refs[radix:]
    rows, points = held.shape[2], held.shape[3]
    mine = frequency_of()
    for half, pair_refs in ((mine, (own_cos, own_sin)), (1 - mine, (far_cos, far_sin))):
        for i, ref in enumerate(pair_refs):
            screen[i, half] = ref[...]
    collect(in_refs, held)
    (cells,) = row_inverse(held, tw, inverse, radix, 1)
    turned = []
    for m in range(radix):
        at = slice(m * points, (m + 1) * points)
        factor = [screen[i, :, :, at].reshape(rows, points) for i in range(2)]
        part = turn(cells[m], factor, False)
        for half in range(2):
            for i in range(2):
                field[half, i, :, at] = part[i][half * rows // 2 : (half + 1) * rows // 2]
        turned.append(part)
    kept = mine ^ lax.axis_index("depth")
    keep_ref[...] = field[kept]
    send_ref[...] = field[1 - kept]
    value = row_forward([turned], tw, forward)
    store_blocks(held, value, radix, rows, points)
    spread(held, out_refs)


def column_kernel(radix, source, hre, him, tw, forward, inverse, target):
    points, width = hre.shape[1], hre.shape[2]
    rows = source.rows
    per = points // rows

    def block(m, part):
        pieces = [source.ref[source.at(m * per + i, part)] for i in range(per)]
        return jnp.concatenate(pieces, axis=0)

    parts = small_transform([(block(m, 0), block(m, 1)) for m in range(radix)], -1.0)
    columns = []
    for r, part in enumerate(parts):
        if r > 0:
            factor = (tw[:, 2 * r : 2 * r + 1], tw[:, 2 * r + 1 : 2 * r + 2])
            part = turn(part, factor, False)
        columns.append(jnp.concatenate(part, axis=0))
    spectrum = table_times(forward, jnp.concatenate(columns, axis=1))
    columns = []
    for r in range(radix):
        at = slice(r * width, (r + 1) * width)
        part = turn((spectrum[:points, at], spectrum[points:, at]), (hre[r], him[r]), False)
        columns.append(jnp.concatenate(part, axis=0))
    back = table_times(inverse, jnp.concatenate(columns, axis=1))
    parts = []
    for r in range(radix):
        at = slice(r * width, (r + 1) * width)
        part = (back[:points, at], back[points:, at])
        if r > 0:
            factor = (tw[:, 2 * r : 2 * r + 1], tw[:, 2 * r + 1 : 2 * r + 2])
            part = turn(part, factor, True)
        parts.append(part)
    for m, (re, im) in enumerate(small_transform(parts, 1.0)):
        for i in range(per):
            at = slice(i * rows, (i + 1) * rows)
            target.ref[target.at(m * per + i, 0)] = re[at]
            target.ref[target.at(m * per + i, 1)] = im[at]


def middle_kernel(radix, *refs):
    in_refs, refs = refs[:radix], refs[radix:]
    (own_cos, own_sin, far_cos, far_sin, tw, inverse, forward), refs = refs[:7], refs[7:]
    out_refs, (keep_ref, send_ref, held, field, screen) = refs[:radix], refs[radix:]
    rows, points = held.shape[2], held.shape[3]
    mine = frequency_of()
    for half, pair_refs in ((mine, (own_cos, own_sin)), (1 - mine, (far_cos, far_sin))):
        for i, ref in enumerate(pair_refs):
            screen[i, half] = ref[...]
    collect(in_refs, held)
    (cells,) = row_inverse(held, tw, inverse, radix, 1)
    turned = []
    for m in range(radix):
        at = slice(m * points, (m + 1) * points)
        factor = [screen[i, :, :, at].reshape(rows, points) for i in range(2)]
        part = turn(cells[m], factor, False)
        for half in range(2):
            for i in range(2):
                field[half, i, :, at] = part[i][half * rows // 2 : (half + 1) * rows // 2]
        turned.append(part)
    kept = mine ^ lax.axis_index("depth")
    keep_ref[...] = field[kept]
    send_ref[...] = field[1 - kept]
    value = row_forward([turned], tw, forward)
    store_blocks(held, value, radix, rows, points)
    spread(held, out_refs)


def column_kernel(radix, source, hre, him, tw, forward, inverse, target):
    points, width = hre.shape[1], hre.shape[2]
    rows = source.rows
    per = points // rows

    def block(m, part):
        pieces = [source.ref[source.at(m * per + i, part)] for i in range(per)]
        return jnp.concatenate(pieces, axis=0)

    parts = small_transform([(block(m, 0), block(m, 1)) for m in range(radix)], -1.0)
    columns = []
    for r, part in enumerate(parts):
        if r > 0:
            factor = (tw[:, 2 * r : 2 * r + 1], tw[:, 2 * r + 1 : 2 * r + 2])
            part = turn(part, factor, False)
        columns.append(jnp.concatenate(part, axis=0))
    spectrum = table_times(forward, jnp.concatenate(columns, axis=1))
    columns = []
    for r in range(radix):
        at = slice(r * width, (r + 1) * width)
        part = turn((spectrum[:points, at], spectrum[points:, at]), (hre[r], him[r]), False)
        columns.append(jnp.concatenate(part, axis=0))
    back = table_times(inverse, jnp.concatenate(columns, axis=1))
    parts = []
    for r in range(radix):
        at = slice(r * width, (r + 1) * width)
        part = (back[:points, at], back[points:, at])
        if r > 0:
            factor = (tw[:, 2 * r : 2 * r + 1], tw[:, 2 * r + 1 : 2 * r + 2])
            part = turn(part, factor, True)
        parts.append(part)
    for m, (re, im) in enumerate(small_transform(parts, 1.0)):
        for i in range(per):
            at = slice(i * rows, (i + 1) * rows)
            target.ref[target.at(m * per + i, 0)] = re[at]
            target.ref[target.at(m * per + i, 1)] = im[at]


def last_kernel(radix, in_ref, *refs):
    screens, (tw, inverse, out_ref) = refs[:4], refs[4:]
    points = in_ref.shape[3]
    for f, parts in enumerate(row_inverse(in_ref, tw, inverse, radix, 2)):
        for m, part in enumerate(parts):
            at = slice(m * points, (m + 1) * points)
            factor = (screens[2 * f][:, at], screens[2 * f + 1][:, at])
            re, im = turn(part, factor, False)
            out_ref[f, 0, :, at] = re
            out_ref[f, 1, :, at] = im


def output_kernel(own_ref, got_ref, share_ref, more_ref, image_ref, leaving_ref):
    for core, (source, receiver) in enumerate(((own_ref, got_ref), (got_ref, own_ref))):

        @pl.when(lax.axis_index("depth") == core)
        def _():
            leaving_ref[0, 0:2] = source[core]
            leaving_ref[0, 2:4] = receiver[core]
            if core == 0:
                image_ref[0] = share_ref[...] + more_ref[...]
            else:
                terms = [source[f, i] * receiver[f, i] for f in range(2) for i in range(2)]
                image_ref[0] = (terms[0] + terms[1]) + (terms[2] + terms[3])


def signed_wave(positions, length):
    signed = jnp.where(positions < length // 2, positions, positions - length)
    return 2.0 * jnp.pi / length * signed.astype(jnp.float32)


def cos_sin(x):
    turns = jnp.floor(x * (2.0 / np.pi) + 0.5)
    rest = ((x - turns * 1.5703125) - turns * 4.837512969970703e-04) - turns * 7.549789948768648e-08
    square = rest * rest
    sine = 2.75573192e-06 - 2.50521084e-08 * square
    sine = -1.98412698e-04 + square * sine
    sine = 8.33333333e-03 + square * sine
    sine = -1.66666667e-01 + square * sine
    sine = rest + rest * square * sine
    cosine = -2.75573192e-07 + 2.08767570e-09 * square
    cosine = 2.48015873e-05 + square * cosine
    cosine = -1.38888889e-03 + square * cosine
    cosine = 4.16666667e-02 + square * cosine
    cosine = 1.0 - 0.5 * square + square * square * cosine
    count = turns.astype(jnp.int32)
    odd = (count & 1) == 1
    new_cos, new_sin = jnp.where(odd, sine, cosine), jnp.where(odd, cosine, sine)
    new_cos = jnp.where(((count + 1) & 2) == 2, -new_cos, new_cos)
    new_sin = jnp.where((count & 2) == 2, -new_sin, new_sin)
    return new_cos, new_sin


def factor_kernel(radix, freq_ref, ref_ref, slow_ref, other_ref, far_ref, sent_ref, tw_ref, *outs):
    (tw_out, hre_a, him_a, hre_b, him_b), outs = outs[:5], outs[5:]
    tw_out[...] = tw_ref[...]
    col_radix, points, width = hre_a.shape
    length = col_radix * points
    core = lax.axis_index("depth")
    first = core == 0
    sign = jnp.where(first, -1.0, 1.0)
    omegas = [omega_step * freq_ref[f].astype(jnp.float32) for f in range(2)]
    omega = jnp.where(frequency_of() == 0, omegas[0], omegas[1])
    scale = 1.0 / (length * length)
    row_at = lax.broadcasted_iota(jnp.int32, (1, width), 1) * radix + residue_of()
    row_square = signed_wave(row_at, length) ** 2
    for r in range(col_radix):
        col_at = lax.broadcasted_iota(jnp.int32, (points, width), 0) * col_radix + r
        plane_waves = signed_wave(col_at, length) ** 2 + row_square
        for level, (hre, him) in enumerate(((hre_a, him_a), (hre_b, him_b))):
            radicand = (omega * ref_ref[level]) ** 2 - plane_waves
            vertical = jnp.sqrt(jnp.maximum(radicand, 0.0)) * depth_step
            damping = scale * jnp.exp(-jnp.sqrt(jnp.maximum(-radicand, 0.0)) * depth_step)
            cosine, sine = cos_sin(vertical)
            hre[r], him[r] = damping * cosine, sign * damping * sine

    def screen(slow, level, frequency, at):
        cosine, sine = cos_sin(frequency * (slow - ref_ref[level]) * depth_step)
        outs[at][...], outs[at + 1][...] = cosine, sign * sine

    own, other = slow_ref[0], other_ref[0]
    screen(jnp.where(first, own, other), 0, omega, 0)
    screen(jnp.where(first, far_ref[...], sent_ref[...]), 0, omega, 2)
    last = jnp.where(first, other, own)
    for f in range(2):
        screen(last, 1, omegas[f], 4 + 2 * f)


def call(kernel, out_shapes, scratch, args, held=True, scalars=()):
    vmem = pl.BlockSpec(memory_space=pltpu.VMEM)
    smem = pl.BlockSpec(memory_space=pltpu.SMEM)
    shape = pltpu.VMEM if held else jax.ShapeDtypeStruct
    return pl.pallas_call(
        kernel,
        in_specs=[smem] * len(scalars) + [vmem] * len(args),
        out_specs=[vmem] * len(out_shapes),
        out_shape=[shape(s, jnp.float32) for s in out_shapes],
        scratch_shapes=[pltpu.VMEM(s, jnp.float32) for s in scratch],
        compiler_params=pltpu.CompilerParams(vmem_limit_bytes=kernel_vmem),
    )(*scalars, *[pltpu.with_memory_space_constraint(a, pltpu.VMEM) for a in args])


def shards(planes, slowness, ref_slowness, freq_index):
    freqs, _, rows, length = planes.shape
    ranks = lax.axis_size("row")
    radix = ranks // 2
    points = length // radix
    col_radix = length // lanes
    core = lax.axis_index("depth")

    row_forward_table, row_inverse_table = real_form(points)
    col_inverse_table, col_forward_table = real_form(lanes)
    row_tw = twiddles(length, radix)
    col_tw = twiddles(length, col_radix).transpose(2, 0, 1).reshape(lanes, 2 * col_radix)
    swap = [(0, 1), (1, 0)]
    both = ("depth", "row")

    def flat(c, r):
        return c * ranks + r

    def inner(arrays):
        got = [arrays[0]]
        for step in range(1, radix):
            got.append(lax.ppermute(arrays[step], "row", [(r, r ^ step) for r in range(ranks)]))
        return got

    def exchange(x):
        return lax.all_to_all(x, "row", split_axis=0, concat_axis=0, tiled=True)

    far = lax.ppermute(slowness[0], both, [(flat(0, r), flat(0, r ^ radix)) for r in range(ranks)])
    other = lax.ppermute(slowness, "depth", swap)
    blocks = (ranks, 2, rows, points)
    quarter = (2, 2 * rows, points)
    half_field = (2, rows, length)
    per_freq = (ranks // freqs,) + blocks[1:]
    spectra = pl.pallas_call(
        functools.partial(first_kernel, radix),
        grid_spec=pltpu.PrefetchScalarGridSpec(
            num_scalar_prefetch=1,
            grid=(freqs,),
            in_specs=[
                pl.BlockSpec((1, 2, rows, length), lambda f, c: (f, c[0], 0, 0)),
                pl.BlockSpec(row_tw.shape, lambda f, c: (0, 0, 0)),
                pl.BlockSpec(row_forward_table.shape, lambda f, c: (0, 0, 0)),
            ],
            out_specs=pl.BlockSpec(per_freq, lambda f, c: (f, 0, 0, 0)),
        ),
        out_shape=jax.ShapeDtypeStruct(blocks, jnp.float32),
    )(core.astype(jnp.int32).reshape(1), planes, row_tw, row_forward_table)

    sent = lax.ppermute(far, "depth", [(0, 1)])
    plane = (rows, length)
    factor = (col_radix, lanes, points)
    held_tw, *factors = call(
        functools.partial(factor_kernel, radix),
        [row_tw.shape] + [factor] * 4 + [plane] * 8,
        [],
        (slowness, other, far, sent, row_tw),
        scalars=(freq_index, ref_slowness),
    )
    propagator_a, propagator_b = factors[:2], factors[2:4]
    screens_a, screens_b = factors[4:8], factors[8:12]
    columns = exchange(spectra)
    quarters = call(
        functools.partial(columns_to_quarters, col_radix),
        [quarter] * radix,
        [(radix,) + quarter],
        (columns, *propagator_a, col_tw, col_forward_table, col_inverse_table),
    )
    quarters = inner(quarters)
    *quarters, keep, send = call(
        functools.partial(middle_kernel, radix),
        [quarter] * radix + [half_field] * 2,
        [(radix,) + quarter, (2,) + half_field, (2,) + half_field],
        (*quarters, *screens_a, held_tw, row_inverse_table, row_forward_table),
    )
    quarters = inner(quarters)
    got = lax.ppermute(send, "depth", swap)
    share = keep[0] * got[0] + keep[1] * got[1]
    more = lax.ppermute(share, both, [(flat(1, r), flat(0, r ^ radix)) for r in range(ranks)])
    (columns,) = call(
        functools.partial(quarters_to_columns, col_radix, radix),
        [blocks],
        [(radix,) + quarter],
        (*quarters, *propagator_b, col_tw, col_forward_table, col_inverse_table),
    )
    cells = exchange(columns)
    (fields,) = call(
        functools.partial(last_kernel, radix),
        [(freqs,) + half_field],
        [],
        (cells, *screens_b, held_tw, row_inverse_table),
    )
    swapped = lax.ppermute(fields, "depth", swap)
    image, leaving = call(
        output_kernel,
        [(1, rows, length), (1,) + planes.shape[1:]],
        [],
        (fields, swapped, share, more),
        held=False,
    )
    return image, leaving


def solution(mesh):
    in_specs = (P("groups", None, "row", None), P("depth", "row", None), P(), P())
    out_specs = (P(("groups", "depth"), "row", None), P(("groups", "depth"), None, "row", None))
    return jax.shard_map(shards, mesh=mesh, in_specs=in_specs, out_specs=out_specs, check_vma=False)
```

```python
import functools

import jax
import jax.numpy as jnp
import numpy as np
from jax import lax
from jax.experimental import pallas as pl
from jax.experimental.pallas import tpu as pltpu
from jax.sharding import PartitionSpec as P


omega_step = 0.05
depth_step = 1.0
lanes = 128
kernel_vmem = 24 << 20


def pair(table):
    high = table.astype(jnp.bfloat16)
    low = (table - high.astype(np.float64)).astype(jnp.bfloat16)
    return np.stack([high, low])


def real_form(points):
    product = np.outer(np.arange(points), np.arange(points)) % points
    angle = 2.0 * np.pi / points * product
    c, s = np.cos(angle), np.sin(angle)
    return pair(np.block([[c, -s], [s, c]])), pair(np.block([[c, s], [-s, c]]))


def twiddles(length, radix):
    points = length // radix
    angle = 2.0 * np.pi / length * np.outer(np.arange(radix), np.arange(points))
    return np.stack([np.cos(angle), -np.sin(angle)], axis=1).astype(np.float32)


def split(x):
    high = x.astype(jnp.bfloat16)
    return high, (x - high.astype(jnp.float32)).astype(jnp.bfloat16)


def dot(a, b):
    return jnp.dot(a, b, preferred_element_type=jnp.float32)


def times_table(x, table):
    high, low = split(x)
    return dot(high, table[0]) + dot(low, table[0]) + dot(high, table[1])


def table_times(table, x):
    high, low = split(x)
    return dot(table[0], high) + dot(table[0], low) + dot(table[1], high)


def scaled(value, factor):
    if value is None or factor == 0.0:
        return None
    if factor == 1.0:
        return value
    return -value if factor == -1.0 else value * factor


def plus(a, b):
    if a is None:
        return b
    return a if b is None else a + b


def small_transform(parts, sign):
    radix = len(parts)
    if radix == 1:
        return parts
    if radix % 2 == 0:
        half = radix // 2
        even = small_transform(parts[0::2], sign)
        odd = small_transform(parts[1::2], sign)
        first, second = [], []
        for r in range(half):
            angle = sign * 2.0 * np.pi * r / radix
            c, s = float(np.round(np.cos(angle), 15)), float(np.round(np.sin(angle), 15))
            ore, oim = odd[r]
            tre = plus(scaled(ore, c), scaled(oim, -s))
            tim = plus(scaled(oim, c), scaled(ore, s))
            ere, eim = even[r]
            first.append((ere + tre, eim + tim))
            second.append((ere - tre, eim - tim))
        return first + second
    raise ValueError("radix")


def turn(part, factor, conjugate):
    re, im = part
    fre, fim = factor
    if conjugate:
        return re * fre + im * fim, im * fre - re * fim
    return re * fre - im * fim, im * fre + re * fim


def rows_of(parts):
    return jnp.concatenate([jnp.concatenate(part, axis=1) for part in parts], axis=0)


def row_forward(cells, tw, table):
    stacked = []
    for parts in cells:
        for r, part in enumerate(small_transform(parts, -1.0)):
            factor = (tw[r, 0:1], tw[r, 1:2])
            stacked.append(part if r == 0 else turn(part, factor, False))
    return times_table(rows_of(stacked), table)


def row_inverse(ref, tw, table, radix, planes):
    rows, points = ref.shape[2], ref.shape[3]
    count = planes * radix
    stacked = jnp.concatenate(
        [ref[:, 0].reshape(count * rows, points), ref[:, 1].reshape(count * rows, points)], axis=1
    )
    out = times_table(stacked, table)
    cells = []
    for p in range(planes):
        parts = []
        for r in range(radix):
            at = (p * radix + r) * rows
            part = (out[at : at + rows, :points], out[at : at + rows, points:])
            parts.append(part if r == 0 else turn(part, (tw[r, 0:1], tw[r, 1:2]), True))
        cells.append(small_transform(parts, 1.0))
    return cells


def store_blocks(out_ref, value, count, rows, points):
    out_ref[:, 0] = value[:, :points].reshape(count, rows, points)
    out_ref[:, 1] = value[:, points:].reshape(count, rows, points)


def first_kernel(radix, planes_ref, tw, table, *rest):
    out_refs, (loaded, held, sems) = rest[:-3], rest[-3:]
    freqs, _, rows, length = loaded.shape
    points = length // radix
    core = lax.axis_index("depth")
    copies = [
        pltpu.make_async_copy(planes_ref.at[f, pl.ds(2 * core, 2)], loaded.at[f], sems.at[f])
        for f in range(freqs)
    ]
    for copy in copies:
        copy.start()
    for f, copy in enumerate(copies):
        copy.wait()
        parts = [
            tuple(loaded[f, i, :, m * points : (m + 1) * points] for i in range(2)) for m in range(radix)
        ]
        value = row_forward([parts], tw, table)
        at = slice(f * radix, (f + 1) * radix)
        held[at, 0] = value[:, :points].reshape(radix, rows, points)
        held[at, 1] = value[:, points:].reshape(radix, rows, points)
    spread(held, out_refs, lax.axis_index("row"))


def residue_of():
    return lax.rem(lax.axis_index("row"), lax.axis_size("row") // 2)


def frequency_of():
    return lax.axis_index("row") // (lax.axis_size("row") // 2)


def spread(held, out_refs, own):
    for step, ref in enumerate(out_refs):
        ref[...] = held[own ^ step]


def collect(in_refs, held, own):
    for step, ref in enumerate(in_refs):
        held[own ^ step] = ref[...]


def quarter_place(block, ranks):
    return block % (ranks // 2), block // (ranks // 2)


class Blocks:
    def __init__(self, ref, ranks, rows):
        self.ref, self.ranks, self.rows = ref, ranks, rows

    def at(self, block, part):
        return block, part


class Quarters(Blocks):
    def at(self, block, part):
        quarter, half = quarter_place(block, self.ranks)
        return quarter, part, slice(half * self.rows, (half + 1) * self.rows)


def columns_to_quarters(col_radix, ranks, *refs):
    in_refs, (hre, him, tw, forward, inverse), rest = refs[:ranks], refs[ranks : ranks + 5], refs[ranks + 5 :]
    out_refs, (blocks, quarters) = rest[:-2], rest[-2:]
    rows = blocks.shape[2]
    collect(in_refs, blocks, lax.axis_index("row"))
    source, target = Blocks(blocks, ranks, rows), Quarters(quarters, ranks, rows)
    column_kernel(col_radix, source, hre, him, tw, forward, inverse, target)
    spread(quarters, out_refs, residue_of())


def quarters_to_columns(col_radix, radix, *refs):
    in_refs, (hre, him, tw, forward, inverse), rest = refs[:radix], refs[radix : radix + 5], refs[radix + 5 :]
    out_refs, (blocks, quarters) = rest[:-2], rest[-2:]
    ranks, rows = blocks.shape[0], blocks.shape[2]
    collect(in_refs, quarters, residue_of())
    source, target = Quarters(quarters, ranks, rows), Blocks(blocks, ranks, rows)
    column_kernel(col_radix, source, hre, him, tw, forward, inverse, target)
    spread(blocks, out_refs, lax.axis_index("row"))


def column_kernel(radix, source, hre, him, tw, forward, inverse, target):
    points, width = hre.shape[1], hre.shape[2]
    rows = source.rows
    per = points // rows

    def block(m, part):
        pieces = [source.ref[source.at(m * per + i, part)] for i in range(per)]
        return jnp.concatenate(pieces, axis=0)

    parts = small_transform([(block(m, 0), block(m, 1)) for m in range(radix)], -1.0)
    columns = []
    for r, part in enumerate(parts):
        if r > 0:
            factor = (tw[:, 2 * r : 2 * r + 1], tw[:, 2 * r + 1 : 2 * r + 2])
            part = turn(part, factor, False)
        columns.append(jnp.concatenate(part, axis=0))
    spectrum = table_times(forward, jnp.concatenate(columns, axis=1))
    columns = []
    for r in range(radix):
        at = slice(r * width, (r + 1) * width)
        part = turn((spectrum[:points, at], spectrum[points:, at]), (hre[r], him[r]), False)
        columns.append(jnp.concatenate(part, axis=0))
    back = table_times(inverse, jnp.concatenate(columns, axis=1))
    parts = []
    for r in range(radix):
        at = slice(r * width, (r + 1) * width)
        part = (back[:points, at], back[points:, at])
        if r > 0:
            factor = (tw[:, 2 * r : 2 * r + 1], tw[:, 2 * r + 1 : 2 * r + 2])
            part = turn(part, factor, True)
        parts.append(part)
    for m, (re, im) in enumerate(small_transform(parts, 1.0)):
        for i in range(per):
            at = slice(i * rows, (i + 1) * rows)
            target.ref[target.at(m * per + i, 0)] = re[at]
            target.ref[target.at(m * per + i, 1)] = im[at]


def middle_kernel(radix, *refs):
    in_refs, refs = refs[:radix], refs[radix:]
    (own_cos, own_sin, far_cos, far_sin, tw, inverse, forward), refs = refs[:7], refs[7:]
    out_refs, (keep_ref, send_ref, held, field, screen) = refs[:radix], refs[radix:]
    rows, points = held.shape[2], held.shape[3]
    mine = frequency_of()
    for half, pair_refs in ((mine, (own_cos, own_sin)), (1 - mine, (far_cos, far_sin))):
        for i, ref in enumerate(pair_refs):
            screen[i, half] = ref[...]
    collect(in_refs, held, residue_of())
    (cells,) = row_inverse(held, tw, inverse, radix, 1)
    turned = []
    for m in range(radix):
        at = slice(m * points, (m + 1) * points)
        factor = [screen[i, :, :, at].reshape(rows, points) for i in range(2)]
        part = turn(cells[m], factor, False)
        for half in range(2):
            for i in range(2):
                field[half, i, :, at] = part[i][half * rows // 2 : (half + 1) * rows // 2]
        turned.append(part)
    kept = mine ^ lax.axis_index("depth")
    keep_ref[...] = field[kept]
    send_ref[...] = field[1 - kept]
    value = row_forward([turned], tw, forward)
    store_blocks(held, value, radix, rows, points)
    spread(held, out_refs, residue_of())


def column_kernel(radix, source, hre, him, tw, forward, inverse, target):
    points, width = hre.shape[1], hre.shape[2]
    rows = source.rows
    per = points // rows

    def block(m, part):
        pieces = [source.ref[source.at(m * per + i, part)] for i in range(per)]
        return jnp.concatenate(pieces, axis=0)

    parts = small_transform([(block(m, 0), block(m, 1)) for m in range(radix)], -1.0)
    columns = []
    for r, part in enumerate(parts):
        if r > 0:
            factor = (tw[:, 2 * r : 2 * r + 1], tw[:, 2 * r + 1 : 2 * r + 2])
            part = turn(part, factor, False)
        columns.append(jnp.concatenate(part, axis=0))
    spectrum = table_times(forward, jnp.concatenate(columns, axis=1))
    columns = []
    for r in range(radix):
        at = slice(r * width, (r + 1) * width)
        part = turn((spectrum[:points, at], spectrum[points:, at]), (hre[r], him[r]), False)
        columns.append(jnp.concatenate(part, axis=0))
    back = table_times(inverse, jnp.concatenate(columns, axis=1))
    parts = []
    for r in range(radix):
        at = slice(r * width, (r + 1) * width)
        part = (back[:points, at], back[points:, at])
        if r > 0:
            factor = (tw[:, 2 * r : 2 * r + 1], tw[:, 2 * r + 1 : 2 * r + 2])
            part = turn(part, factor, True)
        parts.append(part)
    for m, (re, im) in enumerate(small_transform(parts, 1.0)):
        for i in range(per):
            at = slice(i * rows, (i + 1) * rows)
            target.ref[target.at(m * per + i, 0)] = re[at]
            target.ref[target.at(m * per + i, 1)] = im[at]


def last_kernel(radix, ranks, *refs):
    in_refs, screens, (tw, inverse, out_ref, held) = refs[:ranks], refs[ranks : ranks + 4], refs[ranks + 4 :]
    points = held.shape[3]
    collect(in_refs, held, lax.axis_index("row"))
    for f, parts in enumerate(row_inverse(held, tw, inverse, radix, 2)):
        for m, part in enumerate(parts):
            at = slice(m * points, (m + 1) * points)
            factor = (screens[2 * f][:, at], screens[2 * f + 1][:, at])
            re, im = turn(part, factor, False)
            out_ref[f, 0, :, at] = re
            out_ref[f, 1, :, at] = im


def output_kernel(own_ref, got_ref, share_ref, more_ref, image_ref, leaving_ref):
    for core, (source, receiver) in enumerate(((own_ref, got_ref), (got_ref, own_ref))):

        @pl.when(lax.axis_index("depth") == core)
        def _():
            leaving_ref[0, 0:2] = source[core]
            leaving_ref[0, 2:4] = receiver[core]
            if core == 0:
                image_ref[0] = share_ref[...] + more_ref[...]
            else:
                terms = [source[f, i] * receiver[f, i] for f in range(2) for i in range(2)]
                image_ref[0] = (terms[0] + terms[1]) + (terms[2] + terms[3])


def signed_wave(positions, length):
    signed = jnp.where(positions < length // 2, positions, positions - length)
    return 2.0 * jnp.pi / length * signed.astype(jnp.float32)


def cos_sin(x):
    turns = jnp.floor(x * (2.0 / np.pi) + 0.5)
    rest = ((x - turns * 1.5703125) - turns * 4.837512969970703e-04) - turns * 7.549789948768648e-08
    square = rest * rest
    sine = 2.75573192e-06 - 2.50521084e-08 * square
    sine = -1.98412698e-04 + square * sine
    sine = 8.33333333e-03 + square * sine
    sine = -1.66666667e-01 + square * sine
    sine = rest + rest * square * sine
    cosine = -2.75573192e-07 + 2.08767570e-09 * square
    cosine = 2.48015873e-05 + square * cosine
    cosine = -1.38888889e-03 + square * cosine
    cosine = 4.16666667e-02 + square * cosine
    cosine = 1.0 - 0.5 * square + square * square * cosine
    count = turns.astype(jnp.int32)
    odd = (count & 1) == 1
    new_cos, new_sin = jnp.where(odd, sine, cosine), jnp.where(odd, cosine, sine)
    new_cos = jnp.where(((count + 1) & 2) == 2, -new_cos, new_cos)
    new_sin = jnp.where((count & 2) == 2, -new_sin, new_sin)
    return new_cos, new_sin


def factor_kernel(radix, freq_ref, ref_ref, slow_ref, other_ref, far_ref, sent_ref, tw_ref, *outs):
    (tw_out, hre_a, him_a, hre_b, him_b), outs = outs[:5], outs[5:]
    tw_out[...] = tw_ref[...]
    col_radix, points, width = hre_a.shape
    length = col_radix * points
    core = lax.axis_index("depth")
    first = core == 0
    sign = jnp.where(first, -1.0, 1.0)
    omegas = [omega_step * freq_ref[f].astype(jnp.float32) for f in range(2)]
    omega = jnp.where(frequency_of() == 0, omegas[0], omegas[1])
    scale = 1.0 / (length * length)
    row_at = lax.broadcasted_iota(jnp.int32, (1, width), 1) * radix + residue_of()
    row_square = signed_wave(row_at, length) ** 2
    for r in range(col_radix):
        col_at = lax.broadcasted_iota(jnp.int32, (points, width), 0) * col_radix + r
        plane_waves = signed_wave(col_at, length) ** 2 + row_square
        for level, (hre, him) in enumerate(((hre_a, him_a), (hre_b, him_b))):
            radicand = (omega * ref_ref[level]) ** 2 - plane_waves
            vertical = jnp.sqrt(jnp.maximum(radicand, 0.0)) * depth_step
            damping = scale * jnp.exp(-jnp.sqrt(jnp.maximum(-radicand, 0.0)) * depth_step)
            cosine, sine = cos_sin(vertical)
            hre[r], him[r] = damping * cosine, sign * damping * sine

    def screen(slow, level, frequency, at):
        cosine, sine = cos_sin(frequency * (slow - ref_ref[level]) * depth_step)
        outs[at][...], outs[at + 1][...] = cosine, sign * sine

    own, other = slow_ref[0], other_ref[0]
    screen(jnp.where(first, own, other), 0, omega, 0)
    screen(jnp.where(first, far_ref[...], sent_ref[...]), 0, omega, 2)
    last = jnp.where(first, other, own)
    for f in range(2):
        screen(last, 1, omegas[f], 4 + 2 * f)


def call(kernel, out_shapes, scratch, args, held=True, scalars=()):
    vmem = pl.BlockSpec(memory_space=pltpu.VMEM)
    smem = pl.BlockSpec(memory_space=pltpu.SMEM)
    shape = pltpu.VMEM if held else jax.ShapeDtypeStruct
    return pl.pallas_call(
        kernel,
        in_specs=[smem] * len(scalars) + [vmem] * len(args),
        out_specs=[vmem] * len(out_shapes),
        out_shape=[shape(s, jnp.float32) for s in out_shapes],
        scratch_shapes=[pltpu.VMEM(s, jnp.float32) for s in scratch],
        compiler_params=pltpu.CompilerParams(vmem_limit_bytes=kernel_vmem),
    )(*scalars, *[pltpu.with_memory_space_constraint(a, pltpu.VMEM) for a in args])


def shards(planes, slowness, ref_slowness, freq_index):
    freqs, _, rows, length = planes.shape
    ranks = lax.axis_size("row")
    radix = ranks // 2
    points = length // radix
    col_radix = length // lanes

    row_forward_table, row_inverse_table = real_form(points)
    col_inverse_table, col_forward_table = real_form(lanes)
    row_tw = twiddles(length, radix)
    col_tw = twiddles(length, col_radix).transpose(2, 0, 1).reshape(lanes, 2 * col_radix)
    swap = [(0, 1), (1, 0)]
    both = ("depth", "row")

    def flat(c, r):
        return c * ranks + r

    def hop(array, step):
        return lax.ppermute(array, "row", [(r, r ^ step) for r in range(ranks)])

    def exchange(arrays, steps):
        got = list(arrays)
        for step in steps:
            got[step] = hop(arrays[step], step)
        return got

    inner_steps = list(range(radix - 1, 0, -1))
    outer_steps = list(range(radix, ranks)) + list(range(1, radix))

    far = lax.ppermute(slowness[0], both, [(flat(0, r), flat(0, r ^ radix)) for r in range(ranks)])
    other = lax.ppermute(slowness, "depth", swap)
    blocks = (ranks, 2, rows, points)
    quarter = (2, 2 * rows, points)
    half_field = (2, rows, length)
    vmem, hbm = (pl.BlockSpec(memory_space=space) for space in (pltpu.VMEM, pl.ANY))
    spectra = pl.pallas_call(
        functools.partial(first_kernel, radix),
        in_specs=[hbm, vmem, vmem],
        out_specs=[vmem] * ranks,
        out_shape=[pltpu.VMEM(blocks[1:], jnp.float32)] * ranks,
        scratch_shapes=[
            pltpu.VMEM((freqs,) + half_field, jnp.float32),
            pltpu.VMEM(blocks, jnp.float32),
            pltpu.SemaphoreType.DMA((freqs,)),
        ],
    )(planes, row_tw, row_forward_table)
    sent = lax.ppermute(far, "depth", [(0, 1)])
    plane = (rows, length)
    factor = (col_radix, lanes, points)
    held_tw, *factors = call(
        functools.partial(factor_kernel, radix),
        [row_tw.shape] + [factor] * 4 + [plane] * 8,
        [],
        (slowness, other, far, sent, row_tw),
        scalars=(freq_index, ref_slowness),
    )
    propagator_a, propagator_b = factors[:2], factors[2:4]
    screens_a, screens_b = factors[4:8], factors[8:12]
    columns = exchange(spectra, outer_steps)
    quarters = call(
        functools.partial(columns_to_quarters, col_radix, ranks),
        [quarter] * radix,
        [blocks, (radix,) + quarter],
        (*columns, *propagator_a, col_tw, col_forward_table, col_inverse_table),
    )
    quarters = exchange(quarters, inner_steps)
    *quarters, keep, send = call(
        functools.partial(middle_kernel, radix),
        [quarter] * radix + [half_field] * 2,
        [(radix,) + quarter, (2,) + half_field, (2,) + half_field],
        (*quarters, *screens_a, held_tw, row_inverse_table, row_forward_table),
    )
    quarters = exchange(quarters, inner_steps)
    got = lax.ppermute(send, "depth", swap)
    share = keep[0] * got[0] + keep[1] * got[1]
    more = lax.ppermute(share, both, [(flat(1, r), flat(0, r ^ radix)) for r in range(ranks)])
    columns = call(
        functools.partial(quarters_to_columns, col_radix, radix),
        [blocks[1:]] * ranks,
        [blocks, (radix,) + quarter],
        (*quarters, *propagator_b, col_tw, col_forward_table, col_inverse_table),
    )
    cells = exchange(columns, outer_steps)
    (fields,) = call(
        functools.partial(last_kernel, radix, ranks),
        [(freqs,) + half_field],
        [blocks],
        (*cells, *screens_b, held_tw, row_inverse_table),
    )
    swapped = lax.ppermute(fields, "depth", swap)
    image, leaving = call(
        output_kernel,
        [(1, rows, length), (1,) + planes.shape[1:]],
        [],
        (fields, swapped, share, more),
        held=False,
    )
    return image, leaving


def solution(mesh):
    in_specs = (P("groups", None, "row", None), P("depth", "row", None), P(), P())
    out_specs = (P(("groups", "depth"), "row", None), P(("groups", "depth"), None, "row", None))
    return jax.shard_map(shards, mesh=mesh, in_specs=in_specs, out_specs=out_specs, check_vma=False)
```

```python
import functools

import jax
import jax.numpy as jnp
import numpy as np
from jax import lax
from jax.experimental import pallas as pl
from jax.experimental.pallas import tpu as pltpu
from jax.sharding import PartitionSpec as P


omega_step = 0.05
depth_step = 1.0
lanes = 128
kernel_vmem = 24 << 20


def pair(table):
    high = table.astype(jnp.bfloat16)
    low = (table - high.astype(np.float64)).astype(jnp.bfloat16)
    return np.stack([high, low])


def real_form(points):
    product = np.outer(np.arange(points), np.arange(points)) % points
    angle = 2.0 * np.pi / points * product
    c, s = np.cos(angle), np.sin(angle)
    return pair(np.block([[c, -s], [s, c]])), pair(np.block([[c, s], [-s, c]]))


def twiddles(length, radix):
    points = length // radix
    angle = 2.0 * np.pi / length * np.outer(np.arange(radix), np.arange(points))
    return np.stack([np.cos(angle), -np.sin(angle)], axis=1).astype(np.float32)


def split(x):
    high = x.astype(jnp.bfloat16)
    return high, (x - high.astype(jnp.float32)).astype(jnp.bfloat16)


def dot(a, b):
    return jnp.dot(a, b, preferred_element_type=jnp.float32)


def times_table(x, table):
    high, low = split(x)
    return dot(high, table[0]) + dot(low, table[0]) + dot(high, table[1])


def table_times(table, x):
    high, low = split(x)
    return dot(table[0], high) + dot(table[0], low) + dot(table[1], high)


def scaled(value, factor):
    if value is None or factor == 0.0:
        return None
    if factor == 1.0:
        return value
    return -value if factor == -1.0 else value * factor


def plus(a, b):
    if a is None:
        return b
    return a if b is None else a + b


def small_transform(parts, sign):
    radix = len(parts)
    if radix == 1:
        return parts
    if radix % 2 == 0:
        half = radix // 2
        even = small_transform(parts[0::2], sign)
        odd = small_transform(parts[1::2], sign)
        first, second = [], []
        for r in range(half):
            angle = sign * 2.0 * np.pi * r / radix
            c, s = float(np.round(np.cos(angle), 15)), float(np.round(np.sin(angle), 15))
            ore, oim = odd[r]
            tre = plus(scaled(ore, c), scaled(oim, -s))
            tim = plus(scaled(oim, c), scaled(ore, s))
            ere, eim = even[r]
            first.append((ere + tre, eim + tim))
            second.append((ere - tre, eim - tim))
        return first + second
    raise ValueError("radix")


def turn(part, factor, conjugate):
    re, im = part
    fre, fim = factor
    if conjugate:
        return re * fre + im * fim, im * fre - re * fim
    return re * fre - im * fim, im * fre + re * fim


def rows_of(parts):
    return jnp.concatenate([jnp.concatenate(part, axis=1) for part in parts], axis=0)


def row_forward(cells, tw, table):
    stacked = []
    for parts in cells:
        for r, part in enumerate(small_transform(parts, -1.0)):
            factor = (tw[r, 0:1], tw[r, 1:2])
            stacked.append(part if r == 0 else turn(part, factor, False))
    return times_table(rows_of(stacked), table)


def row_inverse(ref, tw, table, radix, planes):
    rows, points = ref.shape[2], ref.shape[3]
    count = planes * radix
    stacked = jnp.concatenate(
        [ref[:, 0].reshape(count * rows, points), ref[:, 1].reshape(count * rows, points)], axis=1
    )
    out = times_table(stacked, table)
    cells = []
    for p in range(planes):
        parts = []
        for r in range(radix):
            at = (p * radix + r) * rows
            part = (out[at : at + rows, :points], out[at : at + rows, points:])
            parts.append(part if r == 0 else turn(part, (tw[r, 0:1], tw[r, 1:2]), True))
        cells.append(small_transform(parts, 1.0))
    return cells


def store_blocks(out_ref, value, count, rows, points):
    out_ref[:, 0] = value[:, :points].reshape(count, rows, points)
    out_ref[:, 1] = value[:, points:].reshape(count, rows, points)


def first_kernel(radix, planes_ref, tw_ref, table_ref, *rest):
    out_refs, (loaded, tw, table, held, sems) = rest[:-5], rest[-5:]
    freqs, _, rows, length = loaded.shape
    points = length // radix
    core = lax.axis_index("depth")
    copies = [
        pltpu.make_async_copy(planes_ref.at[f, pl.ds(2 * core, 2)], loaded.at[f], sems.at[f])
        for f in range(freqs)
    ]
    constants = [
        pltpu.make_async_copy(table_ref, table, sems.at[freqs]),
        pltpu.make_async_copy(tw_ref, tw, sems.at[freqs + 1]),
    ]
    for copy in copies + constants:
        copy.start()
    for copy in constants:
        copy.wait()
    for f, copy in enumerate(copies):
        copy.wait()
        parts = [
            tuple(loaded[f, i, :, m * points : (m + 1) * points] for i in range(2)) for m in range(radix)
        ]
        value = row_forward([parts], tw, table)
        at = slice(f * radix, (f + 1) * radix)
        held[at, 0] = value[:, :points].reshape(radix, rows, points)
        held[at, 1] = value[:, points:].reshape(radix, rows, points)
    spread(held, out_refs, lax.axis_index("row"))


def residue_of():
    return lax.rem(lax.axis_index("row"), lax.axis_size("row") // 2)


def frequency_of():
    return lax.axis_index("row") // (lax.axis_size("row") // 2)


def spread(held, out_refs, own):
    for step, ref in enumerate(out_refs):
        ref[...] = held[own ^ step]


def collect(in_refs, held, own):
    for step, ref in enumerate(in_refs):
        held[own ^ step] = ref[...]


def quarter_place(block, ranks):
    return block % (ranks // 2), block // (ranks // 2)


class Blocks:
    def __init__(self, ref, ranks, rows):
        self.ref, self.ranks, self.rows = ref, ranks, rows

    def at(self, block, part):
        return block, part


class Quarters(Blocks):
    def at(self, block, part):
        quarter, half = quarter_place(block, self.ranks)
        return quarter, part, slice(half * self.rows, (half + 1) * self.rows)


def columns_to_quarters(col_radix, ranks, *refs):
    in_refs, (hre, him, tw, forward, inverse), rest = refs[:ranks], refs[ranks : ranks + 5], refs[ranks + 5 :]
    out_refs, (blocks, quarters) = rest[:-2], rest[-2:]
    rows = blocks.shape[2]
    collect(in_refs, blocks, lax.axis_index("row"))
    source, target = Blocks(blocks, ranks, rows), Quarters(quarters, ranks, rows)
    column_kernel(col_radix, source, hre, him, tw, forward, inverse, target)
    spread(quarters, out_refs, residue_of())


def quarters_to_columns(col_radix, radix, *refs):
    in_refs, (hre, him, tw, forward, inverse), rest = refs[:radix], refs[radix : radix + 5], refs[radix + 5 :]
    out_refs, (blocks, quarters) = rest[:-2], rest[-2:]
    ranks, rows = blocks.shape[0], blocks.shape[2]
    collect(in_refs, quarters, residue_of())
    source, target = Quarters(quarters, ranks, rows), Blocks(blocks, ranks, rows)
    column_kernel(col_radix, source, hre, him, tw, forward, inverse, target)
    spread(blocks, out_refs, lax.axis_index("row"))


def column_kernel(radix, source, hre, him, tw, forward, inverse, target):
    points, width = hre.shape[1], hre.shape[2]
    rows = source.rows
    per = points // rows

    def block(m, part):
        pieces = [source.ref[source.at(m * per + i, part)] for i in range(per)]
        return jnp.concatenate(pieces, axis=0)

    parts = small_transform([(block(m, 0), block(m, 1)) for m in range(radix)], -1.0)
    columns = []
    for r, part in enumerate(parts):
        if r > 0:
            factor = (tw[:, 2 * r : 2 * r + 1], tw[:, 2 * r + 1 : 2 * r + 2])
            part = turn(part, factor, False)
        columns.append(jnp.concatenate(part, axis=0))
    spectrum = table_times(forward, jnp.concatenate(columns, axis=1))
    columns = []
    for r in range(radix):
        at = slice(r * width, (r + 1) * width)
        part = turn((spectrum[:points, at], spectrum[points:, at]), (hre[r], him[r]), False)
        columns.append(jnp.concatenate(part, axis=0))
    back = table_times(inverse, jnp.concatenate(columns, axis=1))
    parts = []
    for r in range(radix):
        at = slice(r * width, (r + 1) * width)
        part = (back[:points, at], back[points:, at])
        if r > 0:
            factor = (tw[:, 2 * r : 2 * r + 1], tw[:, 2 * r + 1 : 2 * r + 2])
            part = turn(part, factor, True)
        parts.append(part)
    for m, (re, im) in enumerate(small_transform(parts, 1.0)):
        for i in range(per):
            at = slice(i * rows, (i + 1) * rows)
            target.ref[target.at(m * per + i, 0)] = re[at]
            target.ref[target.at(m * per + i, 1)] = im[at]


def middle_kernel(radix, *refs):
    in_refs, refs = refs[:radix], refs[radix:]
    (own_cos, own_sin, far_cos, far_sin, tw, inverse, forward), refs = refs[:7], refs[7:]
    out_refs, (keep_ref, send_ref, held, field, screen) = refs[:radix], refs[radix:]
    rows, points = held.shape[2], held.shape[3]
    mine = frequency_of()
    for half, pair_refs in ((mine, (own_cos, own_sin)), (1 - mine, (far_cos, far_sin))):
        for i, ref in enumerate(pair_refs):
            screen[i, half] = ref[...]
    collect(in_refs, held, residue_of())
    (cells,) = row_inverse(held, tw, inverse, radix, 1)
    turned = []
    for m in range(radix):
        at = slice(m * points, (m + 1) * points)
        factor = [screen[i, :, :, at].reshape(rows, points) for i in range(2)]
        part = turn(cells[m], factor, False)
        for half in range(2):
            for i in range(2):
                field[half, i, :, at] = part[i][half * rows // 2 : (half + 1) * rows // 2]
        turned.append(part)
    kept = mine ^ lax.axis_index("depth")
    keep_ref[...] = field[kept]
    send_ref[...] = field[1 - kept]
    value = row_forward([turned], tw, forward)
    store_blocks(held, value, radix, rows, points)
    spread(held, out_refs, residue_of())


def column_kernel(radix, source, hre, him, tw, forward, inverse, target):
    points, width = hre.shape[1], hre.shape[2]
    rows = source.rows
    per = points // rows

    def block(m, part):
        pieces = [source.ref[source.at(m * per + i, part)] for i in range(per)]
        return jnp.concatenate(pieces, axis=0)

    parts = small_transform([(block(m, 0), block(m, 1)) for m in range(radix)], -1.0)
    columns = []
    for r, part in enumerate(parts):
        if r > 0:
            factor = (tw[:, 2 * r : 2 * r + 1], tw[:, 2 * r + 1 : 2 * r + 2])
            part = turn(part, factor, False)
        columns.append(jnp.concatenate(part, axis=0))
    spectrum = table_times(forward, jnp.concatenate(columns, axis=1))
    columns = []
    for r in range(radix):
        at = slice(r * width, (r + 1) * width)
        part = turn((spectrum[:points, at], spectrum[points:, at]), (hre[r], him[r]), False)
        columns.append(jnp.concatenate(part, axis=0))
    back = table_times(inverse, jnp.concatenate(columns, axis=1))
    parts = []
    for r in range(radix):
        at = slice(r * width, (r + 1) * width)
        part = (back[:points, at], back[points:, at])
        if r > 0:
            factor = (tw[:, 2 * r : 2 * r + 1], tw[:, 2 * r + 1 : 2 * r + 2])
            part = turn(part, factor, True)
        parts.append(part)
    for m, (re, im) in enumerate(small_transform(parts, 1.0)):
        for i in range(per):
            at = slice(i * rows, (i + 1) * rows)
            target.ref[target.at(m * per + i, 0)] = re[at]
            target.ref[target.at(m * per + i, 1)] = im[at]


def last_kernel(radix, ranks, *refs):
    in_refs, screens, (tw, inverse, out_ref, held) = refs[:ranks], refs[ranks : ranks + 4], refs[ranks + 4 :]
    points = held.shape[3]
    collect(in_refs, held, lax.axis_index("row"))
    for f, parts in enumerate(row_inverse(held, tw, inverse, radix, 2)):
        for m, part in enumerate(parts):
            at = slice(m * points, (m + 1) * points)
            factor = (screens[2 * f][:, at], screens[2 * f + 1][:, at])
            re, im = turn(part, factor, False)
            out_ref[f, 0, :, at] = re
            out_ref[f, 1, :, at] = im


def output_kernel(own_ref, got_ref, share_ref, more_ref, image_ref, leaving_ref):
    for core, (source, receiver) in enumerate(((own_ref, got_ref), (got_ref, own_ref))):

        @pl.when(lax.axis_index("depth") == core)
        def _():
            leaving_ref[0, 0:2] = source[core]
            leaving_ref[0, 2:4] = receiver[core]
            if core == 0:
                image_ref[0] = share_ref[...] + more_ref[...]
            else:
                terms = [source[f, i] * receiver[f, i] for f in range(2) for i in range(2)]
                image_ref[0] = (terms[0] + terms[1]) + (terms[2] + terms[3])


def signed_wave(positions, length):
    signed = jnp.where(positions < length // 2, positions, positions - length)
    return 2.0 * jnp.pi / length * signed.astype(jnp.float32)


def cos_sin(x):
    turns = jnp.floor(x * (2.0 / np.pi) + 0.5)
    rest = ((x - turns * 1.5703125) - turns * 4.837512969970703e-04) - turns * 7.549789948768648e-08
    square = rest * rest
    sine = 2.75573192e-06 - 2.50521084e-08 * square
    sine = -1.98412698e-04 + square * sine
    sine = 8.33333333e-03 + square * sine
    sine = -1.66666667e-01 + square * sine
    sine = rest + rest * square * sine
    cosine = -2.75573192e-07 + 2.08767570e-09 * square
    cosine = 2.48015873e-05 + square * cosine
    cosine = -1.38888889e-03 + square * cosine
    cosine = 4.16666667e-02 + square * cosine
    cosine = 1.0 - 0.5 * square + square * square * cosine
    count = turns.astype(jnp.int32)
    odd = (count & 1) == 1
    new_cos, new_sin = jnp.where(odd, sine, cosine), jnp.where(odd, cosine, sine)
    new_cos = jnp.where(((count + 1) & 2) == 2, -new_cos, new_cos)
    new_sin = jnp.where((count & 2) == 2, -new_sin, new_sin)
    return new_cos, new_sin


def omegas_of(freq_ref):
    omegas = [omega_step * freq_ref[f].astype(jnp.float32) for f in range(2)]
    return omegas, jnp.where(frequency_of() == 0, omegas[0], omegas[1])


def core_sign():
    return jnp.where(lax.axis_index("depth") == 0, -1.0, 1.0)


def propagator(radix, level, freq_ref, ref_ref, hre, him):
    col_radix, points, width = hre.shape
    length = col_radix * points
    _, omega = omegas_of(freq_ref)
    scale = 1.0 / (length * length)
    row_at = lax.broadcasted_iota(jnp.int32, (1, width), 1) * radix + residue_of()
    row_square = signed_wave(row_at, length) ** 2
    for r in range(col_radix):
        col_at = lax.broadcasted_iota(jnp.int32, (points, width), 0) * col_radix + r
        radicand = (omega * ref_ref[level]) ** 2 - (signed_wave(col_at, length) ** 2 + row_square)
        vertical = jnp.sqrt(jnp.maximum(radicand, 0.0)) * depth_step
        damping = scale * jnp.exp(-jnp.sqrt(jnp.maximum(-radicand, 0.0)) * depth_step)
        cosine, sine = cos_sin(vertical)
        hre[r], him[r] = damping * cosine, core_sign() * damping * sine


def screen(slow, slow_ref, omega, cos_ref, sin_ref):
    cosine, sine = cos_sin(omega * (slow - slow_ref) * depth_step)
    cos_ref[...], sin_ref[...] = cosine, core_sign() * sine


def factors_a(radix, freq_ref, ref_ref, tw_ref, tw_out, hre, him):
    tw_out[...] = tw_ref[...]
    propagator(radix, 0, freq_ref, ref_ref, hre, him)


def factors_b(radix, freq_ref, ref_ref, slow_ref, other_ref, far_ref, sent_ref, hre, him, *outs):
    first = lax.axis_index("depth") == 0
    _, omega = omegas_of(freq_ref)
    propagator(radix, 1, freq_ref, ref_ref, hre, him)
    screen(jnp.where(first, slow_ref[0], other_ref[0]), ref_ref[0], omega, *outs[:2])
    screen(jnp.where(first, far_ref[...], sent_ref[...]), ref_ref[0], omega, *outs[2:])


def factors_c(freq_ref, ref_ref, slow_ref, other_ref, keep_ref, got_ref, share_ref, *outs):
    last = jnp.where(lax.axis_index("depth") == 0, other_ref[0], slow_ref[0])
    omegas, _ = omegas_of(freq_ref)
    share_ref[...] = keep_ref[0] * got_ref[0] + keep_ref[1] * got_ref[1]
    for f in range(2):
        screen(last, ref_ref[1], omegas[f], *outs[2 * f : 2 * f + 2])


def call(kernel, out_shapes, scratch, args, held=True, scalars=()):
    vmem = pl.BlockSpec(memory_space=pltpu.VMEM)
    smem = pl.BlockSpec(memory_space=pltpu.SMEM)
    shape = pltpu.VMEM if held else jax.ShapeDtypeStruct
    return pl.pallas_call(
        kernel,
        in_specs=[smem] * len(scalars) + [vmem] * len(args),
        out_specs=[vmem] * len(out_shapes),
        out_shape=[shape(s, jnp.float32) for s in out_shapes],
        scratch_shapes=[pltpu.VMEM(s, jnp.float32) for s in scratch],
        compiler_params=pltpu.CompilerParams(vmem_limit_bytes=kernel_vmem),
    )(*scalars, *[pltpu.with_memory_space_constraint(a, pltpu.VMEM) for a in args])


def shards(planes, slowness, ref_slowness, freq_index):
    freqs, _, rows, length = planes.shape
    ranks = lax.axis_size("row")
    radix = ranks // 2
    points = length // radix
    col_radix = length // lanes

    row_forward_table, row_inverse_table = real_form(points)
    col_inverse_table, col_forward_table = real_form(lanes)
    row_tw = twiddles(length, radix)
    col_tw = twiddles(length, col_radix).transpose(2, 0, 1).reshape(lanes, 2 * col_radix)
    swap = [(0, 1), (1, 0)]
    both = ("depth", "row")

    def flat(c, r):
        return c * ranks + r

    def hop(array, step):
        return lax.ppermute(array, "row", [(r, r ^ step) for r in range(ranks)])

    def exchange(arrays, steps):
        got = list(arrays)
        for step in steps:
            got[step] = hop(arrays[step], step)
        return got

    inner_steps = list(range(1, radix))
    outer_steps = list(range(radix, ranks)) + list(range(1, radix))

    blocks = (ranks, 2, rows, points)
    quarter = (2, 2 * rows, points)
    half_field = (2, rows, length)
    vmem, hbm = (pl.BlockSpec(memory_space=space) for space in (pltpu.VMEM, pl.ANY))
    spectra = pl.pallas_call(
        functools.partial(first_kernel, radix),
        in_specs=[hbm] * 3,
        out_specs=[vmem] * ranks,
        out_shape=[pltpu.VMEM(blocks[1:], jnp.float32)] * ranks,
        scratch_shapes=[
            pltpu.VMEM((freqs,) + half_field, jnp.float32),
            pltpu.VMEM(row_tw.shape, jnp.float32),
            pltpu.VMEM(row_forward_table.shape, jnp.bfloat16),
            pltpu.VMEM(blocks, jnp.float32),
            pltpu.SemaphoreType.DMA((freqs + 2,)),
        ],
    )(planes, row_tw, row_forward_table)
    plane = (rows, length)
    factor = (col_radix, lanes, points)
    scalars = (freq_index, ref_slowness)
    held_tw, *propagator_a = call(
        functools.partial(factors_a, radix),
        [row_tw.shape] + [factor] * 2,
        [],
        (row_tw,),
        scalars=scalars,
    )
    far = lax.ppermute(slowness[0], both, [(flat(0, r), flat(0, r ^ radix)) for r in range(ranks)])
    other = lax.ppermute(slowness, "depth", swap)
    sent = lax.ppermute(far, "depth", [(0, 1)])
    factors = call(
        functools.partial(factors_b, radix),
        [factor] * 2 + [plane] * 4,
        [],
        (slowness, other, far, sent),
        scalars=scalars,
    )
    propagator_b, screens_a = factors[:2], factors[2:]
    columns = exchange(spectra, outer_steps)
    quarters = call(
        functools.partial(columns_to_quarters, col_radix, ranks),
        [quarter] * radix,
        [blocks, (radix,) + quarter],
        (*columns, *propagator_a, col_tw, col_forward_table, col_inverse_table),
    )
    quarters = exchange(quarters, inner_steps)
    *quarters, keep, send = call(
        functools.partial(middle_kernel, radix),
        [quarter] * radix + [half_field] * 2,
        [(radix,) + quarter, (2,) + half_field, (2,) + half_field],
        (*quarters, *screens_a, held_tw, row_inverse_table, row_forward_table),
    )
    quarters = exchange(quarters, inner_steps)
    got = lax.ppermute(send, "depth", swap)
    share, *screens_b = call(
        factors_c, [plane] * 5, [], (slowness, other, keep, got), scalars=scalars
    )
    more = lax.ppermute(share, both, [(flat(1, r), flat(0, r ^ radix)) for r in range(ranks)])
    columns = call(
        functools.partial(quarters_to_columns, col_radix, radix),
        [blocks[1:]] * ranks,
        [blocks, (radix,) + quarter],
        (*quarters, *propagator_b, col_tw, col_forward_table, col_inverse_table),
    )
    cells = exchange(columns, outer_steps)
    (fields,) = call(
        functools.partial(last_kernel, radix, ranks),
        [(freqs,) + half_field],
        [blocks],
        (*cells, *screens_b, held_tw, row_inverse_table),
    )
    swapped = lax.ppermute(fields, "depth", swap)
    image, leaving = call(
        output_kernel,
        [(1, rows, length), (1,) + planes.shape[1:]],
        [],
        (fields, swapped, share, more),
        held=False,
    )
    return image, leaving


def solution(mesh):
    in_specs = (P("groups", None, "row", None), P("depth", "row", None), P(), P())
    out_specs = (P(("groups", "depth"), "row", None), P(("groups", "depth"), None, "row", None))
    return jax.shard_map(shards, mesh=mesh, in_specs=in_specs, out_specs=out_specs, check_vma=False)
```

```python
import functools

import jax
import jax.numpy as jnp
import numpy as np
from jax import lax
from jax.experimental import pallas as pl
from jax.experimental.pallas import tpu as pltpu
from jax.sharding import PartitionSpec as P


omega_step = 0.05
depth_step = 1.0
lanes = 128
kernel_vmem = 24 << 20


def pair(table):
    high = table.astype(jnp.bfloat16)
    low = (table - high.astype(np.float64)).astype(jnp.bfloat16)
    return np.stack([high, low])


def real_form(points):
    product = np.outer(np.arange(points), np.arange(points)) % points
    angle = 2.0 * np.pi / points * product
    c, s = np.cos(angle), np.sin(angle)
    return pair(np.block([[c, -s], [s, c]])), pair(np.block([[c, s], [-s, c]]))


def twiddles(length, radix):
    points = length // radix
    angle = 2.0 * np.pi / length * np.outer(np.arange(radix), np.arange(points))
    return np.stack([np.cos(angle), -np.sin(angle)], axis=1).astype(np.float32)


def split(x):
    high = x.astype(jnp.bfloat16)
    return high, (x - high.astype(jnp.float32)).astype(jnp.bfloat16)


def dot(a, b):
    return jnp.dot(a, b, preferred_element_type=jnp.float32)


def times_table(x, table):
    high, low = split(x)
    return dot(high, table[0]) + dot(low, table[0]) + dot(high, table[1])


def table_times(table, x):
    high, low = split(x)
    return dot(table[0], high) + dot(table[0], low) + dot(table[1], high)


def scaled(value, factor):
    if value is None or factor == 0.0:
        return None
    if factor == 1.0:
        return value
    return -value if factor == -1.0 else value * factor


def plus(a, b):
    if a is None:
        return b
    return a if b is None else a + b


def small_transform(parts, sign):
    radix = len(parts)
    if radix == 1:
        return parts
    if radix % 2 == 0:
        half = radix // 2
        even = small_transform(parts[0::2], sign)
        odd = small_transform(parts[1::2], sign)
        first, second = [], []
        for r in range(half):
            angle = sign * 2.0 * np.pi * r / radix
            c, s = float(np.round(np.cos(angle), 15)), float(np.round(np.sin(angle), 15))
            ore, oim = odd[r]
            tre = plus(scaled(ore, c), scaled(oim, -s))
            tim = plus(scaled(oim, c), scaled(ore, s))
            ere, eim = even[r]
            first.append((ere + tre, eim + tim))
            second.append((ere - tre, eim - tim))
        return first + second
    raise ValueError("radix")


def turn(part, factor, conjugate):
    re, im = part
    fre, fim = factor
    if conjugate:
        return re * fre + im * fim, im * fre - re * fim
    return re * fre - im * fim, im * fre + re * fim


def rows_of(parts):
    return jnp.concatenate([jnp.concatenate(part, axis=1) for part in parts], axis=0)


def row_forward(cells, tw, table):
    stacked = []
    for parts in cells:
        for r, part in enumerate(small_transform(parts, -1.0)):
            factor = (tw[r, 0:1], tw[r, 1:2])
            stacked.append(part if r == 0 else turn(part, factor, False))
    return times_table(rows_of(stacked), table)


def row_inverse(ref, tw, table, radix, planes):
    rows, points = ref.shape[2], ref.shape[3]
    count = planes * radix
    stacked = jnp.concatenate(
        [ref[:, 0].reshape(count * rows, points), ref[:, 1].reshape(count * rows, points)], axis=1
    )
    out = times_table(stacked, table)
    cells = []
    for p in range(planes):
        parts = []
        for r in range(radix):
            at = (p * radix + r) * rows
            part = (out[at : at + rows, :points], out[at : at + rows, points:])
            parts.append(part if r == 0 else turn(part, (tw[r, 0:1], tw[r, 1:2]), True))
        cells.append(small_transform(parts, 1.0))
    return cells


def store_blocks(out_ref, value, count, rows, points):
    out_ref[:, 0] = value[:, :points].reshape(count, rows, points)
    out_ref[:, 1] = value[:, points:].reshape(count, rows, points)


def first_kernel(radix, planes_ref, tw_ref, table_ref, *rest):
    out_refs, (loaded, tw, table, held, sems) = rest[:-5], rest[-5:]
    freqs, _, rows, length = loaded.shape
    points = length // radix
    core = lax.axis_index("depth")
    copies = [
        pltpu.make_async_copy(planes_ref.at[f, pl.ds(2 * core, 2)], loaded.at[f], sems.at[f])
        for f in range(freqs)
    ]
    constants = [
        pltpu.make_async_copy(table_ref, table, sems.at[freqs]),
        pltpu.make_async_copy(tw_ref, tw, sems.at[freqs + 1]),
    ]
    for copy in copies + constants:
        copy.start()
    for copy in constants:
        copy.wait()
    for f, copy in enumerate(copies):
        copy.wait()
        parts = [
            tuple(loaded[f, i, :, m * points : (m + 1) * points] for i in range(2)) for m in range(radix)
        ]
        value = row_forward([parts], tw, table)
        at = slice(f * radix, (f + 1) * radix)
        held[at, 0] = value[:, :points].reshape(radix, rows, points)
        held[at, 1] = value[:, points:].reshape(radix, rows, points)
    spread(held, out_refs, lax.axis_index("row"))


def residue_of():
    return lax.rem(lax.axis_index("row"), lax.axis_size("row") // 2)


def frequency_of():
    return lax.axis_index("row") // (lax.axis_size("row") // 2)


def spread(held, out_refs, own):
    for step, ref in enumerate(out_refs):
        ref[...] = held[own ^ step]


def collect(in_refs, held, own):
    for step, ref in enumerate(in_refs):
        held[own ^ step] = ref[...]


def quarter_place(block, ranks):
    return block % (ranks // 2), block // (ranks // 2)


class Blocks:
    def __init__(self, ref, ranks, rows):
        self.ref, self.ranks, self.rows = ref, ranks, rows

    def at(self, block, part):
        return block, part


class Quarters(Blocks):
    def at(self, block, part):
        quarter, half = quarter_place(block, self.ranks)
        return quarter, part, slice(half * self.rows, (half + 1) * self.rows)


def columns_to_quarters(col_radix, ranks, *refs):
    in_refs, (hre, him, tw, forward, inverse), rest = refs[:ranks], refs[ranks : ranks + 5], refs[ranks + 5 :]
    out_refs, (blocks, quarters) = rest[:-2], rest[-2:]
    rows = blocks.shape[2]
    collect(in_refs, blocks, lax.axis_index("row"))
    source, target = Blocks(blocks, ranks, rows), Quarters(quarters, ranks, rows)
    column_kernel(col_radix, source, hre, him, tw, forward, inverse, target)
    spread(quarters, out_refs, residue_of())


def quarters_to_columns(col_radix, radix, *refs):
    in_refs, (hre, him, tw, forward, inverse), rest = refs[:radix], refs[radix : radix + 5], refs[radix + 5 :]
    out_refs, (blocks, quarters) = rest[:-2], rest[-2:]
    ranks, rows = blocks.shape[0], blocks.shape[2]
    collect(in_refs, quarters, residue_of())
    source, target = Quarters(quarters, ranks, rows), Blocks(blocks, ranks, rows)
    column_kernel(col_radix, source, hre, him, tw, forward, inverse, target)
    spread(blocks, out_refs, lax.axis_index("row"))


def column_kernel(radix, source, hre, him, tw, forward, inverse, target):
    points, width = hre.shape[1], hre.shape[2]
    rows = source.rows
    per = points // rows

    def block(m, part):
        pieces = [source.ref[source.at(m * per + i, part)] for i in range(per)]
        return jnp.concatenate(pieces, axis=0)

    parts = small_transform([(block(m, 0), block(m, 1)) for m in range(radix)], -1.0)
    columns = []
    for r, part in enumerate(parts):
        if r > 0:
            factor = (tw[:, 2 * r : 2 * r + 1], tw[:, 2 * r + 1 : 2 * r + 2])
            part = turn(part, factor, False)
        columns.append(jnp.concatenate(part, axis=0))
    spectrum = table_times(forward, jnp.concatenate(columns, axis=1))
    columns = []
    for r in range(radix):
        at = slice(r * width, (r + 1) * width)
        part = turn((spectrum[:points, at], spectrum[points:, at]), (hre[r], him[r]), False)
        columns.append(jnp.concatenate(part, axis=0))
    back = table_times(inverse, jnp.concatenate(columns, axis=1))
    parts = []
    for r in range(radix):
        at = slice(r * width, (r + 1) * width)
        part = (back[:points, at], back[points:, at])
        if r > 0:
            factor = (tw[:, 2 * r : 2 * r + 1], tw[:, 2 * r + 1 : 2 * r + 2])
            part = turn(part, factor, True)
        parts.append(part)
    for m, (re, im) in enumerate(small_transform(parts, 1.0)):
        for i in range(per):
            at = slice(i * rows, (i + 1) * rows)
            target.ref[target.at(m * per + i, 0)] = re[at]
            target.ref[target.at(m * per + i, 1)] = im[at]


def middle_kernel(radix, *refs):
    in_refs, refs = refs[:radix], refs[radix:]
    (own_cos, own_sin, far_cos, far_sin, tw, inverse, forward), refs = refs[:7], refs[7:]
    out_refs, (keep_ref, send_ref, held, field, screen) = refs[:radix], refs[radix:]
    rows, points = held.shape[2], held.shape[3]
    mine = frequency_of()
    for half, pair_refs in ((mine, (own_cos, own_sin)), (1 - mine, (far_cos, far_sin))):
        for i, ref in enumerate(pair_refs):
            screen[i, half] = ref[...]
    collect(in_refs, held, residue_of())
    (cells,) = row_inverse(held, tw, inverse, radix, 1)
    turned = []
    for m in range(radix):
        at = slice(m * points, (m + 1) * points)
        factor = [screen[i, :, :, at].reshape(rows, points) for i in range(2)]
        part = turn(cells[m], factor, False)
        for half in range(2):
            for i in range(2):
                field[half, i, :, at] = part[i][half * rows // 2 : (half + 1) * rows // 2]
        turned.append(part)
    kept = mine ^ lax.axis_index("depth") ^ 1
    keep_ref[...] = field[kept]
    send_ref[...] = field[1 - kept]
    value = row_forward([turned], tw, forward)
    store_blocks(held, value, radix, rows, points)
    spread(held, out_refs, residue_of())


def column_kernel(radix, source, hre, him, tw, forward, inverse, target):
    points, width = hre.shape[1], hre.shape[2]
    rows = source.rows
    per = points // rows

    def block(m, part):
        pieces = [source.ref[source.at(m * per + i, part)] for i in range(per)]
        return jnp.concatenate(pieces, axis=0)

    parts = small_transform([(block(m, 0), block(m, 1)) for m in range(radix)], -1.0)
    columns = []
    for r, part in enumerate(parts):
        if r > 0:
            factor = (tw[:, 2 * r : 2 * r + 1], tw[:, 2 * r + 1 : 2 * r + 2])
            part = turn(part, factor, False)
        columns.append(jnp.concatenate(part, axis=0))
    spectrum = table_times(forward, jnp.concatenate(columns, axis=1))
    columns = []
    for r in range(radix):
        at = slice(r * width, (r + 1) * width)
        part = turn((spectrum[:points, at], spectrum[points:, at]), (hre[r], him[r]), False)
        columns.append(jnp.concatenate(part, axis=0))
    back = table_times(inverse, jnp.concatenate(columns, axis=1))
    parts = []
    for r in range(radix):
        at = slice(r * width, (r + 1) * width)
        part = (back[:points, at], back[points:, at])
        if r > 0:
            factor = (tw[:, 2 * r : 2 * r + 1], tw[:, 2 * r + 1 : 2 * r + 2])
            part = turn(part, factor, True)
        parts.append(part)
    for m, (re, im) in enumerate(small_transform(parts, 1.0)):
        for i in range(per):
            at = slice(i * rows, (i + 1) * rows)
            target.ref[target.at(m * per + i, 0)] = re[at]
            target.ref[target.at(m * per + i, 1)] = im[at]


def last_kernel(radix, ranks, *refs):
    in_refs, screens, refs = refs[:ranks], refs[ranks : ranks + 4], refs[ranks + 4 :]
    share_ref, tw, inverse, out_ref, held = refs
    points = held.shape[3]
    out_ref[4] = share_ref[...]
    collect(in_refs, held, lax.axis_index("row"))
    for f, parts in enumerate(row_inverse(held, tw, inverse, radix, 2)):
        for m, part in enumerate(parts):
            at = slice(m * points, (m + 1) * points)
            factor = (screens[2 * f][:, at], screens[2 * f + 1][:, at])
            re, im = turn(part, factor, False)
            out_ref[2 * f, :, at] = re
            out_ref[2 * f + 1, :, at] = im


def output_kernel(own_ref, got_ref, more_ref, image_ref, leaving_ref):
    for core, (source, receiver) in enumerate(((own_ref, got_ref), (got_ref, own_ref))):

        @pl.when(lax.axis_index("depth") == core)
        def _():
            leaving_ref[0, 0:2] = source[2 * core : 2 * core + 2]
            leaving_ref[0, 2:4] = receiver[2 * core : 2 * core + 2]
            if core == 0:
                image_ref[0] = got_ref[4] + more_ref[...]
            else:
                terms = [source[i] * receiver[i] for i in range(4)]
                image_ref[0] = (terms[0] + terms[1]) + (terms[2] + terms[3])


def signed_wave(positions, length):
    signed = jnp.where(positions < length // 2, positions, positions - length)
    return 2.0 * jnp.pi / length * signed.astype(jnp.float32)


def cos_sin(x):
    turns = jnp.floor(x * (2.0 / np.pi) + 0.5)
    rest = ((x - turns * 1.5703125) - turns * 4.837512969970703e-04) - turns * 7.549789948768648e-08
    square = rest * rest
    sine = 2.75573192e-06 - 2.50521084e-08 * square
    sine = -1.98412698e-04 + square * sine
    sine = 8.33333333e-03 + square * sine
    sine = -1.66666667e-01 + square * sine
    sine = rest + rest * square * sine
    cosine = -2.75573192e-07 + 2.08767570e-09 * square
    cosine = 2.48015873e-05 + square * cosine
    cosine = -1.38888889e-03 + square * cosine
    cosine = 4.16666667e-02 + square * cosine
    cosine = 1.0 - 0.5 * square + square * square * cosine
    count = turns.astype(jnp.int32)
    odd = (count & 1) == 1
    new_cos, new_sin = jnp.where(odd, sine, cosine), jnp.where(odd, cosine, sine)
    new_cos = jnp.where(((count + 1) & 2) == 2, -new_cos, new_cos)
    new_sin = jnp.where((count & 2) == 2, -new_sin, new_sin)
    return new_cos, new_sin


def omegas_of(freq_ref):
    omegas = [omega_step * freq_ref[f].astype(jnp.float32) for f in range(2)]
    return omegas, jnp.where(frequency_of() == 0, omegas[0], omegas[1])


def core_sign():
    return jnp.where(lax.axis_index("depth") == 0, -1.0, 1.0)


def propagator(radix, level, freq_ref, ref_ref, hre, him):
    col_radix, points, width = hre.shape
    length = col_radix * points
    _, omega = omegas_of(freq_ref)
    scale = 1.0 / (length * length)
    row_at = lax.broadcasted_iota(jnp.int32, (1, width), 1) * radix + residue_of()
    row_square = signed_wave(row_at, length) ** 2
    for r in range(col_radix):
        col_at = lax.broadcasted_iota(jnp.int32, (points, width), 0) * col_radix + r
        radicand = (omega * ref_ref[level]) ** 2 - (signed_wave(col_at, length) ** 2 + row_square)
        vertical = jnp.sqrt(jnp.maximum(radicand, 0.0)) * depth_step
        damping = scale * jnp.exp(-jnp.sqrt(jnp.maximum(-radicand, 0.0)) * depth_step)
        cosine, sine = cos_sin(vertical)
        hre[r], him[r] = damping * cosine, core_sign() * damping * sine


def screen(slow, slow_ref, omega, cos_ref, sin_ref):
    cosine, sine = cos_sin(omega * (slow - slow_ref) * depth_step)
    cos_ref[...], sin_ref[...] = cosine, core_sign() * sine


def factors_a(radix, freq_ref, ref_ref, tw_ref, tw_out, hre, him):
    tw_out[...] = tw_ref[...]
    propagator(radix, 0, freq_ref, ref_ref, hre, him)


def factors_b(freq_ref, ref_ref, slow_ref, other_ref, far_ref, sent_ref, *outs):
    first = lax.axis_index("depth") == 0
    _, omega = omegas_of(freq_ref)
    screen(jnp.where(first, slow_ref[0], other_ref[0]), ref_ref[0], omega, *outs[:2])
    screen(jnp.where(first, far_ref[...], sent_ref[...]), ref_ref[0], omega, *outs[2:])


def factors_c(radix, freq_ref, ref_ref, slow_ref, other_ref, keep_ref, got_ref, hre, him, share_ref, *outs):
    propagator(radix, 1, freq_ref, ref_ref, hre, him)
    last = jnp.where(lax.axis_index("depth") == 0, other_ref[0], slow_ref[0])
    omegas, _ = omegas_of(freq_ref)
    share_ref[...] = keep_ref[0] * got_ref[0] + keep_ref[1] * got_ref[1]
    for f in range(2):
        screen(last, ref_ref[1], omegas[f], *outs[2 * f : 2 * f + 2])


def call(kernel, out_shapes, scratch, args, held=True, scalars=()):
    vmem = pl.BlockSpec(memory_space=pltpu.VMEM)
    smem = pl.BlockSpec(memory_space=pltpu.SMEM)
    shape = pltpu.VMEM if held else jax.ShapeDtypeStruct
    return pl.pallas_call(
        kernel,
        in_specs=[smem] * len(scalars) + [vmem] * len(args),
        out_specs=[vmem] * len(out_shapes),
        out_shape=[shape(s, jnp.float32) for s in out_shapes],
        scratch_shapes=[pltpu.VMEM(s, jnp.float32) for s in scratch],
        compiler_params=pltpu.CompilerParams(vmem_limit_bytes=kernel_vmem),
    )(*scalars, *[pltpu.with_memory_space_constraint(a, pltpu.VMEM) for a in args])


def shards(planes, slowness, ref_slowness, freq_index):
    freqs, _, rows, length = planes.shape
    ranks = lax.axis_size("row")
    radix = ranks // 2
    points = length // radix
    col_radix = length // lanes

    row_forward_table, row_inverse_table = real_form(points)
    col_inverse_table, col_forward_table = real_form(lanes)
    row_tw = twiddles(length, radix)
    col_tw = twiddles(length, col_radix).transpose(2, 0, 1).reshape(lanes, 2 * col_radix)
    swap = [(0, 1), (1, 0)]
    both = ("depth", "row")

    def flat(c, r):
        return c * ranks + r

    def hop(array, step):
        return lax.ppermute(array, "row", [(r, r ^ step) for r in range(ranks)])

    def exchange(arrays, steps):
        got = list(arrays)
        for step in steps:
            got[step] = hop(arrays[step], step)
        return got

    inner_steps = list(range(1, radix))
    outer_steps = list(range(radix, ranks)) + list(range(1, radix))

    blocks = (ranks, 2, rows, points)
    quarter = (2, 2 * rows, points)
    half_field = (2, rows, length)
    vmem, hbm = (pl.BlockSpec(memory_space=space) for space in (pltpu.VMEM, pl.ANY))
    spectra = pl.pallas_call(
        functools.partial(first_kernel, radix),
        in_specs=[hbm] * 3,
        out_specs=[vmem] * ranks,
        out_shape=[pltpu.VMEM(blocks[1:], jnp.float32)] * ranks,
        scratch_shapes=[
            pltpu.VMEM((freqs,) + half_field, jnp.float32),
            pltpu.VMEM(row_tw.shape, jnp.float32),
            pltpu.VMEM(row_forward_table.shape, jnp.bfloat16),
            pltpu.VMEM(blocks, jnp.float32),
            pltpu.SemaphoreType.DMA((freqs + 2,)),
        ],
    )(planes, row_tw, row_forward_table)
    plane = (rows, length)
    factor = (col_radix, lanes, points)
    scalars = (freq_index, ref_slowness)
    held_tw, *propagator_a = call(
        functools.partial(factors_a, radix),
        [row_tw.shape] + [factor] * 2,
        [],
        (row_tw,),
        scalars=scalars,
    )
    far = lax.ppermute(slowness[0], both, [(flat(0, r), flat(0, r ^ radix)) for r in range(ranks)])
    other = lax.ppermute(slowness, "depth", swap)
    sent = lax.ppermute(far, "depth", [(0, 1)])
    screens_a = call(factors_b, [plane] * 4, [], (slowness, other, far, sent), scalars=scalars)
    columns = exchange(spectra, outer_steps)
    quarters = call(
        functools.partial(columns_to_quarters, col_radix, ranks),
        [quarter] * radix,
        [blocks, (radix,) + quarter],
        (*columns, *propagator_a, col_tw, col_forward_table, col_inverse_table),
    )
    quarters = exchange(quarters, inner_steps)
    *quarters, keep, send = call(
        functools.partial(middle_kernel, radix),
        [quarter] * radix + [half_field] * 2,
        [(radix,) + quarter, (2,) + half_field, (2,) + half_field],
        (*quarters, *screens_a, held_tw, row_inverse_table, row_forward_table),
    )
    quarters = exchange(quarters, inner_steps)
    got = lax.ppermute(send, "depth", swap)
    factors = call(
        functools.partial(factors_c, radix),
        [factor] * 2 + [plane] * 5,
        [],
        (slowness, other, keep, got),
        scalars=scalars,
    )
    propagator_b, share, screens_b = factors[:2], factors[2], factors[3:]
    more = lax.ppermute(share, both, [(flat(0, r), flat(0, r ^ radix)) for r in range(ranks)])
    columns = call(
        functools.partial(quarters_to_columns, col_radix, radix),
        [blocks[1:]] * ranks,
        [blocks, (radix,) + quarter],
        (*quarters, *propagator_b, col_tw, col_forward_table, col_inverse_table),
    )
    cells = exchange(columns, outer_steps)
    (fields,) = call(
        functools.partial(last_kernel, radix, ranks),
        [(2 * freqs + 1,) + plane],
        [blocks],
        (*cells, *screens_b, share, held_tw, row_inverse_table),
    )
    swapped = lax.ppermute(fields, "depth", swap)
    image, leaving = call(
        output_kernel,
        [(1, rows, length), (1,) + planes.shape[1:]],
        [],
        (fields, swapped, more),
        held=False,
    )
    return image, leaving


def solution(mesh):
    in_specs = (P("groups", None, "row", None), P("depth", "row", None), P(), P())
    out_specs = (P(("groups", "depth"), "row", None), P(("groups", "depth"), None, "row", None))
    return jax.shard_map(shards, mesh=mesh, in_specs=in_specs, out_specs=out_specs, check_vma=False)
```

```python
import functools

import jax
import jax.numpy as jnp
import numpy as np
from jax import lax
from jax.experimental import pallas as pl
from jax.experimental.pallas import tpu as pltpu
from jax.sharding import PartitionSpec as P


omega_step = 0.05
depth_step = 1.0
lanes = 128
kernel_vmem = 24 << 20


def pair(table):
    high = table.astype(jnp.bfloat16)
    low = (table - high.astype(np.float64)).astype(jnp.bfloat16)
    return np.stack([high, low])


def real_form(points):
    product = np.outer(np.arange(points), np.arange(points)) % points
    angle = 2.0 * np.pi / points * product
    c, s = np.cos(angle), np.sin(angle)
    return pair(np.block([[c, -s], [s, c]])), pair(np.block([[c, s], [-s, c]]))


def twiddles(length, radix):
    points = length // radix
    angle = 2.0 * np.pi / length * np.outer(np.arange(radix), np.arange(points))
    return np.stack([np.cos(angle), -np.sin(angle)], axis=1).astype(np.float32)


def split(x):
    high = x.astype(jnp.bfloat16)
    return high, (x - high.astype(jnp.float32)).astype(jnp.bfloat16)


def dot(a, b):
    return jnp.dot(a, b, preferred_element_type=jnp.float32)


def times_table(x, table):
    high, low = split(x)
    return dot(high, table[0]) + dot(low, table[0]) + dot(high, table[1])


def table_times(table, x):
    high, low = split(x)
    return dot(table[0], high) + dot(table[0], low) + dot(table[1], high)


def scaled(value, factor):
    if value is None or factor == 0.0:
        return None
    if factor == 1.0:
        return value
    return -value if factor == -1.0 else value * factor


def plus(a, b):
    if a is None:
        return b
    return a if b is None else a + b


def small_transform(parts, sign):
    radix = len(parts)
    if radix == 1:
        return parts
    if radix % 2 == 0:
        half = radix // 2
        even = small_transform(parts[0::2], sign)
        odd = small_transform(parts[1::2], sign)
        first, second = [], []
        for r in range(half):
            angle = sign * 2.0 * np.pi * r / radix
            c, s = float(np.round(np.cos(angle), 15)), float(np.round(np.sin(angle), 15))
            ore, oim = odd[r]
            tre = plus(scaled(ore, c), scaled(oim, -s))
            tim = plus(scaled(oim, c), scaled(ore, s))
            ere, eim = even[r]
            first.append((ere + tre, eim + tim))
            second.append((ere - tre, eim - tim))
        return first + second
    raise ValueError("radix")


def turn(part, factor, conjugate):
    re, im = part
    fre, fim = factor
    if conjugate:
        return re * fre + im * fim, im * fre - re * fim
    return re * fre - im * fim, im * fre + re * fim


def rows_of(parts):
    return jnp.concatenate([jnp.concatenate(part, axis=1) for part in parts], axis=0)


def row_forward(cells, tw, table):
    stacked = []
    for parts in cells:
        for r, part in enumerate(small_transform(parts, -1.0)):
            factor = (tw[r, 0:1], tw[r, 1:2])
            stacked.append(part if r == 0 else turn(part, factor, False))
    return times_table(rows_of(stacked), table)


def row_inverse(ref, tw, table, radix, planes):
    rows, points = ref.shape[2], ref.shape[3]
    count = planes * radix
    stacked = jnp.concatenate(
        [ref[:, 0].reshape(count * rows, points), ref[:, 1].reshape(count * rows, points)], axis=1
    )
    out = times_table(stacked, table)
    cells = []
    for p in range(planes):
        parts = []
        for r in range(radix):
            at = (p * radix + r) * rows
            part = (out[at : at + rows, :points], out[at : at + rows, points:])
            parts.append(part if r == 0 else turn(part, (tw[r, 0:1], tw[r, 1:2]), True))
        cells.append(small_transform(parts, 1.0))
    return cells


def store_blocks(out_ref, value, count, rows, points):
    out_ref[:, 0] = value[:, :points].reshape(count, rows, points)
    out_ref[:, 1] = value[:, points:].reshape(count, rows, points)


def first_kernel(radix, planes_ref, tw_ref, table_ref, *rest):
    out_refs, (loaded, tw, table, held, sems) = rest[:-5], rest[-5:]
    freqs, _, rows, length = loaded.shape
    points = length // radix
    core = lax.axis_index("depth")
    copies = [
        pltpu.make_async_copy(planes_ref.at[f, pl.ds(2 * core, 2)], loaded.at[f], sems.at[f])
        for f in range(freqs)
    ]
    constants = [
        pltpu.make_async_copy(table_ref, table, sems.at[freqs]),
        pltpu.make_async_copy(tw_ref, tw, sems.at[freqs + 1]),
    ]
    for copy in copies + constants:
        copy.start()
    for copy in constants:
        copy.wait()
    for f, copy in enumerate(copies):
        copy.wait()
        parts = [
            tuple(loaded[f, i, :, m * points : (m + 1) * points] for i in range(2)) for m in range(radix)
        ]
        value = row_forward([parts], tw, table)
        at = slice(f * radix, (f + 1) * radix)
        held[at, 0] = value[:, :points].reshape(radix, rows, points)
        held[at, 1] = value[:, points:].reshape(radix, rows, points)
    spread(held, out_refs, lax.axis_index("row"))


def residue_of():
    return lax.rem(lax.axis_index("row"), lax.axis_size("row") // 2)


def frequency_of():
    return lax.axis_index("row") // (lax.axis_size("row") // 2)


def spread(held, out_refs, own):
    for step, ref in enumerate(out_refs):
        ref[...] = held[own ^ step]


def collect(in_refs, held, own):
    for step, ref in enumerate(in_refs):
        held[own ^ step] = ref[...]


def quarter_place(block, ranks):
    return block % (ranks // 2), block // (ranks // 2)


class Blocks:
    def __init__(self, ref, ranks, rows):
        self.ref, self.ranks, self.rows = ref, ranks, rows

    def at(self, block, part):
        return block, part


class Quarters(Blocks):
    def at(self, block, part):
        quarter, half = quarter_place(block, self.ranks)
        return quarter, part, slice(half * self.rows, (half + 1) * self.rows)


def columns_to_quarters(col_radix, ranks, *refs):
    in_refs, (hre, him, tw, forward, inverse), rest = refs[:ranks], refs[ranks : ranks + 5], refs[ranks + 5 :]
    out_refs, (blocks, quarters) = rest[:-2], rest[-2:]
    rows = blocks.shape[2]
    collect(in_refs, blocks, lax.axis_index("row"))
    source, target = Blocks(blocks, ranks, rows), Quarters(quarters, ranks, rows)
    column_kernel(col_radix, source, hre, him, tw, forward, inverse, target)
    spread(quarters, out_refs, residue_of())


def quarters_to_columns(col_radix, radix, *refs):
    in_refs, (hre, him, tw, forward, inverse), rest = refs[:radix], refs[radix : radix + 5], refs[radix + 5 :]
    out_refs, (blocks, quarters) = rest[:-2], rest[-2:]
    ranks, rows = blocks.shape[0], blocks.shape[2]
    collect(in_refs, quarters, residue_of())
    source, target = Quarters(quarters, ranks, rows), Blocks(blocks, ranks, rows)
    column_kernel(col_radix, source, hre, him, tw, forward, inverse, target)
    spread(blocks, out_refs, lax.axis_index("row"))


def column_kernel(radix, source, hre, him, tw, forward, inverse, target):
    points, width = hre.shape[1], hre.shape[2]
    rows = source.rows
    per = points // rows

    def block(m, part):
        pieces = [source.ref[source.at(m * per + i, part)] for i in range(per)]
        return jnp.concatenate(pieces, axis=0)

    parts = small_transform([(block(m, 0), block(m, 1)) for m in range(radix)], -1.0)
    columns = []
    for r, part in enumerate(parts):
        if r > 0:
            factor = (tw[:, 2 * r : 2 * r + 1], tw[:, 2 * r + 1 : 2 * r + 2])
            part = turn(part, factor, False)
        columns.append(jnp.concatenate(part, axis=0))
    spectrum = table_times(forward, jnp.concatenate(columns, axis=1))
    columns = []
    for r in range(radix):
        at = slice(r * width, (r + 1) * width)
        part = turn((spectrum[:points, at], spectrum[points:, at]), (hre[r], him[r]), False)
        columns.append(jnp.concatenate(part, axis=0))
    back = table_times(inverse, jnp.concatenate(columns, axis=1))
    parts = []
    for r in range(radix):
        at = slice(r * width, (r + 1) * width)
        part = (back[:points, at], back[points:, at])
        if r > 0:
            factor = (tw[:, 2 * r : 2 * r + 1], tw[:, 2 * r + 1 : 2 * r + 2])
            part = turn(part, factor, True)
        parts.append(part)
    for m, (re, im) in enumerate(small_transform(parts, 1.0)):
        for i in range(per):
            at = slice(i * rows, (i + 1) * rows)
            target.ref[target.at(m * per + i, 0)] = re[at]
            target.ref[target.at(m * per + i, 1)] = im[at]


def middle_kernel(radix, *refs):
    in_refs, refs = refs[:radix], refs[radix:]
    (own_cos, own_sin, far_cos, far_sin, tw, inverse, forward), refs = refs[:7], refs[7:]
    out_refs, (keep_ref, send_ref, held, field, screen) = refs[:radix], refs[radix:]
    rows, points = held.shape[2], held.shape[3]
    mine = frequency_of()
    for half, pair_refs in ((mine, (own_cos, own_sin)), (1 - mine, (far_cos, far_sin))):
        for i, ref in enumerate(pair_refs):
            screen[i, half] = ref[...]
    collect(in_refs, held, residue_of())
    (cells,) = row_inverse(held, tw, inverse, radix, 1)
    turned = []
    for m in range(radix):
        at = slice(m * points, (m + 1) * points)
        factor = [screen[i, :, :, at].reshape(rows, points) for i in range(2)]
        part = turn(cells[m], factor, False)
        for half in range(2):
            for i in range(2):
                field[half, i, :, at] = part[i][half * rows // 2 : (half + 1) * rows // 2]
        turned.append(part)
    kept = mine ^ lax.axis_index("depth")
    keep_ref[...] = field[kept]
    send_ref[...] = field[1 - kept]
    value = row_forward([turned], tw, forward)
    store_blocks(held, value, radix, rows, points)
    spread(held, out_refs, residue_of())


def column_kernel(radix, source, hre, him, tw, forward, inverse, target):
    points, width = hre.shape[1], hre.shape[2]
    rows = source.rows
    per = points // rows

    def block(m, part):
        pieces = [source.ref[source.at(m * per + i, part)] for i in range(per)]
        return jnp.concatenate(pieces, axis=0)

    parts = small_transform([(block(m, 0), block(m, 1)) for m in range(radix)], -1.0)
    columns = []
    for r, part in enumerate(parts):
        if r > 0:
            factor = (tw[:, 2 * r : 2 * r + 1], tw[:, 2 * r + 1 : 2 * r + 2])
            part = turn(part, factor, False)
        columns.append(jnp.concatenate(part, axis=0))
    spectrum = table_times(forward, jnp.concatenate(columns, axis=1))
    columns = []
    for r in range(radix):
        at = slice(r * width, (r + 1) * width)
        part = turn((spectrum[:points, at], spectrum[points:, at]), (hre[r], him[r]), False)
        columns.append(jnp.concatenate(part, axis=0))
    back = table_times(inverse, jnp.concatenate(columns, axis=1))
    parts = []
    for r in range(radix):
        at = slice(r * width, (r + 1) * width)
        part = (back[:points, at], back[points:, at])
        if r > 0:
            factor = (tw[:, 2 * r : 2 * r + 1], tw[:, 2 * r + 1 : 2 * r + 2])
            part = turn(part, factor, True)
        parts.append(part)
    for m, (re, im) in enumerate(small_transform(parts, 1.0)):
        for i in range(per):
            at = slice(i * rows, (i + 1) * rows)
            target.ref[target.at(m * per + i, 0)] = re[at]
            target.ref[target.at(m * per + i, 1)] = im[at]


def last_kernel(radix, ranks, *refs):
    in_refs, screens, (tw, inverse, out_ref, held) = refs[:ranks], refs[ranks : ranks + 4], refs[ranks + 4 :]
    points = held.shape[3]
    collect(in_refs, held, lax.axis_index("row"))
    for f, parts in enumerate(row_inverse(held, tw, inverse, radix, 2)):
        for m, part in enumerate(parts):
            at = slice(m * points, (m + 1) * points)
            factor = (screens[2 * f][:, at], screens[2 * f + 1][:, at])
            re, im = turn(part, factor, False)
            out_ref[f, 0, :, at] = re
            out_ref[f, 1, :, at] = im


def output_kernel(own_ref, got_ref, share_ref, more_ref, image_ref, leaving_ref):
    for core, (source, receiver) in enumerate(((own_ref, got_ref), (got_ref, own_ref))):

        @pl.when(lax.axis_index("depth") == core)
        def _():
            leaving_ref[0, 0:2] = source[core]
            leaving_ref[0, 2:4] = receiver[core]
            if core == 0:
                image_ref[0] = share_ref[...] + more_ref[...]
            else:
                terms = [source[f, i] * receiver[f, i] for f in range(2) for i in range(2)]
                image_ref[0] = (terms[0] + terms[1]) + (terms[2] + terms[3])


def signed_wave(positions, length):
    signed = jnp.where(positions < length // 2, positions, positions - length)
    return 2.0 * jnp.pi / length * signed.astype(jnp.float32)


def cos_sin(x):
    turns = jnp.floor(x * (2.0 / np.pi) + 0.5)
    rest = ((x - turns * 1.5703125) - turns * 4.837512969970703e-04) - turns * 7.549789948768648e-08
    square = rest * rest
    sine = 2.75573192e-06 - 2.50521084e-08 * square
    sine = -1.98412698e-04 + square * sine
    sine = 8.33333333e-03 + square * sine
    sine = -1.66666667e-01 + square * sine
    sine = rest + rest * square * sine
    cosine = -2.75573192e-07 + 2.08767570e-09 * square
    cosine = 2.48015873e-05 + square * cosine
    cosine = -1.38888889e-03 + square * cosine
    cosine = 4.16666667e-02 + square * cosine
    cosine = 1.0 - 0.5 * square + square * square * cosine
    count = turns.astype(jnp.int32)
    odd = (count & 1) == 1
    new_cos, new_sin = jnp.where(odd, sine, cosine), jnp.where(odd, cosine, sine)
    new_cos = jnp.where(((count + 1) & 2) == 2, -new_cos, new_cos)
    new_sin = jnp.where((count & 2) == 2, -new_sin, new_sin)
    return new_cos, new_sin


def omegas_of(freq_ref):
    omegas = [omega_step * freq_ref[f].astype(jnp.float32) for f in range(2)]
    return omegas, jnp.where(frequency_of() == 0, omegas[0], omegas[1])


def core_sign():
    return jnp.where(lax.axis_index("depth") == 0, -1.0, 1.0)


def propagator(radix, level, freq_ref, ref_ref, hre, him):
    col_radix, points, width = hre.shape
    length = col_radix * points
    _, omega = omegas_of(freq_ref)
    scale = 1.0 / (length * length)
    row_at = lax.broadcasted_iota(jnp.int32, (1, width), 1) * radix + residue_of()
    row_square = signed_wave(row_at, length) ** 2
    for r in range(col_radix):
        col_at = lax.broadcasted_iota(jnp.int32, (points, width), 0) * col_radix + r
        radicand = (omega * ref_ref[level]) ** 2 - (signed_wave(col_at, length) ** 2 + row_square)
        vertical = jnp.sqrt(jnp.maximum(radicand, 0.0)) * depth_step
        damping = scale * jnp.exp(-jnp.sqrt(jnp.maximum(-radicand, 0.0)) * depth_step)
        cosine, sine = cos_sin(vertical)
        hre[r], him[r] = damping * cosine, core_sign() * damping * sine


def screen(slow, slow_ref, omega, cos_ref, sin_ref):
    cosine, sine = cos_sin(omega * (slow - slow_ref) * depth_step)
    cos_ref[...], sin_ref[...] = cosine, core_sign() * sine


def factors_a(radix, freq_ref, ref_ref, tw_ref, tw_out, hre, him):
    tw_out[...] = tw_ref[...]
    propagator(radix, 0, freq_ref, ref_ref, hre, him)


def factors_b(freq_ref, ref_ref, slow_ref, other_ref, far_ref, sent_ref, *outs):
    first = lax.axis_index("depth") == 0
    _, omega = omegas_of(freq_ref)
    screen(jnp.where(first, slow_ref[0], other_ref[0]), ref_ref[0], omega, *outs[:2])
    screen(jnp.where(first, far_ref[...], sent_ref[...]), ref_ref[0], omega, *outs[2:])


def factors_c(radix, freq_ref, ref_ref, slow_ref, other_ref, keep_ref, got_ref, hre, him, share_ref, *outs):
    propagator(radix, 1, freq_ref, ref_ref, hre, him)
    last = jnp.where(lax.axis_index("depth") == 0, other_ref[0], slow_ref[0])
    omegas, _ = omegas_of(freq_ref)
    share_ref[...] = keep_ref[0] * got_ref[0] + keep_ref[1] * got_ref[1]
    for f in range(2):
        screen(last, ref_ref[1], omegas[f], *outs[2 * f : 2 * f + 2])


def call(kernel, out_shapes, scratch, args, held=True, scalars=()):
    vmem = pl.BlockSpec(memory_space=pltpu.VMEM)
    smem = pl.BlockSpec(memory_space=pltpu.SMEM)
    shape = pltpu.VMEM if held else jax.ShapeDtypeStruct
    return pl.pallas_call(
        kernel,
        in_specs=[smem] * len(scalars) + [vmem] * len(args),
        out_specs=[vmem] * len(out_shapes),
        out_shape=[shape(s, jnp.float32) for s in out_shapes],
        scratch_shapes=[pltpu.VMEM(s, jnp.float32) for s in scratch],
        compiler_params=pltpu.CompilerParams(vmem_limit_bytes=kernel_vmem),
    )(*scalars, *[pltpu.with_memory_space_constraint(a, pltpu.VMEM) for a in args])


def shards(planes, slowness, ref_slowness, freq_index):
    freqs, _, rows, length = planes.shape
    ranks = lax.axis_size("row")
    radix = ranks // 2
    points = length // radix
    col_radix = length // lanes

    row_forward_table, row_inverse_table = real_form(points)
    col_inverse_table, col_forward_table = real_form(lanes)
    row_tw = twiddles(length, radix)
    col_tw = twiddles(length, col_radix).transpose(2, 0, 1).reshape(lanes, 2 * col_radix)
    swap = [(0, 1), (1, 0)]
    both = ("depth", "row")

    def flat(c, r):
        return c * ranks + r

    def hop(array, step):
        return lax.ppermute(array, "row", [(r, r ^ step) for r in range(ranks)])

    def exchange(arrays, steps):
        got = list(arrays)
        for step in steps:
            got[step] = hop(arrays[step], step)
        return got

    inner_steps = list(range(1, radix))
    outer_steps = list(range(radix, ranks)) + list(range(1, radix))

    blocks = (ranks, 2, rows, points)
    quarter = (2, 2 * rows, points)
    half_field = (2, rows, length)
    vmem, hbm = (pl.BlockSpec(memory_space=space) for space in (pltpu.VMEM, pl.ANY))
    spectra = pl.pallas_call(
        functools.partial(first_kernel, radix),
        in_specs=[hbm] * 3,
        out_specs=[vmem] * ranks,
        out_shape=[pltpu.VMEM(blocks[1:], jnp.float32)] * ranks,
        scratch_shapes=[
            pltpu.VMEM((freqs,) + half_field, jnp.float32),
            pltpu.VMEM(row_tw.shape, jnp.float32),
            pltpu.VMEM(row_forward_table.shape, jnp.bfloat16),
            pltpu.VMEM(blocks, jnp.float32),
            pltpu.SemaphoreType.DMA((freqs + 2,)),
        ],
    )(planes, row_tw, row_forward_table)
    plane = (rows, length)
    factor = (col_radix, lanes, points)
    scalars = (freq_index, ref_slowness)
    held_tw, *propagator_a = call(
        functools.partial(factors_a, radix),
        [row_tw.shape] + [factor] * 2,
        [],
        (row_tw,),
        scalars=scalars,
    )
    far = lax.ppermute(slowness[0], both, [(flat(0, r), flat(0, r ^ radix)) for r in range(ranks)])
    other = lax.ppermute(slowness, "depth", swap)
    sent = lax.ppermute(far, "depth", [(0, 1)])
    screens_a = call(factors_b, [plane] * 4, [], (slowness, other, far, sent), scalars=scalars)
    columns = exchange(spectra, outer_steps)
    quarters = call(
        functools.partial(columns_to_quarters, col_radix, ranks),
        [quarter] * radix,
        [blocks, (radix,) + quarter],
        (*columns, *propagator_a, col_tw, col_forward_table, col_inverse_table),
    )
    quarters = exchange(quarters, inner_steps)
    *quarters, keep, send = call(
        functools.partial(middle_kernel, radix),
        [quarter] * radix + [half_field] * 2,
        [(radix,) + quarter, (2,) + half_field, (2,) + half_field],
        (*quarters, *screens_a, held_tw, row_inverse_table, row_forward_table),
    )
    quarters = exchange(quarters, inner_steps)
    got = lax.ppermute(send, "depth", swap)
    factors = call(
        functools.partial(factors_c, radix),
        [factor] * 2 + [plane] * 5,
        [],
        (slowness, other, keep, got),
        scalars=scalars,
    )
    propagator_b, share, screens_b = factors[:2], factors[2], factors[3:]
    more = lax.ppermute(share, both, [(flat(1, r), flat(0, r ^ radix)) for r in range(ranks)])
    columns = call(
        functools.partial(quarters_to_columns, col_radix, radix),
        [blocks[1:]] * ranks,
        [blocks, (radix,) + quarter],
        (*quarters, *propagator_b, col_tw, col_forward_table, col_inverse_table),
    )
    cells = exchange(columns, outer_steps)
    (fields,) = call(
        functools.partial(last_kernel, radix, ranks),
        [(freqs,) + half_field],
        [blocks],
        (*cells, *screens_b, held_tw, row_inverse_table),
    )
    swapped = lax.ppermute(fields, "depth", swap)
    image, leaving = call(
        output_kernel,
        [(1, rows, length), (1,) + planes.shape[1:]],
        [],
        (fields, swapped, share, more),
        held=False,
    )
    return image, leaving


def solution(mesh):
    in_specs = (P("groups", None, "row", None), P("depth", "row", None), P(), P())
    out_specs = (P(("groups", "depth"), "row", None), P(("groups", "depth"), None, "row", None))
    return jax.shard_map(shards, mesh=mesh, in_specs=in_specs, out_specs=out_specs, check_vma=False)
```

```python
import functools

import jax
import jax.numpy as jnp
import numpy as np
from jax import lax
from jax.experimental import pallas as pl
from jax.experimental.pallas import tpu as pltpu
from jax.sharding import PartitionSpec as P


omega_step = 0.05
depth_step = 1.0
lanes = 128
kernel_vmem = 24 << 20


def pair(table):
    high = table.astype(jnp.bfloat16)
    low = (table - high.astype(np.float64)).astype(jnp.bfloat16)
    return np.stack([high, low])


def real_form(points):
    product = np.outer(np.arange(points), np.arange(points)) % points
    angle = 2.0 * np.pi / points * product
    c, s = np.cos(angle), np.sin(angle)
    return pair(np.block([[c, -s], [s, c]])), pair(np.block([[c, s], [-s, c]]))


def twiddles(length, radix):
    points = length // radix
    angle = 2.0 * np.pi / length * np.outer(np.arange(radix), np.arange(points))
    return np.stack([np.cos(angle), -np.sin(angle)], axis=1).astype(np.float32)


def split(x):
    high = x.astype(jnp.bfloat16)
    return high, (x - high.astype(jnp.float32)).astype(jnp.bfloat16)


def dot(a, b):
    return jnp.dot(a, b, preferred_element_type=jnp.float32)


def times_table(x, table):
    high, low = split(x)
    return dot(high, table[0]) + dot(low, table[0]) + dot(high, table[1])


def table_times(table, x):
    high, low = split(x)
    return dot(table[0], high) + dot(table[0], low) + dot(table[1], high)


def scaled(value, factor):
    if value is None or factor == 0.0:
        return None
    if factor == 1.0:
        return value
    return -value if factor == -1.0 else value * factor


def plus(a, b):
    if a is None:
        return b
    return a if b is None else a + b


def small_transform(parts, sign):
    radix = len(parts)
    if radix == 1:
        return parts
    if radix % 2 == 0:
        half = radix // 2
        even = small_transform(parts[0::2], sign)
        odd = small_transform(parts[1::2], sign)
        first, second = [], []
        for r in range(half):
            angle = sign * 2.0 * np.pi * r / radix
            c, s = float(np.round(np.cos(angle), 15)), float(np.round(np.sin(angle), 15))
            ore, oim = odd[r]
            tre = plus(scaled(ore, c), scaled(oim, -s))
            tim = plus(scaled(oim, c), scaled(ore, s))
            ere, eim = even[r]
            first.append((ere + tre, eim + tim))
            second.append((ere - tre, eim - tim))
        return first + second
    raise ValueError("radix")


def turn(part, factor, conjugate):
    re, im = part
    fre, fim = factor
    if conjugate:
        return re * fre + im * fim, im * fre - re * fim
    return re * fre - im * fim, im * fre + re * fim


def rows_of(parts):
    return jnp.concatenate([jnp.concatenate(part, axis=1) for part in parts], axis=0)


def row_forward(cells, tw, table):
    stacked = []
    for parts in cells:
        for r, part in enumerate(small_transform(parts, -1.0)):
            factor = (tw[r, 0:1], tw[r, 1:2])
            stacked.append(part if r == 0 else turn(part, factor, False))
    return times_table(rows_of(stacked), table)


def row_inverse(ref, tw, table, radix, planes):
    rows, points = ref.shape[2], ref.shape[3]
    count = planes * radix
    stacked = jnp.concatenate(
        [ref[:, 0].reshape(count * rows, points), ref[:, 1].reshape(count * rows, points)], axis=1
    )
    out = times_table(stacked, table)
    cells = []
    for p in range(planes):
        parts = []
        for r in range(radix):
            at = (p * radix + r) * rows
            part = (out[at : at + rows, :points], out[at : at + rows, points:])
            parts.append(part if r == 0 else turn(part, (tw[r, 0:1], tw[r, 1:2]), True))
        cells.append(small_transform(parts, 1.0))
    return cells


def store_blocks(out_ref, value, count, rows, points):
    out_ref[:, 0] = value[:, :points].reshape(count, rows, points)
    out_ref[:, 1] = value[:, points:].reshape(count, rows, points)


def first_kernel(radix, planes_ref, tw_ref, table_ref, *rest):
    out_refs, (loaded, tw, table, held, sems) = rest[:-5], rest[-5:]
    freqs, _, rows, length = loaded.shape
    points = length // radix
    core = lax.axis_index("depth")
    copies = [
        pltpu.make_async_copy(planes_ref.at[f, pl.ds(2 * core, 2)], loaded.at[f], sems.at[f])
        for f in range(freqs)
    ]
    constants = [
        pltpu.make_async_copy(table_ref, table, sems.at[freqs]),
        pltpu.make_async_copy(tw_ref, tw, sems.at[freqs + 1]),
    ]
    for copy in copies + constants:
        copy.start()
    for copy in constants:
        copy.wait()
    for f, copy in enumerate(copies):
        copy.wait()
        parts = [
            tuple(loaded[f, i, :, m * points : (m + 1) * points] for i in range(2)) for m in range(radix)
        ]
        value = row_forward([parts], tw, table)
        at = slice(f * radix, (f + 1) * radix)
        held[at, 0] = value[:, :points].reshape(radix, rows, points)
        held[at, 1] = value[:, points:].reshape(radix, rows, points)
    spread(held, out_refs, lax.axis_index("row"))


def residue_of():
    return lax.rem(lax.axis_index("row"), lax.axis_size("row") // 2)


def frequency_of():
    return lax.axis_index("row") // (lax.axis_size("row") // 2)


def spread(held, out_refs, own):
    for step, ref in enumerate(out_refs):
        ref[0:2] = held[own ^ step]


def collect(in_refs, held, own):
    for step, ref in enumerate(in_refs):
        held[own ^ step] = ref[0:2]


def quarter_place(block, ranks):
    return block % (ranks // 2), block // (ranks // 2)


class Blocks:
    def __init__(self, ref, ranks, rows):
        self.ref, self.ranks, self.rows = ref, ranks, rows

    def at(self, block, part):
        return block, part


class Quarters(Blocks):
    def at(self, block, part):
        quarter, half = quarter_place(block, self.ranks)
        return quarter, part, slice(half * self.rows, (half + 1) * self.rows)


def columns_to_quarters(col_radix, ranks, *refs):
    in_refs, (hre, him, tw, forward, inverse), rest = refs[:ranks], refs[ranks : ranks + 5], refs[ranks + 5 :]
    out_refs, (blocks, quarters) = rest[:-2], rest[-2:]
    rows = blocks.shape[2]
    collect(in_refs, blocks, lax.axis_index("row"))
    source, target = Blocks(blocks, ranks, rows), Quarters(quarters, ranks, rows)
    column_kernel(col_radix, source, hre, him, tw, forward, inverse, target)
    spread(quarters, out_refs, residue_of())


def quarters_to_columns(col_radix, radix, *refs):
    in_refs, (share_ref, hre, him, tw, forward, inverse), rest = refs[:radix], refs[radix : radix + 6], refs[radix + 6 :]
    out_refs, (blocks, quarters) = rest[:-2], rest[-2:]
    ranks, rows, width = blocks.shape[0], blocks.shape[2], blocks.shape[3]
    collect(in_refs, quarters, residue_of())
    for k in range(radix):
        at = slice(k % 2 * rows // 2, (k % 2 + 1) * rows // 2)
        out_refs[radix][2 + k // 2, at] = share_ref[rows // 2 :, k * width : (k + 1) * width]
    source, target = Quarters(quarters, ranks, rows), Blocks(blocks, ranks, rows)
    column_kernel(col_radix, source, hre, him, tw, forward, inverse, target)
    spread(blocks, out_refs, lax.axis_index("row"))


def column_kernel(radix, source, hre, him, tw, forward, inverse, target):
    points, width = hre.shape[1], hre.shape[2]
    rows = source.rows
    per = points // rows

    def block(m, part):
        pieces = [source.ref[source.at(m * per + i, part)] for i in range(per)]
        return jnp.concatenate(pieces, axis=0)

    parts = small_transform([(block(m, 0), block(m, 1)) for m in range(radix)], -1.0)
    columns = []
    for r, part in enumerate(parts):
        if r > 0:
            factor = (tw[:, 2 * r : 2 * r + 1], tw[:, 2 * r + 1 : 2 * r + 2])
            part = turn(part, factor, False)
        columns.append(jnp.concatenate(part, axis=0))
    spectrum = table_times(forward, jnp.concatenate(columns, axis=1))
    columns = []
    for r in range(radix):
        at = slice(r * width, (r + 1) * width)
        part = turn((spectrum[:points, at], spectrum[points:, at]), (hre[r], him[r]), False)
        columns.append(jnp.concatenate(part, axis=0))
    back = table_times(inverse, jnp.concatenate(columns, axis=1))
    parts = []
    for r in range(radix):
        at = slice(r * width, (r + 1) * width)
        part = (back[:points, at], back[points:, at])
        if r > 0:
            factor = (tw[:, 2 * r : 2 * r + 1], tw[:, 2 * r + 1 : 2 * r + 2])
            part = turn(part, factor, True)
        parts.append(part)
    for m, (re, im) in enumerate(small_transform(parts, 1.0)):
        for i in range(per):
            at = slice(i * rows, (i + 1) * rows)
            target.ref[target.at(m * per + i, 0)] = re[at]
            target.ref[target.at(m * per + i, 1)] = im[at]


def middle_kernel(radix, *refs):
    in_refs, refs = refs[:radix], refs[radix:]
    (own_cos, own_sin, far_cos, far_sin, tw, inverse, forward), refs = refs[:7], refs[7:]
    out_refs, (keep_ref, send_ref, held, field, screen) = refs[:radix], refs[radix:]
    rows, points = held.shape[2], held.shape[3]
    mine = frequency_of()
    for half, pair_refs in ((mine, (own_cos, own_sin)), (1 - mine, (far_cos, far_sin))):
        for i, ref in enumerate(pair_refs):
            screen[i, half] = ref[...]
    collect(in_refs, held, residue_of())
    (cells,) = row_inverse(held, tw, inverse, radix, 1)
    turned = []
    for m in range(radix):
        at = slice(m * points, (m + 1) * points)
        factor = [screen[i, :, :, at].reshape(rows, points) for i in range(2)]
        part = turn(cells[m], factor, False)
        for half in range(2):
            for i in range(2):
                field[half, i, :, at] = part[i][half * rows // 2 : (half + 1) * rows // 2]
        turned.append(part)
    core, part_rows = lax.axis_index("depth"), rows // 4
    for ref, sub in ((keep_ref, core), (send_ref, 1 - core)):
        at = pl.ds(pl.multiple_of(sub * part_rows, 8), part_rows)
        for place, block in enumerate((mine, 1 - mine)):
            ref[:, place * part_rows : (place + 1) * part_rows] = field[block, :, at]
    value = row_forward([turned], tw, forward)
    store_blocks(held, value, radix, rows, points)
    spread(held, out_refs, residue_of())


def column_kernel(radix, source, hre, him, tw, forward, inverse, target):
    points, width = hre.shape[1], hre.shape[2]
    rows = source.rows
    per = points // rows

    def block(m, part):
        pieces = [source.ref[source.at(m * per + i, part)] for i in range(per)]
        return jnp.concatenate(pieces, axis=0)

    parts = small_transform([(block(m, 0), block(m, 1)) for m in range(radix)], -1.0)
    columns = []
    for r, part in enumerate(parts):
        if r > 0:
            factor = (tw[:, 2 * r : 2 * r + 1], tw[:, 2 * r + 1 : 2 * r + 2])
            part = turn(part, factor, False)
        columns.append(jnp.concatenate(part, axis=0))
    spectrum = table_times(forward, jnp.concatenate(columns, axis=1))
    columns = []
    for r in range(radix):
        at = slice(r * width, (r + 1) * width)
        part = turn((spectrum[:points, at], spectrum[points:, at]), (hre[r], him[r]), False)
        columns.append(jnp.concatenate(part, axis=0))
    back = table_times(inverse, jnp.concatenate(columns, axis=1))
    parts = []
    for r in range(radix):
        at = slice(r * width, (r + 1) * width)
        part = (back[:points, at], back[points:, at])
        if r > 0:
            factor = (tw[:, 2 * r : 2 * r + 1], tw[:, 2 * r + 1 : 2 * r + 2])
            part = turn(part, factor, True)
        parts.append(part)
    for m, (re, im) in enumerate(small_transform(parts, 1.0)):
        for i in range(per):
            at = slice(i * rows, (i + 1) * rows)
            target.ref[target.at(m * per + i, 0)] = re[at]
            target.ref[target.at(m * per + i, 1)] = im[at]


def last_kernel(radix, ranks, *refs):
    in_refs, screens, refs = refs[:ranks], refs[ranks : ranks + 4], refs[ranks + 4 :]
    share_ref, tw, inverse, out_ref, held = refs
    rows, points = held.shape[2], held.shape[3]
    for k in range(radix):
        at, columns = slice(k % 2 * rows // 2, (k % 2 + 1) * rows // 2), slice(k * points, (k + 1) * points)
        out_ref[4, : rows // 2, columns] = share_ref[: rows // 2, columns] + in_refs[radix][2 + k // 2, at]
    collect(in_refs, held, lax.axis_index("row"))
    for f, parts in enumerate(row_inverse(held, tw, inverse, radix, 2)):
        for m, part in enumerate(parts):
            at = slice(m * points, (m + 1) * points)
            factor = (screens[2 * f][:, at], screens[2 * f + 1][:, at])
            re, im = turn(part, factor, False)
            out_ref[2 * f, :, at] = re
            out_ref[2 * f + 1, :, at] = im


def output_kernel(own_ref, got_ref, image_ref, leaving_ref):
    half = own_ref.shape[1] // 2
    for core, (source, receiver) in enumerate(((own_ref, got_ref), (got_ref, own_ref))):

        @pl.when(lax.axis_index("depth") == core)
        def _():
            leaving_ref[0, 0:2] = source[2 * core : 2 * core + 2]
            leaving_ref[0, 2:4] = receiver[2 * core : 2 * core + 2]
            if core == 0:
                image_ref[0, :half] = own_ref[4, :half]
                image_ref[0, half:] = got_ref[4, :half]
            else:
                terms = [source[i] * receiver[i] for i in range(4)]
                image_ref[0] = (terms[0] + terms[1]) + (terms[2] + terms[3])


def signed_wave(positions, length):
    signed = jnp.where(positions < length // 2, positions, positions - length)
    return 2.0 * jnp.pi / length * signed.astype(jnp.float32)


def cos_sin(x):
    turns = jnp.floor(x * (2.0 / np.pi) + 0.5)
    rest = ((x - turns * 1.5703125) - turns * 4.837512969970703e-04) - turns * 7.549789948768648e-08
    square = rest * rest
    sine = 2.75573192e-06 - 2.50521084e-08 * square
    sine = -1.98412698e-04 + square * sine
    sine = 8.33333333e-03 + square * sine
    sine = -1.66666667e-01 + square * sine
    sine = rest + rest * square * sine
    cosine = -2.75573192e-07 + 2.08767570e-09 * square
    cosine = 2.48015873e-05 + square * cosine
    cosine = -1.38888889e-03 + square * cosine
    cosine = 4.16666667e-02 + square * cosine
    cosine = 1.0 - 0.5 * square + square * square * cosine
    count = turns.astype(jnp.int32)
    odd = (count & 1) == 1
    new_cos, new_sin = jnp.where(odd, sine, cosine), jnp.where(odd, cosine, sine)
    new_cos = jnp.where(((count + 1) & 2) == 2, -new_cos, new_cos)
    new_sin = jnp.where((count & 2) == 2, -new_sin, new_sin)
    return new_cos, new_sin


def omegas_of(freq_ref):
    omegas = [omega_step * freq_ref[f].astype(jnp.float32) for f in range(2)]
    return omegas, jnp.where(frequency_of() == 0, omegas[0], omegas[1])


def core_sign():
    return jnp.where(lax.axis_index("depth") == 0, -1.0, 1.0)


def propagator(radix, level, freq_ref, ref_ref, hre, him):
    col_radix, points, width = hre.shape
    length = col_radix * points
    _, omega = omegas_of(freq_ref)
    scale = 1.0 / (length * length)
    row_at = lax.broadcasted_iota(jnp.int32, (1, width), 1) * radix + residue_of()
    row_square = signed_wave(row_at, length) ** 2
    for r in range(col_radix):
        col_at = lax.broadcasted_iota(jnp.int32, (points, width), 0) * col_radix + r
        radicand = (omega * ref_ref[level]) ** 2 - (signed_wave(col_at, length) ** 2 + row_square)
        vertical = jnp.sqrt(jnp.maximum(radicand, 0.0)) * depth_step
        damping = scale * jnp.exp(-jnp.sqrt(jnp.maximum(-radicand, 0.0)) * depth_step)
        cosine, sine = cos_sin(vertical)
        hre[r], him[r] = damping * cosine, core_sign() * damping * sine


def screen(slow, slow_ref, omega, cos_ref, sin_ref):
    cosine, sine = cos_sin(omega * (slow - slow_ref) * depth_step)
    cos_ref[...], sin_ref[...] = cosine, core_sign() * sine


def factors_a(radix, freq_ref, ref_ref, tw_ref, tw_out, hre, him):
    tw_out[...] = tw_ref[...]
    propagator(radix, 0, freq_ref, ref_ref, hre, him)


def factors_b(freq_ref, ref_ref, slow_ref, other_ref, far_ref, sent_ref, *outs):
    first = lax.axis_index("depth") == 0
    _, omega = omegas_of(freq_ref)
    screen(jnp.where(first, slow_ref[0], other_ref[0]), ref_ref[0], omega, *outs[:2])
    screen(jnp.where(first, far_ref[...], sent_ref[...]), ref_ref[0], omega, *outs[2:])


def factors_c(radix, freq_ref, ref_ref, slow_ref, other_ref, keep_ref, got_ref, hre, him, share_ref, *outs):
    propagator(radix, 1, freq_ref, ref_ref, hre, him)
    last = jnp.where(lax.axis_index("depth") == 0, other_ref[0], slow_ref[0])
    omegas, _ = omegas_of(freq_ref)
    share_ref[...] = keep_ref[0] * got_ref[0] + keep_ref[1] * got_ref[1]
    for f in range(2):
        screen(last, ref_ref[1], omegas[f], *outs[2 * f : 2 * f + 2])


def call(kernel, out_shapes, scratch, args, held=True, scalars=()):
    vmem = pl.BlockSpec(memory_space=pltpu.VMEM)
    smem = pl.BlockSpec(memory_space=pltpu.SMEM)
    shape = pltpu.VMEM if held else jax.ShapeDtypeStruct
    return pl.pallas_call(
        kernel,
        in_specs=[smem] * len(scalars) + [vmem] * len(args),
        out_specs=[vmem] * len(out_shapes),
        out_shape=[shape(s, jnp.float32) for s in out_shapes],
        scratch_shapes=[pltpu.VMEM(s, jnp.float32) for s in scratch],
        compiler_params=pltpu.CompilerParams(vmem_limit_bytes=kernel_vmem),
    )(*scalars, *[pltpu.with_memory_space_constraint(a, pltpu.VMEM) for a in args])


def shards(planes, slowness, ref_slowness, freq_index):
    freqs, _, rows, length = planes.shape
    ranks = lax.axis_size("row")
    radix = ranks // 2
    points = length // radix
    col_radix = length // lanes

    row_forward_table, row_inverse_table = real_form(points)
    col_inverse_table, col_forward_table = real_form(lanes)
    row_tw = twiddles(length, radix)
    col_tw = twiddles(length, col_radix).transpose(2, 0, 1).reshape(lanes, 2 * col_radix)
    swap = [(0, 1), (1, 0)]
    both = ("depth", "row")

    def flat(c, r):
        return c * ranks + r

    def hop(array, step):
        return lax.ppermute(array, "row", [(r, r ^ step) for r in range(ranks)])

    def exchange(arrays, steps):
        got = list(arrays)
        for step in steps:
            got[step] = hop(arrays[step], step)
        return got

    inner_steps = list(range(1, radix))
    outer_steps = list(range(radix, ranks)) + list(range(1, radix))

    blocks = (ranks, 2, rows, points)
    quarter = (2, 2 * rows, points)
    half_field = (2, rows, length)
    vmem, hbm = (pl.BlockSpec(memory_space=space) for space in (pltpu.VMEM, pl.ANY))
    spectra = pl.pallas_call(
        functools.partial(first_kernel, radix),
        in_specs=[hbm] * 3,
        out_specs=[vmem] * ranks,
        out_shape=[pltpu.VMEM(blocks[1:], jnp.float32)] * ranks,
        scratch_shapes=[
            pltpu.VMEM((freqs,) + half_field, jnp.float32),
            pltpu.VMEM(row_tw.shape, jnp.float32),
            pltpu.VMEM(row_forward_table.shape, jnp.bfloat16),
            pltpu.VMEM(blocks, jnp.float32),
            pltpu.SemaphoreType.DMA((freqs + 2,)),
        ],
    )(planes, row_tw, row_forward_table)
    plane = (rows, length)
    factor = (col_radix, lanes, points)
    scalars = (freq_index, ref_slowness)
    held_tw, *propagator_a = call(
        functools.partial(factors_a, radix),
        [row_tw.shape] + [factor] * 2,
        [],
        (row_tw,),
        scalars=scalars,
    )
    far = lax.ppermute(slowness[0], both, [(flat(0, r), flat(0, r ^ radix)) for r in range(ranks)])
    other = lax.ppermute(slowness, "depth", swap)
    sent = lax.ppermute(far, "depth", [(0, 1)])
    screens_a = call(factors_b, [plane] * 4, [], (slowness, other, far, sent), scalars=scalars)
    columns = exchange(spectra, outer_steps)
    quarters = call(
        functools.partial(columns_to_quarters, col_radix, ranks),
        [quarter] * radix,
        [blocks, (radix,) + quarter],
        (*columns, *propagator_a, col_tw, col_forward_table, col_inverse_table),
    )
    quarters = exchange(quarters, inner_steps)
    *quarters, keep, send = call(
        functools.partial(middle_kernel, radix),
        [quarter] * radix + [half_field] * 2,
        [(radix,) + quarter, (2,) + half_field, (2,) + half_field],
        (*quarters, *screens_a, held_tw, row_inverse_table, row_forward_table),
    )
    quarters = exchange(quarters, inner_steps)
    got = lax.ppermute(send, "depth", swap)
    factors = call(
        functools.partial(factors_c, radix),
        [factor] * 2 + [plane] * 5,
        [],
        (slowness, other, keep, got),
        scalars=scalars,
    )
    propagator_b, share, screens_b = factors[:2], factors[2], factors[3:]
    columns = call(
        functools.partial(quarters_to_columns, col_radix, radix),
        [(2 + radix // 2 if step == radix else 2,) + blocks[2:] for step in range(ranks)],
        [blocks, (radix,) + quarter],
        (*quarters, share, *propagator_b, col_tw, col_forward_table, col_inverse_table),
    )
    cells = exchange(columns, outer_steps)
    (fields,) = call(
        functools.partial(last_kernel, radix, ranks),
        [(2 * freqs + 1,) + plane],
        [blocks],
        (*cells, *screens_b, share, held_tw, row_inverse_table),
    )
    swapped = lax.ppermute(fields, "depth", swap)
    image, leaving = call(
        output_kernel,
        [(1, rows, length), (1,) + planes.shape[1:]],
        [],
        (fields, swapped),
        held=False,
    )
    return image, leaving


def solution(mesh):
    in_specs = (P("groups", None, "row", None), P("depth", "row", None), P(), P())
    out_specs = (P(("groups", "depth"), "row", None), P(("groups", "depth"), None, "row", None))
    return jax.shard_map(shards, mesh=mesh, in_specs=in_specs, out_specs=out_specs, check_vma=False)
```
